512 devices in a mesh: gx: 16 (over z), gy: 8 (over y, x_lo), gz: 4 (over x_hi, core).
Axes of the slice: x: 4 (x_hi: 2, x_lo: 2; x = x_hi * 2 + x_lo), y: 4, z: 16, core: 2. Of those that a mesh axis runs over, the one named last changes fastest.
Arguments:
- start_disp: float32 [3, 128, 64, 512], P(None, 'gx', 'gy', 'gz'), may hold values from -2 to 2
- inertial: float32 [3, 128, 64, 512], P(None, 'gx', 'gy', 'gz'), may hold values from -1 to 1
- material: int32 [128, 64, 512], P('gx', 'gy', 'gz'), may hold values from 0 to 7
- pinned: int32 [128, 64, 512], P('gx', 'gy', 'gz'), may hold values 0 or 1
- stiffness: float32 [8], replicated, may hold values from 3 to 100
Outputs:
- displacement: float32 [3, 128, 64, 512], P(None, 'gx', 'gy', 'gz')
The draws below stay inside these ranges and needn't reach their ends.
All inputs are finite; a program needn't handle non-finite values. No bound on the sum of `pinned` on one device may be relied on, other than what follows from the above.
Results may differ from the reference program's by a relative error of at most 0.0003.
Values sent between devices are 32-bit elements; how exact they have to be, the bound alone decides.
A program may use at most 64 MiB of HBM per device.

```python
import math
import jax
import jax.numpy as jnp
from jax import lax

CX = 8
ITERS = 4
POLAR_STEPS = 6
MATS = 8
NX = 128
NY = 64
NZ = 512


def set_ends(drawn, rng, low, largest):
    spot = [jax.random.randint(jax.random.fold_in(rng, axis), (), 0, length) for axis, length in enumerate(drawn.shape)]
    main_axis = drawn.shape.index(max(drawn.shape))
    next_to = spot[:main_axis] + [(spot[main_axis] + 1) % drawn.shape[main_axis]] + spot[main_axis + 1:]
    return drawn.at[tuple(spot)].set(low).at[tuple(next_to)].set(largest)


def levels(own_key, dims, split, low, largest):
    loudness, own = 1.0, jax.random.fold_in(own_key, 6)
    for position, shards_of in split:
        draws = jnp.exp(jax.random.uniform(jax.random.fold_in(own, position), (shards_of,), jnp.float32, low / len(split), largest / len(split)))
        loudness = loudness * jnp.repeat(draws, dims[position] // shards_of).reshape([-1 if axis == position else 1 for axis in range(len(dims))])
    return loudness


def gaussian(stream_key, extent, spread, most, cuts=(), kind=jnp.bfloat16):
    level = levels(stream_key, extent, cuts, -0.22, 0.18) if cuts else 1.0
    values = jax.random.normal(stream_key, extent, jnp.float32) * spread * level
    return jnp.minimum(jnp.maximum(values, -most), most).astype(kind)


def setup_inputs(seed: int = 0) -> dict:
    key_of = jax.random.split(jax.random.key(seed), 6)
    return {
        "start_disp": gaussian(key_of[0], (3, NX, NY, NZ), 0.5, 2.0, ((1, 16), (2, 8), (3, 4)), jnp.float32),
        "inertial": gaussian(key_of[1], (3, NX, NY, NZ), 0.25, 1.0, ((1, 16), (2, 8), (3, 4)), jnp.float32),
        "material": set_ends(jax.random.randint(key_of[2], (NX, NY, NZ), 0, MATS), jax.random.fold_in(key_of[2], 1), 0, MATS - 1).astype(jnp.int32),
        "pinned": set_ends((jax.random.randint(key_of[3], (NX, NY, NZ), 0, 16) < 1).astype(jnp.int32), jax.random.fold_in(key_of[3], 1), 0, 1),
        "stiffness": jnp.clip(jnp.exp(jax.random.uniform(key_of[4], (MATS,), jnp.float32, math.log(3.0), math.log(100.0))), 3.0, 100.0),
    }


inertia = 1.0
relax = 0.6
radius = 0.9

def forward_diff(field, axis):
    size = field.shape[axis]
    return lax.slice_in_dim(field, 1, size, axis=axis) - lax.slice_in_dim(field, 0, size - 1, axis=axis)

def pair_sum(field, axis):
    size = field.shape[axis]
    return lax.slice_in_dim(field, 1, size, axis=axis) + lax.slice_in_dim(field, 0, size - 1, axis=axis)

def gradient(field, axis):
    result = forward_diff(field, axis)
    for other in range(3):
        if other != axis:
            result = pair_sum(result, other)
    return 0.25 * result

def project(nodes, welem):
    deform = [[gradient(nodes[c], d) + (1.0 if c == d else 0.0) for d in range(3)] for c in range(3)]
    total = sum((deform[c][d] * deform[c][d] for c in range(3) for d in range(3)))
    scale = jnp.maximum(jnp.sqrt(total / 3.0), 1.0)
    rotate = [[deform[c][d] / scale for d in range(3)] for c in range(3)]
    for step in range(POLAR_STEPS):
        middle = [[(1.5 if i == j else 0.0) - 0.5 * sum((rotate[k][i] * rotate[k][j] for k in range(3))) for j in range(3)] for i in range(3)]
        rotate = [[sum((rotate[c][j] * middle[j][d] for j in range(3))) for d in range(3)] for c in range(3)]
    return [welem * (deform[c][d] - rotate[c][d]) for c in range(3) for d in range(3)]

def assemble(stress):
    forces = []
    for c in range(3):
        total = 0.0
        for d in range(3):
            term = stress[3 * c + d]
            for other in range(3):
                if other != d:
                    term = pair_sum(term, other)
            total = total - 0.25 * forward_diff(term, d)
        forces.append(total)
    return jnp.stack(forces)

def diagonal(welem):
    total = welem
    for axis in range(3):
        total = pair_sum(total, axis)
    return inertia + 3.0 / 16.0 * total

def lookup(material, stiffness):
    total = jnp.zeros(material.shape, jnp.float32)
    for index in range(MATS):
        total = total + jnp.where(material == index, stiffness[index], 0.0)
    return total

def reference(start_disp, inertial, material, pinned, stiffness):
    grid_x = lax.broadcasted_iota(jnp.int32, material.shape, 0)
    grid_y = lax.broadcasted_iota(jnp.int32, material.shape, 1)
    grid_z = lax.broadcasted_iota(jnp.int32, material.shape, 2)
    valid = (grid_x < NX - 1) & (grid_y < NY - 1) & (grid_z < NZ - 1)
    weights = jnp.where(valid, lookup(material, stiffness), 0.0)
    welem = jnp.pad(weights, ((1, 0), (1, 0), (1, 0)))
    diag = diagonal(welem)
    pins = pinned[None] > 0
    disp = jnp.where(pins, inertial, start_disp)
    previous = disp
    omega = 1.0
    blocks = NX // CX
    for step in range(ITERS):
        padded = jnp.pad(disp, ((0, 0), (1, 1), (1, 1), (1, 1)))

        def block_forces(index):
            start = (index * CX).astype(jnp.int32)
            nodes = lax.dynamic_slice_in_dim(padded, start, CX + 2, 1)
            wslab = lax.dynamic_slice_in_dim(welem, start, CX + 1, 0)
            return assemble(project([nodes[0], nodes[1], nodes[2]], wslab))
        parts = lax.map(block_forces, jnp.arange(blocks, dtype=jnp.int32))
        forces = jnp.moveaxis(parts, 0, 1).reshape(3, NX, NY, NZ)
        target = disp - relax * (inertia * (disp - inertial) + forces) / diag[None]
        if step == 0:
            fresh = target
        else:
            omega = 2.0 / (2.0 - radius * radius) if step == 1 else 4.0 / (4.0 - radius * radius * omega)
            fresh = omega * (target - previous) + previous
        fresh = jnp.where(pins, inertial, fresh)
        previous = disp
        disp = fresh
    return disp
```

```python
import functools

import jax
import jax.numpy as jnp
from jax import lax
from jax.experimental import pallas as pl
from jax.experimental.pallas import tpu as pltpu
from jax.sharding import PartitionSpec as P

ITERS = 4
POLAR_STEPS = 6
MATS = 8

relax = 0.6
radius = 0.9

AXES = ("gx", "gy", "gz")
BX = 8
HALO = 2
EX = BX + 2 * HALO
EZ = 128 + 2 * HALO
SLAB = 13
ROWS = 176
VOFF = 16
DIRS = [
    (dx, dy, dz)
    for dx in (-1, 0, 1)
    for dy in (-1, 0, 1)
    for dz in (-1, 0, 1)
    if (dx, dy, dz) != (0, 0, 0)
]


def every(conds):
    conds = [c for c in conds if c is not True]
    return functools.reduce(lambda p, q: p & q, conds) if conds else True


def guarded(cond, act):
    if cond is True:
        act()
    else:
        pl.when(cond)(act)


class Group:
    def __init__(self, width, refs):
        self.h = width
        self.ro, self.ry, self.sy, self.szo, self.szy, self.zo, self.zy, self.ssem, self.rsem = refs
        self.count = self.ro.shape[0]

    @staticmethod
    def scratch(width, count):
        f = jnp.float32
        return [
            pltpu.VMEM((count, EX, BX, 128), f),
            pltpu.VMEM((count, EX, 2, width, 128), f),
            pltpu.VMEM((count, BX, 2, width, 128), f),
            pltpu.VMEM((BX, BX, 128), f),
            pltpu.VMEM((BX, 2, width, 128), f),
            pltpu.VMEM((2, EX, BX, 128), f),
            pltpu.VMEM((2, EX, 2, width, 128), f),
            pltpu.SemaphoreType.DMA((len(DIRS),)),
            pltpu.SemaphoreType.DMA((len(DIRS),)),
        ]

    def copy(self, index, pos):
        dx, dy, dz = DIRS[index]
        h = self.h
        src_x = {-1: (0, h), 0: (0, BX), 1: (BX - h, h)}[dx]
        dst_x = {-1: (HALO + BX, h), 0: (HALO, BX), 1: (HALO - h, h)}[dx]
        src_side, dst_side = {-1: (0, 1), 0: (0, 0), 1: (1, 0)}[dy]
        zside = 0 if dz == 1 else 1
        sx, tx = pl.ds(*src_x), pl.ds(*dst_x)
        if dz == 0:
            if dy == 0:
                src = self.ro.at[:, pl.ds(HALO + src_x[0], src_x[1])]
                dst = self.ro.at[:, tx]
            else:
                src, dst = self.sy.at[:, sx, src_side], self.ry.at[:, tx, dst_side]
        elif dy == 0:
            src, dst = self.szo.at[sx], self.zo.at[zside, tx]
        else:
            src, dst = self.szy.at[sx, src_side], self.zy.at[zside, tx, dst_side]
        return pltpu.make_async_remote_copy(
            src_ref=src,
            dst_ref=dst,
            send_sem=self.ssem.at[index],
            recv_sem=self.rsem.at[index],
            device_id={a: p + d for a, p, d in zip(AXES, pos, DIRS[index])},
            device_id_type=pl.DeviceIdType.MESH,
        )

    def put(self, i, tiles, lane):
        h = self.h
        pack = jnp.zeros_like(tiles[0])
        for c, tile in enumerate(tiles):
            self.ro[c, HALO + i] = tile
            self.sy[c, i, 0] = tile[0:h]
            self.sy[c, i, 1] = tile[BX - h : BX]
            low = pltpu.roll(tile, 4 * c, 1) if c else tile
            high = pltpu.roll(tile, 4 * c + 4, 1)
            inside = (lane >= 4 * c) & (lane < 4 * c + 2)
            pack = jnp.where(inside, low, pack)
            inside = (lane >= 4 * c + 2) & (lane < 4 * c + 4)
            pack = jnp.where(inside, high, pack)
        self.szo[i] = pack
        self.szy[i, 0] = pack[0:h]
        self.szy[i, 1] = pack[BX - h : BX]

    def clear(self, has):
        for d, (start, size) in ((-1, (0, HALO)), (1, (HALO + BX, HALO))):

            def clear_x(start=start, size=size):
                for x in range(start, start + size):
                    for c in range(self.count):
                        self.ro[c, x] = jnp.zeros((BX, 128), jnp.float32)
                        self.ry[c, x] = jnp.zeros(self.ry.shape[2:], jnp.float32)
                    for s in range(2):
                        self.zo[s, x] = jnp.zeros((BX, 128), jnp.float32)
                        self.zy[s, x] = jnp.zeros(self.zy.shape[2:], jnp.float32)

            pl.when(jnp.logical_not(has[0][d]))(clear_x)

            def clear_y(side=(0 if d == -1 else 1)):
                for x in range(EX):
                    for c in range(self.count):
                        self.ry[c, x, side] = jnp.zeros((self.h, 128), jnp.float32)
                    for s in range(2):
                        self.zy[s, x, side] = jnp.zeros((self.h, 128), jnp.float32)

            pl.when(jnp.logical_not(has[1][d]))(clear_y)

            def clear_z(side=(0 if d == -1 else 1)):
                for x in range(EX):
                    self.zo[side, x] = jnp.zeros((BX, 128), jnp.float32)
                    self.zy[side, x] = jnp.zeros(self.zy.shape[2:], jnp.float32)

            pl.when(jnp.logical_not(has[2][d]))(clear_z)

    def send(self, pos, has):
        for index, d in enumerate(DIRS):
            guarded(every([has[a][d[a]] for a in range(3)]), self.copy(index, pos).start)

    def wait_recv(self, pos, has):
        for index, d in enumerate(DIRS):
            guarded(every([has[a][-d[a]] for a in range(3)]), self.copy(index, pos).wait_recv)

    def wait_send(self, pos, has):
        for index, d in enumerate(DIRS):
            guarded(every([has[a][d[a]] for a in range(3)]), self.copy(index, pos).wait_send)

    def to_flat(self, targets):
        h = self.h
        count = self.count
        for part in range(2):
            rows = BX if part == 0 else 2 * h
            lane = lax.broadcasted_iota(jnp.int32, (rows, 128), 1)
            main, zs = (self.ro, self.zo) if part == 0 else (self.ry, self.zy)
            zero = jnp.zeros((rows, 128), jnp.float32)
            before = [zero] * count
            high = zero
            for place in range(SLAB):
                last = place == SLAB - 1
                low = zero if last else zs[0, place].reshape(rows, 128)
                both = jnp.where((lane & 3) < 2, high, low)
                if not last:
                    high = zs[1, place].reshape(rows, 128)
                for c in range(count):
                    now = (
                        zero
                        if last
                        else pltpu.roll(main[c, place].reshape(rows, 128), 4 * place + 2, 1)
                    )
                    ends = pltpu.roll(both, (4 * place - 2 - 4 * c) % 128, 1)
                    flat = jnp.where(
                        lane >= 4 * place + 2,
                        now,
                        jnp.where(lane < 4 * place - 2, before[c], ends),
                    )
                    before[c] = now
                    out = targets[c]
                    if part == 0:
                        out[pl.ds(HALO * SLAB + place, BX, stride=SLAB), :] = flat
                    elif h == 1:
                        out[pl.ds(SLAB + place, 2, stride=9 * SLAB), :] = flat
                    else:
                        out[pl.ds(place, 2, stride=SLAB), :] = flat[0:2]
                        out[pl.ds(10 * SLAB + place, 2, stride=SLAB), :] = flat[2:4]


def own_tile(flat, place, lane):
    start = HALO * SLAB + place
    shift = 4 * place + 2
    first = flat[pl.ds(start, BX, stride=SLAB), :]
    second = flat[pl.ds(start + 1, BX, stride=SLAB), :]
    return pltpu.roll(jnp.where(lane >= shift, first, second), 128 - shift, 1)


def loop(start, rows, step, body):
    trips = -(-rows // step)
    lax.fori_loop(0, trips, lambda t, carry: (body(start + t * step), carry)[1], 0)


def after(ref, row, n, lane, shift):
    whole, part = divmod(shift, 128)
    near = ref[pl.ds(row + whole, n), :]
    far = ref[pl.ds(row + whole + 1, n), :]
    return pltpu.roll(jnp.where(lane < part, far, near), 128 - part, 1)


def earlier(ref, row, n, lane, shift):
    whole, part = divmod(shift, 128)
    near = ref[pl.ds(row - whole, n), :]
    far = ref[pl.ds(row - whole - 1, n), :]
    return pltpu.roll(jnp.where(lane >= 128 - part, far, near), part, 1)


def differences(u, grads, start, rows, n):
    lane = lax.broadcasted_iota(jnp.int32, (n, 128), 1)

    def body(r):
        for c in range(3):
            ref = u.at[c]
            a00 = ref[pl.ds(r, n), :]
            a01 = after(ref, r, n, lane, 1)
            a10 = after(ref, r, n, lane, EZ)
            a11 = after(ref, r, n, lane, EZ + 1)
            s0, s1 = a00 + a01, a10 + a11
            grads[3 * c, pl.ds(r, n), :] = s1 - s0
            grads[3 * c + 1, pl.ds(r, n), :] = s0 + s1
            grads[3 * c + 2, pl.ds(r, n), :] = (a01 - a00) + (a11 - a10)

    loop(start, rows, n, body)


def stresses(grads, weights, corners, spread, start, rows, n):
    def body(r):
        def at(k, row):
            return grads[k, pl.ds(row, n), :]

        deform = []
        for c in range(3):
            fx = at(3 * c, r) + at(3 * c, r + SLAB)
            fy = at(3 * c + 1, r + SLAB) - at(3 * c + 1, r)
            fz = at(3 * c + 2, r) + at(3 * c + 2, r + SLAB)
            deform.append([fx, fy, fz])
        for c in range(3):
            deform[c][c] = deform[c][c] + 1.0
        rows_sq = [
            deform[c][0] * deform[c][0] + deform[c][1] * deform[c][1] + deform[c][2] * deform[c][2]
            for c in range(3)
        ]
        total = rows_sq[0] + rows_sq[1] + rows_sq[2]
        scale = jnp.minimum(lax.rsqrt(total * (2.0 / 3.0)), 0.5**0.5)
        y = [[deform[c][d] * scale for d in range(3)] for c in range(3)]
        weight = weights[pl.ds(r, n), :]
        heavy = weight * 2.0**0.5
        for step in range(POLAR_STEPS):

            def gram(i, j):
                return y[0][i] * y[0][j] + y[1][i] * y[1][j] + y[2][i] * y[2][j]

            d0, d1, d2 = 1.5 - gram(0, 0), 1.5 - gram(1, 1), 1.5 - gram(2, 2)
            o01, o02, o12 = gram(0, 1), gram(0, 2), gram(1, 2)
            if step == POLAR_STEPS - 1:
                d0, d1, d2 = d0 * heavy, d1 * heavy, d2 * heavy
                o01, o02, o12 = o01 * heavy, o02 * heavy, o12 * heavy
            y = [
                [
                    y[c][0] * d0 - (y[c][1] * o01 + y[c][2] * o02),
                    y[c][1] * d1 - (y[c][0] * o01 + y[c][2] * o12),
                    y[c][2] * d2 - (y[c][0] * o02 + y[c][1] * o12),
                ]
                for c in range(3)
            ]
        for c in range(3):
            px, py, pz = (weight * deform[c][d] - y[c][d] for d in range(3))
            s, t = py + px, py - px
            parts = (s + pz, s - pz, t + pz, t - pz)
            for k in range(4):
                corners[4 * c + k, pl.ds(r + VOFF, n), :] = parts[k]
            for k in range(4):
                below = corners[4 * c + k, pl.ds(r + VOFF - SLAB, n), :]
                spread[4 * c + k, pl.ds(r, n), :] = below - parts[3 - k]

    loop(start, rows, n, body)


def update(u, prev, fresh, inertial, rate, spread, omega, start, rows, n):
    lane = lax.broadcasted_iota(jnp.int32, (n, 128), 1)

    def body(r):
        a = rate[pl.ds(r, n), :]
        for c in range(3):
            force = (
                earlier(spread.at[4 * c], r, n, lane, EZ + 1)
                + earlier(spread.at[4 * c + 1], r, n, lane, EZ)
            ) + (
                earlier(spread.at[4 * c + 2], r, n, lane, 1)
                + spread[4 * c + 3, pl.ds(r, n), :]
            )
            here = u[c, pl.ds(r, n), :]
            new = here - a * ((here - inertial[c, pl.ds(r, n), :]) + force)
            if omega is not None:
                old = prev[c, pl.ds(r, n), :]
                new = omega * (new - old) + old
            fresh[c, pl.ds(r, n), :] = new

    loop(start, rows, n, body)


def kernel(
    start_hbm,
    inertial_hbm,
    material_hbm,
    pinned_hbm,
    stiffness,
    out,
    start_v,
    inertial_v,
    material_v,
    pinned_v,
    in_sems,
    ulat,
    wflat,
    iflat,
    pflat,
    rate,
    grads,
    corners,
    spread,
    *group_refs,
):
    pos = [lax.axis_index(a) for a in AXES]
    sizes = [lax.axis_size(a) for a in AXES]
    has = [{-1: p > 0, 0: True, 1: p < n - 1} for p, n in zip(pos, sizes)]
    loads = [
        pltpu.make_async_copy(src, dst, in_sems.at[i])
        for i, (src, dst) in enumerate(
            (
                (start_hbm, start_v),
                (inertial_hbm, inertial_v),
                (material_hbm, material_v),
                (pinned_hbm, pinned_v),
            )
        )
    ]
    for load in loads:
        load.start()
    nine = len(group_refs) // 3
    first = Group(HALO, group_refs[:nine])
    targets = Group(1, group_refs[nine : 2 * nine])
    second = Group(HALO, group_refs[2 * nine :])
    first.clear(has)
    targets.clear(has)

    barrier = pltpu.get_barrier_semaphore()
    for d in DIRS:

        def greet(d=d):
            pl.semaphore_signal(
                barrier,
                inc=1,
                device_id={a: p + e for a, p, e in zip(AXES, pos, d)},
                device_id_type=pl.DeviceIdType.MESH,
            )

        guarded(every([has[a][d[a]] for a in range(3)]), greet)

    for load in loads:
        load.wait()
    lane = lax.broadcasted_iota(jnp.int32, (BX, 128), 1)
    grid_y = lax.broadcasted_iota(jnp.int32, (BX, 128), 0) + pos[1] * BX
    grid_z = lane + pos[2] * 128
    inner = (grid_y < BX * sizes[1] - 1) & (grid_z < 128 * sizes[2] - 1)

    def pack(i, carry):
        pins = pinned_v[i] > 0
        goal = [inertial_v[c, i] * 0.25 for c in range(3)]
        disp = [jnp.where(pins, goal[c], start_v[c, i] * 0.25) for c in range(3)]
        kinds = material_v[i]
        weight = jnp.zeros((BX, 128), jnp.float32)
        for m in range(MATS):
            weight = jnp.where(kinds == m, stiffness[m] * 0.0625, weight)
        valid = inner & (pos[0] * BX + i < BX * sizes[0] - 1)
        first.put(i, disp + [jnp.where(valid, weight, 0.0)], lane)
        targets.put(i, goal + [jnp.where(pins, 1.0, 0.0)], lane)
        return carry

    lax.fori_loop(0, BX, pack, 0)
    sides = [1 + (p > 0).astype(jnp.int32) + (p < n - 1).astype(jnp.int32) for p, n in zip(pos, sizes)]
    pl.semaphore_wait(barrier, sides[0] * sides[1] * sides[2] - 1)
    first.send(pos, has)
    targets.send(pos, has)
    second.clear(has)

    u0, u1, u2 = (ulat.at[k] for k in range(3))
    first.wait_recv(pos, has)
    first.to_flat([u0.at[c] for c in range(3)] + [wflat])

    big = (0, 160, 8), (0, 144, 8), (13, 136, 8)
    small = (13, 136, 8), (13, 120, 8), (26, 104, 8)

    differences(u0, grads, *big[0])
    stresses(grads, wflat, corners, spread, *big[1])

    targets.wait_recv(pos, has)
    targets.to_flat([iflat.at[c] for c in range(3)] + [pflat])

    sums = grads.at[0]

    def layers(r):
        sums[pl.ds(r, 8), :] = wflat[pl.ds(r, 8), :] + wflat[pl.ds(r - SLAB, 8), :]

    loop(SLAB, 136, 8, layers)

    def rates(r):
        total = (earlier(sums, r, 8, lane, EZ + 1) + earlier(sums, r, 8, lane, EZ)) + (
            earlier(sums, r, 8, lane, 1) + sums[pl.ds(r, 8), :]
        )
        rate[pl.ds(r, 8), :] = jnp.where(
            pflat[pl.ds(r, 8), :] > 0.0, 0.0, relax / (1.0 + 3.0 * total)
        )

    loop(SLAB, 136, 8, rates)

    omega1 = 2.0 / (2.0 - radius * radius)
    omega2 = 4.0 / (4.0 - radius * radius * omega1)
    omega3 = 4.0 / (4.0 - radius * radius * omega2)

    update(u0, None, u1, iflat, rate, spread, None, *big[2])
    differences(u1, grads, *small[0])
    stresses(grads, wflat, corners, spread, *small[1])
    update(u1, u0, u2, iflat, rate, spread, omega1, *small[2])

    for i in range(BX):
        second.put(i, [own_tile(u2.at[c], HALO + i, lane) for c in range(3)], lane)
    second.send(pos, has)
    second.wait_recv(pos, has)
    second.to_flat([u2.at[c] for c in range(3)])

    differences(u2, grads, *big[0])
    stresses(grads, wflat, corners, spread, *big[1])
    update(u2, u1, u0, iflat, rate, spread, omega2, *big[2])
    differences(u0, grads, *small[0])
    stresses(grads, wflat, corners, spread, *small[1])
    update(u0, u2, u1, iflat, rate, spread, omega3, *small[2])

    for i in range(BX):
        for c in range(3):
            out[c, i] = 4.0 * own_tile(u1.at[c], HALO + i, lane)
    first.wait_send(pos, has)
    targets.wait_send(pos, has)
    second.wait_send(pos, has)


def per_device(start_disp, inertial, material, pinned, stiffness):
    f = jnp.float32
    flat = (ROWS, 128)
    hbm = pl.BlockSpec(memory_space=pl.ANY)
    return pl.pallas_call(
        kernel,
        out_shape=jax.ShapeDtypeStruct(start_disp.shape, f),
        in_specs=[hbm, hbm, hbm, hbm, pl.BlockSpec(memory_space=pltpu.SMEM)],
        out_specs=pl.BlockSpec(memory_space=pltpu.VMEM),
        scratch_shapes=[
            pltpu.VMEM(start_disp.shape, f),
            pltpu.VMEM(inertial.shape, f),
            pltpu.VMEM(material.shape, jnp.int32),
            pltpu.VMEM(pinned.shape, jnp.int32),
            pltpu.SemaphoreType.DMA((4,)),
            pltpu.VMEM((3, 3, *flat), f),
            pltpu.VMEM(flat, f),
            pltpu.VMEM((3, *flat), f),
            pltpu.VMEM(flat, f),
            pltpu.VMEM(flat, f),
            pltpu.VMEM((9, *flat), f),
            pltpu.VMEM((12, *flat), f),
            pltpu.VMEM((12, *flat), f),
            *Group.scratch(HALO, 4),
            *Group.scratch(1, 4),
            *Group.scratch(HALO, 3),
        ],
        compiler_params=pltpu.CompilerParams(collective_id=0, has_side_effects=True),
    )(start_disp, inertial, material, pinned, stiffness)


def solution(mesh):
    placed = (
        P(None, "gx", "gy", "gz"),
        P(None, "gx", "gy", "gz"),
        P("gx", "gy", "gz"),
        P("gx", "gy", "gz"),
        P(),
    )
    return jax.shard_map(
        per_device, mesh=mesh, in_specs=placed, out_specs=P(None, "gx", "gy", "gz"), check_vma=False
    )
```

```python
import functools

import jax
import jax.numpy as jnp
from jax import lax
from jax.experimental import pallas as pl
from jax.experimental.pallas import tpu as pltpu
from jax.sharding import PartitionSpec as P

ITERS = 4
POLAR_STEPS = 6
MATS = 8

relax = 0.6
radius = 0.9

AXES = ("gx", "gy", "gz")
BX = 8
HALO = 2
EX = BX + 2 * HALO
EZ = 128 + 2 * HALO
SLAB = 13
ROWS = 176
VOFF = 16
ROLLED = 20
DIRS = [
    (dx, dy, dz)
    for dx in (-1, 0, 1)
    for dy in (-1, 0, 1)
    for dz in (-1, 0, 1)
    if (dx, dy, dz) != (0, 0, 0)
]


def every(conds):
    conds = [c for c in conds if c is not True]
    return functools.reduce(lambda p, q: p & q, conds) if conds else True


def guarded(cond, act):
    if cond is True:
        act()
    else:
        pl.when(cond)(act)


class Group:
    def __init__(self, width, refs):
        self.h = width
        self.ro, self.ry, self.sy, self.szo, self.szy, self.zo, self.zy, self.ssem, self.rsem = refs
        self.count = self.ro.shape[0]

    @staticmethod
    def scratch(width, count):
        f = jnp.float32
        return [
            pltpu.VMEM((count, EX, BX, 128), f),
            pltpu.VMEM((count, EX, 2, width, 128), f),
            pltpu.VMEM((count, BX, 2, width, 128), f),
            pltpu.VMEM((BX, BX, 128), f),
            pltpu.VMEM((BX, 2, width, 128), f),
            pltpu.VMEM((2, EX, BX, 128), f),
            pltpu.VMEM((2, EX, 2, width, 128), f),
            pltpu.SemaphoreType.DMA((len(DIRS),)),
            pltpu.SemaphoreType.DMA((len(DIRS),)),
        ]

    def copy(self, index, pos):
        dx, dy, dz = DIRS[index]
        h = self.h
        src_x = {-1: (0, h), 0: (0, BX), 1: (BX - h, h)}[dx]
        dst_x = {-1: (HALO + BX, h), 0: (HALO, BX), 1: (HALO - h, h)}[dx]
        src_side, dst_side = {-1: (0, 1), 0: (0, 0), 1: (1, 0)}[dy]
        zside = 0 if dz == 1 else 1
        sx, tx = pl.ds(*src_x), pl.ds(*dst_x)
        if dz == 0:
            if dy == 0:
                src = self.ro.at[:, pl.ds(HALO + src_x[0], src_x[1])]
                dst = self.ro.at[:, tx]
            else:
                src, dst = self.sy.at[:, sx, src_side], self.ry.at[:, tx, dst_side]
        elif dy == 0:
            src, dst = self.szo.at[sx], self.zo.at[zside, tx]
        else:
            src, dst = self.szy.at[sx, src_side], self.zy.at[zside, tx, dst_side]
        return pltpu.make_async_remote_copy(
            src_ref=src,
            dst_ref=dst,
            send_sem=self.ssem.at[index],
            recv_sem=self.rsem.at[index],
            device_id={a: p + d for a, p, d in zip(AXES, pos, DIRS[index])},
            device_id_type=pl.DeviceIdType.MESH,
        )

    def put(self, i, tiles, lane):
        h = self.h
        pack = jnp.zeros_like(tiles[0])
        for c, tile in enumerate(tiles):
            self.ro[c, HALO + i] = tile
            self.sy[c, i, 0] = tile[0:h]
            self.sy[c, i, 1] = tile[BX - h : BX]
            low = pltpu.roll(tile, 4 * c, 1) if c else tile
            high = pltpu.roll(tile, 4 * c + 4, 1)
            inside = (lane >= 4 * c) & (lane < 4 * c + 2)
            pack = jnp.where(inside, low, pack)
            inside = (lane >= 4 * c + 2) & (lane < 4 * c + 4)
            pack = jnp.where(inside, high, pack)
        self.szo[i] = pack
        self.szy[i, 0] = pack[0:h]
        self.szy[i, 1] = pack[BX - h : BX]

    def clear(self, has):
        for d, (start, size) in ((-1, (0, HALO)), (1, (HALO + BX, HALO))):

            def clear_x(start=start, size=size):
                for x in range(start, start + size):
                    for c in range(self.count):
                        self.ro[c, x] = jnp.zeros((BX, 128), jnp.float32)
                        self.ry[c, x] = jnp.zeros(self.ry.shape[2:], jnp.float32)
                    for s in range(2):
                        self.zo[s, x] = jnp.zeros((BX, 128), jnp.float32)
                        self.zy[s, x] = jnp.zeros(self.zy.shape[2:], jnp.float32)

            pl.when(jnp.logical_not(has[0][d]))(clear_x)

            def clear_y(side=(0 if d == -1 else 1)):
                for x in range(EX):
                    for c in range(self.count):
                        self.ry[c, x, side] = jnp.zeros((self.h, 128), jnp.float32)
                    for s in range(2):
                        self.zy[s, x, side] = jnp.zeros((self.h, 128), jnp.float32)

            pl.when(jnp.logical_not(has[1][d]))(clear_y)

            def clear_z(side=(0 if d == -1 else 1)):
                for x in range(EX):
                    self.zo[side, x] = jnp.zeros((BX, 128), jnp.float32)
                    self.zy[side, x] = jnp.zeros(self.zy.shape[2:], jnp.float32)

            pl.when(jnp.logical_not(has[2][d]))(clear_z)

    def send(self, pos, has):
        for index, d in enumerate(DIRS):
            guarded(every([has[a][d[a]] for a in range(3)]), self.copy(index, pos).start)

    def wait_recv(self, pos, has):
        for index, d in enumerate(DIRS):
            guarded(every([has[a][-d[a]] for a in range(3)]), self.copy(index, pos).wait_recv)

    def wait_send(self, pos, has):
        for index, d in enumerate(DIRS):
            guarded(every([has[a][d[a]] for a in range(3)]), self.copy(index, pos).wait_send)

    def to_flat(self, targets):
        h = self.h
        count = self.count
        for part in range(2):
            rows = BX if part == 0 else 2 * h
            lane = lax.broadcasted_iota(jnp.int32, (rows, 128), 1)
            main, zs = (self.ro, self.zo) if part == 0 else (self.ry, self.zy)
            zero = jnp.zeros((rows, 128), jnp.float32)
            before = [zero] * count
            high = zero
            for place in range(SLAB):
                last = place == SLAB - 1
                low = zero if last else zs[0, place].reshape(rows, 128)
                both = jnp.where((lane & 3) < 2, high, low)
                if not last:
                    high = zs[1, place].reshape(rows, 128)
                for c in range(count):
                    now = (
                        zero
                        if last
                        else pltpu.roll(main[c, place].reshape(rows, 128), 4 * place + 2, 1)
                    )
                    ends = pltpu.roll(both, (4 * place - 2 - 4 * c) % 128, 1)
                    flat = jnp.where(
                        lane >= 4 * place + 2,
                        now,
                        jnp.where(lane < 4 * place - 2, before[c], ends),
                    )
                    before[c] = now
                    out = targets[c]
                    if part == 0:
                        out[pl.ds(HALO * SLAB + place, BX, stride=SLAB), :] = flat
                    elif h == 1:
                        out[pl.ds(SLAB + place, 2, stride=9 * SLAB), :] = flat
                    else:
                        out[pl.ds(place, 2, stride=SLAB), :] = flat[0:2]
                        out[pl.ds(10 * SLAB + place, 2, stride=SLAB), :] = flat[2:4]


def own_tile(flat, place, lane):
    start = HALO * SLAB + place
    shift = 4 * place + 2
    first = flat[pl.ds(start, BX, stride=SLAB), :]
    second = flat[pl.ds(start + 1, BX, stride=SLAB), :]
    return pltpu.roll(jnp.where(lane >= shift, first, second), 128 - shift, 1)


def loop(start, rows, step, body, unroll=1):
    blocks = -(-rows // step)
    unroll = min(unroll, blocks)

    def trip(t, carry):
        for k in range(unroll):
            body(start + t * (unroll * step) + k * step)
        return carry

    trips = blocks // unroll
    if trips > 1:
        lax.fori_loop(0, trips, trip, 0)
    else:
        trip(0, 0)
    for k in range(trips * unroll, blocks):
        body(start + k * step)


def after(ref, row, n, lane, shift):
    whole, part = divmod(shift, 128)
    near = ref[pl.ds(row + whole, n), :]
    far = ref[pl.ds(row + whole + 1, n), :]
    return pltpu.roll(jnp.where(lane < part, far, near), 128 - part, 1)


def earlier(ref, row, n, lane, shift):
    whole, part = divmod(shift, 128)
    near = ref[pl.ds(row - whole, n), :]
    far = ref[pl.ds(row - whole - 1, n), :]
    return pltpu.roll(jnp.where(lane >= 128 - part, far, near), part, 1)


def differences(u, grads, start, rows, n):
    lane = lax.broadcasted_iota(jnp.int32, (n, 128), 1)

    def body(r):
        for c in range(3):
            ref = u.at[c]
            a00 = ref[pl.ds(r, n), :]
            a01 = after(ref, r, n, lane, 1)
            a10 = after(ref, r, n, lane, EZ)
            a11 = after(ref, r, n, lane, EZ + 1)
            s0, s1 = a00 + a01, a10 + a11
            grads[3 * c, pl.ds(r, n), :] = s1 - s0
            grads[3 * c + 1, pl.ds(r, n), :] = s0 + s1
            grads[3 * c + 2, pl.ds(r, n), :] = (a01 - a00) + (a11 - a10)

    loop(start, rows, n, body, ROLLED)


def stresses(grads, weights, corners, spread, start, rows, n):
    def body(r):
        def at(k, row):
            return grads[k, pl.ds(row, n), :]

        deform = []
        for c in range(3):
            fx = at(3 * c, r) + at(3 * c, r + SLAB)
            fy = at(3 * c + 1, r + SLAB) - at(3 * c + 1, r)
            fz = at(3 * c + 2, r) + at(3 * c + 2, r + SLAB)
            deform.append([fx, fy, fz])
        for c in range(3):
            deform[c][c] = deform[c][c] + 1.0
        rows_sq = [
            deform[c][0] * deform[c][0] + deform[c][1] * deform[c][1] + deform[c][2] * deform[c][2]
            for c in range(3)
        ]
        total = rows_sq[0] + rows_sq[1] + rows_sq[2]
        scale = jnp.minimum(lax.rsqrt(total * (2.0 / 3.0)), 0.5**0.5)
        y = [[deform[c][d] * scale for d in range(3)] for c in range(3)]
        weight = weights[pl.ds(r, n), :]
        heavy = weight * 2.0**0.5
        for step in range(POLAR_STEPS):

            def gram(i, j):
                return y[0][i] * y[0][j] + y[1][i] * y[1][j] + y[2][i] * y[2][j]

            d0, d1, d2 = 1.5 - gram(0, 0), 1.5 - gram(1, 1), 1.5 - gram(2, 2)
            o01, o02, o12 = gram(0, 1), gram(0, 2), gram(1, 2)
            if step == POLAR_STEPS - 1:
                d0, d1, d2 = d0 * heavy, d1 * heavy, d2 * heavy
                o01, o02, o12 = o01 * heavy, o02 * heavy, o12 * heavy
            y = [
                [
                    y[c][0] * d0 - (y[c][1] * o01 + y[c][2] * o02),
                    y[c][1] * d1 - (y[c][0] * o01 + y[c][2] * o12),
                    y[c][2] * d2 - (y[c][0] * o02 + y[c][1] * o12),
                ]
                for c in range(3)
            ]
        for c in range(3):
            px, py, pz = (weight * deform[c][d] - y[c][d] for d in range(3))
            s, t = py + px, py - px
            parts = (s + pz, s - pz, t + pz, t - pz)
            for k in range(4):
                corners[4 * c + k, pl.ds(r + VOFF, n), :] = parts[k]
            for k in range(4):
                below = corners[4 * c + k, pl.ds(r + VOFF - SLAB, n), :]
                spread[4 * c + k, pl.ds(r, n), :] = below - parts[3 - k]

    loop(start, rows, n, body)


def update(u, prev, fresh, inertial, rate, spread, omega, start, rows, n):
    lane = lax.broadcasted_iota(jnp.int32, (n, 128), 1)

    def body(r):
        a = rate[pl.ds(r, n), :]
        for c in range(3):
            force = (
                earlier(spread.at[4 * c], r, n, lane, EZ + 1)
                + earlier(spread.at[4 * c + 1], r, n, lane, EZ)
            ) + (
                earlier(spread.at[4 * c + 2], r, n, lane, 1)
                + spread[4 * c + 3, pl.ds(r, n), :]
            )
            here = u[c, pl.ds(r, n), :]
            new = here - a * ((here - inertial[c, pl.ds(r, n), :]) + force)
            if omega is not None:
                old = prev[c, pl.ds(r, n), :]
                new = omega * (new - old) + old
            fresh[c, pl.ds(r, n), :] = new

    loop(start, rows, n, body, ROLLED)


def kernel(
    start_hbm,
    inertial_hbm,
    material_hbm,
    pinned_hbm,
    stiffness,
    out,
    start_v,
    inertial_v,
    material_v,
    pinned_v,
    in_sems,
    ulat,
    wflat,
    iflat,
    pflat,
    rate,
    grads,
    corners,
    spread,
    *group_refs,
):
    pos = [lax.axis_index(a) for a in AXES]
    sizes = [lax.axis_size(a) for a in AXES]
    has = [{-1: p > 0, 0: True, 1: p < n - 1} for p, n in zip(pos, sizes)]
    loads = [
        pltpu.make_async_copy(src, dst, in_sems.at[i])
        for i, (src, dst) in enumerate(
            (
                (start_hbm, start_v),
                (inertial_hbm, inertial_v),
                (material_hbm, material_v),
                (pinned_hbm, pinned_v),
            )
        )
    ]
    for load in loads:
        load.start()
    nine = len(group_refs) // 3
    first = Group(HALO, group_refs[:nine])
    targets = Group(1, group_refs[nine : 2 * nine])
    second = Group(HALO, group_refs[2 * nine :])
    first.clear(has)
    targets.clear(has)

    barrier = pltpu.get_barrier_semaphore()
    for d in DIRS:

        def greet(d=d):
            pl.semaphore_signal(
                barrier,
                inc=1,
                device_id={a: p + e for a, p, e in zip(AXES, pos, d)},
                device_id_type=pl.DeviceIdType.MESH,
            )

        guarded(every([has[a][d[a]] for a in range(3)]), greet)

    for load in loads:
        load.wait()
    lane = lax.broadcasted_iota(jnp.int32, (BX, 128), 1)
    grid_y = lax.broadcasted_iota(jnp.int32, (BX, 128), 0) + pos[1] * BX
    grid_z = lane + pos[2] * 128
    inner = (grid_y < BX * sizes[1] - 1) & (grid_z < 128 * sizes[2] - 1)

    def pack(i, carry):
        pins = pinned_v[i] > 0
        goal = [inertial_v[c, i] * 0.25 for c in range(3)]
        disp = [jnp.where(pins, goal[c], start_v[c, i] * 0.25) for c in range(3)]
        kinds = material_v[i]
        weight = jnp.zeros((BX, 128), jnp.float32)
        for m in range(MATS):
            weight = jnp.where(kinds == m, stiffness[m] * 0.0625, weight)
        valid = inner & (pos[0] * BX + i < BX * sizes[0] - 1)
        first.put(i, disp + [jnp.where(valid, weight, 0.0)], lane)
        targets.put(i, goal + [jnp.where(pins, 1.0, 0.0)], lane)
        return carry

    lax.fori_loop(0, BX, pack, 0)
    sides = [1 + (p > 0).astype(jnp.int32) + (p < n - 1).astype(jnp.int32) for p, n in zip(pos, sizes)]
    pl.semaphore_wait(barrier, sides[0] * sides[1] * sides[2] - 1)
    first.send(pos, has)
    targets.send(pos, has)
    second.clear(has)

    u0, u1, u2 = (ulat.at[k] for k in range(3))
    first.wait_recv(pos, has)
    first.to_flat([u0.at[c] for c in range(3)] + [wflat])

    big = (0, 160, 8), (0, 144, 8), (13, 136, 8)
    small = (13, 136, 8), (13, 120, 8), (26, 104, 8)

    differences(u0, grads, *big[0])
    stresses(grads, wflat, corners, spread, *big[1])

    targets.wait_recv(pos, has)
    targets.to_flat([iflat.at[c] for c in range(3)] + [pflat])

    sums = grads.at[0]

    def layers(r):
        sums[pl.ds(r, 8), :] = wflat[pl.ds(r, 8), :] + wflat[pl.ds(r - SLAB, 8), :]

    loop(SLAB, 136, 8, layers, ROLLED)

    def rates(r):
        total = (earlier(sums, r, 8, lane, EZ + 1) + earlier(sums, r, 8, lane, EZ)) + (
            earlier(sums, r, 8, lane, 1) + sums[pl.ds(r, 8), :]
        )
        rate[pl.ds(r, 8), :] = jnp.where(
            pflat[pl.ds(r, 8), :] > 0.0, 0.0, relax / (1.0 + 3.0 * total)
        )

    loop(SLAB, 136, 8, rates, ROLLED)

    omega1 = 2.0 / (2.0 - radius * radius)
    omega2 = 4.0 / (4.0 - radius * radius * omega1)
    omega3 = 4.0 / (4.0 - radius * radius * omega2)

    update(u0, None, u1, iflat, rate, spread, None, *big[2])
    differences(u1, grads, *small[0])
    stresses(grads, wflat, corners, spread, *small[1])
    update(u1, u0, u2, iflat, rate, spread, omega1, *small[2])

    for i in range(BX):
        second.put(i, [own_tile(u2.at[c], HALO + i, lane) for c in range(3)], lane)
    second.send(pos, has)
    second.wait_recv(pos, has)
    second.to_flat([u2.at[c] for c in range(3)])

    differences(u2, grads, *big[0])
    stresses(grads, wflat, corners, spread, *big[1])
    update(u2, u1, u0, iflat, rate, spread, omega2, *big[2])
    differences(u0, grads, *small[0])
    stresses(grads, wflat, corners, spread, *small[1])
    update(u0, u2, u1, iflat, rate, spread, omega3, *small[2])

    for i in range(BX):
        for c in range(3):
            out[c, i] = 4.0 * own_tile(u1.at[c], HALO + i, lane)
    first.wait_send(pos, has)
    targets.wait_send(pos, has)
    second.wait_send(pos, has)


def per_device(start_disp, inertial, material, pinned, stiffness):
    f = jnp.float32
    flat = (ROWS, 128)
    hbm = pl.BlockSpec(memory_space=pl.ANY)
    return pl.pallas_call(
        kernel,
        out_shape=jax.ShapeDtypeStruct(start_disp.shape, f),
        in_specs=[hbm, hbm, hbm, hbm, pl.BlockSpec(memory_space=pltpu.SMEM)],
        out_specs=pl.BlockSpec(memory_space=pltpu.VMEM),
        scratch_shapes=[
            pltpu.VMEM(start_disp.shape, f),
            pltpu.VMEM(inertial.shape, f),
            pltpu.VMEM(material.shape, jnp.int32),
            pltpu.VMEM(pinned.shape, jnp.int32),
            pltpu.SemaphoreType.DMA((4,)),
            pltpu.VMEM((3, 3, *flat), f),
            pltpu.VMEM(flat, f),
            pltpu.VMEM((3, *flat), f),
            pltpu.VMEM(flat, f),
            pltpu.VMEM(flat, f),
            pltpu.VMEM((9, *flat), f),
            pltpu.VMEM((12, *flat), f),
            pltpu.VMEM((12, *flat), f),
            *Group.scratch(HALO, 4),
            *Group.scratch(1, 4),
            *Group.scratch(HALO, 3),
        ],
        compiler_params=pltpu.CompilerParams(collective_id=0, has_side_effects=True),
    )(start_disp, inertial, material, pinned, stiffness)


def solution(mesh):
    placed = (
        P(None, "gx", "gy", "gz"),
        P(None, "gx", "gy", "gz"),
        P("gx", "gy", "gz"),
        P("gx", "gy", "gz"),
        P(),
    )
    return jax.shard_map(
        per_device, mesh=mesh, in_specs=placed, out_specs=P(None, "gx", "gy", "gz"), check_vma=False
    )
```

```python
import functools

import jax
import jax.numpy as jnp
from jax import lax
from jax.experimental import pallas as pl
from jax.experimental.pallas import tpu as pltpu
from jax.sharding import PartitionSpec as P

ITERS = 4
POLAR_STEPS = 6
MATS = 8

relax = 0.6
radius = 0.9

AXES = ("gx", "gy", "gz")
BX = 8
HALO = 2
EX = BX + 2 * HALO
EZ = 128 + 2 * HALO
SLAB = 13
ROWS = 176
VOFF = 16
ROLLED = 20
DIRS = [
    (dx, dy, dz)
    for dx in (-1, 0, 1)
    for dy in (-1, 0, 1)
    for dz in (-1, 0, 1)
    if (dx, dy, dz) != (0, 0, 0)
]


def every(conds):
    conds = [c for c in conds if c is not True]
    return functools.reduce(lambda p, q: p & q, conds) if conds else True


def guarded(cond, act):
    if cond is True:
        act()
    else:
        pl.when(cond)(act)


class Group:
    def __init__(self, width, refs):
        self.h = width
        self.ro, self.ry, self.sy, self.szo, self.szy, self.zo, self.zy, self.ssem, self.rsem = refs
        self.count = self.ro.shape[0]

    @staticmethod
    def scratch(width, count):
        f = jnp.float32
        return [
            pltpu.VMEM((count, EX, BX, 128), f),
            pltpu.VMEM((count, EX, 2, width, 128), f),
            pltpu.VMEM((count, BX, 2, width, 128), f),
            pltpu.VMEM((BX, 128), f),
            pltpu.VMEM((2, width, 128), f),
            pltpu.VMEM((2, 3, BX, 128), f),
            pltpu.VMEM((2, 3, 2, width, 128), f),
            pltpu.SemaphoreType.DMA((len(DIRS),)),
            pltpu.SemaphoreType.DMA((len(DIRS),)),
        ]

    def copy(self, index, pos):
        dx, dy, dz = DIRS[index]
        h = self.h
        src_x = {-1: (0, h), 0: (0, BX), 1: (BX - h, h)}[dx]
        dst_x = {-1: (HALO + BX, h), 0: (HALO, BX), 1: (HALO - h, h)}[dx]
        src_side, dst_side = {-1: (0, 1), 0: (0, 0), 1: (1, 0)}[dy]
        zside = 0 if dz == 1 else 1
        slot = 1 - dx
        sx, tx = pl.ds(*src_x), pl.ds(*dst_x)
        if dz == 0:
            if dy == 0:
                src = self.ro.at[:, pl.ds(HALO + src_x[0], src_x[1])]
                dst = self.ro.at[:, tx]
            else:
                src, dst = self.sy.at[:, sx, src_side], self.ry.at[:, tx, dst_side]
        elif dy == 0:
            src, dst = self.szo, self.zo.at[zside, slot]
        else:
            src, dst = self.szy.at[src_side], self.zy.at[zside, slot, dst_side]
        return pltpu.make_async_remote_copy(
            src_ref=src,
            dst_ref=dst,
            send_sem=self.ssem.at[index],
            recv_sem=self.rsem.at[index],
            device_id={a: p + d for a, p, d in zip(AXES, pos, DIRS[index])},
            device_id_type=pl.DeviceIdType.MESH,
        )

    def put(self, i, tiles, pair, pack):
        h = self.h
        for c, tile in enumerate(tiles):
            self.ro[c, HALO + i] = tile
            self.sy[c, i, 0] = tile[0:h]
            self.sy[c, i, 1] = tile[BX - h : BX]
            low = 16 * ((i + 1) % BX) + 4 * c
            high = 16 * i + 4 * c + 2
            pack = jnp.where(pair == low // 2, pltpu.roll(tile, low, 1) if low else tile, pack)
            pack = jnp.where(pair == high // 2, pltpu.roll(tile, (high + 2) % 128, 1), pack)
        return pack

    def seal(self, pack):
        h = self.h
        self.szo[...] = pack
        self.szy[0] = pack[0:h]
        self.szy[1] = pack[BX - h : BX]

    def clear(self, has):
        h = self.h

        def zero(ref, index):
            ref[index] = jnp.zeros(ref.at[index].shape, jnp.float32)

        for d in (-1, 1):
            start = HALO + BX if d == 1 else HALO - h
            side = 0 if d == -1 else 1
            slot = 1 + d

            def clear_x(start=start, slot=slot):
                for c in range(self.count):
                    for x in range(start, start + h):
                        zero(self.ro, (c, x))
                        zero(self.ry, (c, x))
                for s in range(2):
                    zero(self.zo, (s, slot))
                    zero(self.zy, (s, slot))

            pl.when(jnp.logical_not(has[0][d]))(clear_x)

            def clear_y(side=side):
                for c in range(self.count):
                    for x in range(EX):
                        zero(self.ry, (c, x, side))
                for s in range(2):
                    for k in range(3):
                        zero(self.zy, (s, k, side))

            pl.when(jnp.logical_not(has[1][d]))(clear_y)

            def clear_z(side=side):
                for k in range(3):
                    zero(self.zo, (side, k))
                    zero(self.zy, (side, k))

            pl.when(jnp.logical_not(has[2][d]))(clear_z)

    def send(self, pos, has):
        for index, d in sorted(enumerate(DIRS), key=lambda e: e[1][1] == 0):
            guarded(every([has[a][d[a]] for a in range(3)]), self.copy(index, pos).start)

    def wait_recv(self, pos, has, edges):
        for index, d in enumerate(DIRS):
            if (d[1] != 0) == edges:
                guarded(every([has[a][-d[a]] for a in range(3)]), self.copy(index, pos).wait_recv)

    def wait_send(self, pos, has):
        for index, d in enumerate(DIRS):
            guarded(every([has[a][d[a]] for a in range(3)]), self.copy(index, pos).wait_send)

    def to_flat(self, targets, edges):
        h = self.h
        count = self.count
        rows = 2 * h if edges else BX
        lane = lax.broadcasted_iota(jnp.int32, (rows, 128), 1)
        main, zs = (self.ry, self.zy) if edges else (self.ro, self.zo)
        zero = jnp.zeros((rows, 128), jnp.float32)
        low_z, high_z = ([zs[s, k].reshape(rows, 128) for k in range(3)] for s in range(2))
        before = [zero] * count
        for place in range(SLAB):
            first, last = place == 0, place == SLAB - 1
            slot, before_slot = ((p >= HALO) + (p >= HALO + BX) for p in (place, place - 1))
            base = 16 * ((place - HALO) % BX)
            both = jnp.where(
                (lane & 3) < 2,
                zero if first else high_z[before_slot],
                zero if last else low_z[slot],
            )
            for c in range(count):
                now = (
                    zero
                    if last
                    else pltpu.roll(main[c, place].reshape(rows, 128), 4 * place + 2, 1)
                )
                ends = pltpu.roll(both, (4 * place - 2 - 4 * c - base) % 128, 1)
                flat = jnp.where(
                    lane >= 4 * place + 2,
                    now,
                    jnp.where(lane < 4 * place - 2, before[c], ends),
                )
                before[c] = now
                out = targets[c]
                if not edges:
                    out[pl.ds(HALO * SLAB + place, BX, stride=SLAB), :] = flat
                elif h == 1:
                    out[pl.ds(SLAB + place, 2, stride=9 * SLAB), :] = flat
                else:
                    out[pl.ds(place, 2, stride=SLAB), :] = flat[0:2]
                    out[pl.ds(10 * SLAB + place, 2, stride=SLAB), :] = flat[2:4]


def own_tile(flat, place, lane):
    start = HALO * SLAB + place
    shift = 4 * place + 2
    first = flat[pl.ds(start, BX, stride=SLAB), :]
    second = flat[pl.ds(start + 1, BX, stride=SLAB), :]
    return pltpu.roll(jnp.where(lane >= shift, first, second), 128 - shift, 1)


def loop(start, rows, step, body, unroll=1):
    blocks = -(-rows // step)
    unroll = min(unroll, blocks)

    def trip(t, carry):
        for k in range(unroll):
            body(start + t * (unroll * step) + k * step)
        return carry

    trips = blocks // unroll
    if trips > 1:
        lax.fori_loop(0, trips, trip, 0)
    else:
        trip(0, 0)
    for k in range(trips * unroll, blocks):
        body(start + k * step)


def after(ref, row, n, lane, shift):
    whole, part = divmod(shift, 128)
    near = ref[pl.ds(row + whole, n), :]
    far = ref[pl.ds(row + whole + 1, n), :]
    return pltpu.roll(jnp.where(lane < part, far, near), 128 - part, 1)


def earlier(ref, row, n, lane, shift):
    whole, part = divmod(shift, 128)
    near = ref[pl.ds(row - whole, n), :]
    far = ref[pl.ds(row - whole - 1, n), :]
    return pltpu.roll(jnp.where(lane >= 128 - part, far, near), part, 1)


def differences(u, grads, start, rows, n):
    lane = lax.broadcasted_iota(jnp.int32, (n, 128), 1)

    def body(r):
        for c in range(3):
            ref = u.at[c]
            a00 = ref[pl.ds(r, n), :]
            a01 = after(ref, r, n, lane, 1)
            a10 = after(ref, r, n, lane, EZ)
            a11 = after(ref, r, n, lane, EZ + 1)
            s0, s1 = a00 + a01, a10 + a11
            grads[3 * c, pl.ds(r, n), :] = s1 - s0
            grads[3 * c + 1, pl.ds(r, n), :] = s0 + s1
            grads[3 * c + 2, pl.ds(r, n), :] = (a01 - a00) + (a11 - a10)

    loop(start, rows, n, body, ROLLED)


def stresses(grads, weights, corners, spread, start, rows, n):
    def body(r):
        def at(k, row):
            return grads[k, pl.ds(row, n), :]

        deform = []
        for c in range(3):
            fx = at(3 * c, r) + at(3 * c, r + SLAB)
            fy = at(3 * c + 1, r + SLAB) - at(3 * c + 1, r)
            fz = at(3 * c + 2, r) + at(3 * c + 2, r + SLAB)
            deform.append([fx, fy, fz])
        for c in range(3):
            deform[c][c] = deform[c][c] + 1.0
        rows_sq = [
            deform[c][0] * deform[c][0] + deform[c][1] * deform[c][1] + deform[c][2] * deform[c][2]
            for c in range(3)
        ]
        total = rows_sq[0] + rows_sq[1] + rows_sq[2]
        scale = jnp.minimum(lax.rsqrt(total * (2.0 / 3.0)), 0.5**0.5)
        y = [[deform[c][d] * scale for d in range(3)] for c in range(3)]
        weight = weights[pl.ds(r, n), :]
        heavy = weight * 2.0**0.5
        for step in range(POLAR_STEPS):

            def gram(i, j):
                return y[0][i] * y[0][j] + y[1][i] * y[1][j] + y[2][i] * y[2][j]

            d0, d1, d2 = 1.5 - gram(0, 0), 1.5 - gram(1, 1), 1.5 - gram(2, 2)
            o01, o02, o12 = gram(0, 1), gram(0, 2), gram(1, 2)
            if step == POLAR_STEPS - 1:
                d0, d1, d2 = d0 * heavy, d1 * heavy, d2 * heavy
                o01, o02, o12 = o01 * heavy, o02 * heavy, o12 * heavy
            y = [
                [
                    y[c][0] * d0 - (y[c][1] * o01 + y[c][2] * o02),
                    y[c][1] * d1 - (y[c][0] * o01 + y[c][2] * o12),
                    y[c][2] * d2 - (y[c][0] * o02 + y[c][1] * o12),
                ]
                for c in range(3)
            ]
        for c in range(3):
            px, py, pz = (weight * deform[c][d] - y[c][d] for d in range(3))
            s, t = py + px, py - px
            parts = (s + pz, s - pz, t + pz, t - pz)
            for k in range(4):
                corners[4 * c + k, pl.ds(r + VOFF, n), :] = parts[k]
            for k in range(4):
                below = corners[4 * c + k, pl.ds(r + VOFF - SLAB, n), :]
                spread[4 * c + k, pl.ds(r, n), :] = below - parts[3 - k]

    loop(start, rows, n, body)


def respread(corners, spread, row):
    for c in range(3):
        for k in range(4):
            below = corners[4 * c + k, pl.ds(row + VOFF - SLAB, 8), :]
            spread[4 * c + k, pl.ds(row, 8), :] = below - corners[4 * c + 3 - k, pl.ds(row + VOFF, 8), :]


def update(u, prev, fresh, inertial, rate, spread, omega, start, rows, n):
    lane = lax.broadcasted_iota(jnp.int32, (n, 128), 1)

    def body(r):
        a = rate[pl.ds(r, n), :]
        for c in range(3):
            force = (
                earlier(spread.at[4 * c], r, n, lane, EZ + 1)
                + earlier(spread.at[4 * c + 1], r, n, lane, EZ)
            ) + (
                earlier(spread.at[4 * c + 2], r, n, lane, 1)
                + spread[4 * c + 3, pl.ds(r, n), :]
            )
            here = u[c, pl.ds(r, n), :]
            new = here - a * ((here - inertial[c, pl.ds(r, n), :]) + force)
            if omega is not None:
                old = prev[c, pl.ds(r, n), :]
                new = omega * (new - old) + old
            fresh[c, pl.ds(r, n), :] = new

    loop(start, rows, n, body, ROLLED)


def kernel(
    start_hbm,
    inertial_hbm,
    material_hbm,
    pinned_hbm,
    stiffness,
    out,
    start_v,
    inertial_v,
    material_v,
    pinned_v,
    in_sems,
    ulat,
    wflat,
    iflat,
    pflat,
    rate,
    grads,
    corners,
    spread,
    *group_refs,
):
    pos = [lax.axis_index(a) for a in AXES]
    sizes = [lax.axis_size(a) for a in AXES]
    has = [{-1: p > 0, 0: True, 1: p < n - 1} for p, n in zip(pos, sizes)]
    loads = [
        pltpu.make_async_copy(src, dst, in_sems.at[i])
        for i, (src, dst) in enumerate(
            (
                (start_hbm, start_v),
                (inertial_hbm, inertial_v),
                (material_hbm, material_v),
                (pinned_hbm, pinned_v),
            )
        )
    ]
    for load in loads:
        load.start()
    nine = len(group_refs) // 3
    first = Group(HALO, group_refs[:nine])
    targets = Group(1, group_refs[nine : 2 * nine])
    second = Group(HALO, group_refs[2 * nine :])
    barrier = pltpu.get_barrier_semaphore()
    for d in sorted(DIRS, key=lambda e: -sum(map(abs, e))):

        def greet(d=d):
            pl.semaphore_signal(
                barrier,
                inc=1,
                device_id={a: p + e for a, p, e in zip(AXES, pos, d)},
                device_id_type=pl.DeviceIdType.MESH,
            )

        guarded(every([has[a][d[a]] for a in range(3)]), greet)
    first.clear(has)
    targets.clear(has)

    for load in loads:
        load.wait()
    lane = lax.broadcasted_iota(jnp.int32, (BX, 128), 1)
    grid_y = lax.broadcasted_iota(jnp.int32, (BX, 128), 0) + pos[1] * BX
    grid_z = lane + pos[2] * 128
    inner = (grid_y < BX * sizes[1] - 1) & (grid_z < 128 * sizes[2] - 1)

    pair = lane >> 1
    zero = jnp.zeros((BX, 128), jnp.float32)
    packs = [zero, zero]
    for i in range(BX):
        pins = pinned_v[i] > 0
        goal = [inertial_v[c, i] * 0.25 for c in range(3)]
        disp = [jnp.where(pins, goal[c], start_v[c, i] * 0.25) for c in range(3)]
        kinds = material_v[i]
        weight = zero
        for m in range(MATS):
            weight = jnp.where(kinds == m, stiffness[m] * 0.0625, weight)
        valid = inner & (pos[0] * BX + i < BX * sizes[0] - 1)
        packs[0] = first.put(i, disp + [jnp.where(valid, weight, 0.0)], pair, packs[0])
        packs[1] = targets.put(i, goal + [jnp.where(pins, 1.0, 0.0)], pair, packs[1])
    first.seal(packs[0])
    targets.seal(packs[1])

    sides = [1 + (p > 0).astype(jnp.int32) + (p < n - 1).astype(jnp.int32) for p, n in zip(pos, sizes)]
    pl.semaphore_wait(barrier, sides[0] * sides[1] * sides[2] - 1)
    first.send(pos, has)
    targets.send(pos, has)
    second.clear(has)

    u0, u1, u2 = (ulat.at[k] for k in range(3))
    small = (13, 136, 8), (13, 120, 8), (26, 104, 8)
    firsts = [u0.at[c] for c in range(3)] + [wflat]
    goals = [iflat.at[c] for c in range(3)] + [pflat]

    def wide(group, targets, u):
        group.wait_recv(pos, has, False)
        group.to_flat(targets, False)
        differences(u, grads, 26, 104, 8)
        stresses(grads, wflat, corners, spread, 26, 88, 8)
        group.wait_recv(pos, has, True)
        group.to_flat(targets, True)
        differences(u, grads, 0, 32, 8)
        differences(u, grads, 130, 32, 8)
        stresses(grads, wflat, corners, spread, 0, 32, 8)
        stresses(grads, wflat, corners, spread, 114, 32, 8)
        respread(corners, spread, 32)

    wide(first, firsts, u0)
    for edges in (False, True):
        targets.wait_recv(pos, has, edges)
        targets.to_flat(goals, edges)

    sums = grads.at[0]

    def layers(r):
        sums[pl.ds(r, 8), :] = wflat[pl.ds(r, 8), :] + wflat[pl.ds(r - SLAB, 8), :]

    loop(SLAB, 136, 8, layers, ROLLED)

    def rates(r):
        total = (earlier(sums, r, 8, lane, EZ + 1) + earlier(sums, r, 8, lane, EZ)) + (
            earlier(sums, r, 8, lane, 1) + sums[pl.ds(r, 8), :]
        )
        rate[pl.ds(r, 8), :] = jnp.where(
            pflat[pl.ds(r, 8), :] > 0.0, 0.0, relax / (1.0 + 3.0 * total)
        )

    loop(SLAB, 136, 8, rates, ROLLED)

    omega1 = 2.0 / (2.0 - radius * radius)
    omega2 = 4.0 / (4.0 - radius * radius * omega1)
    omega3 = 4.0 / (4.0 - radius * radius * omega2)

    update(u0, None, u1, iflat, rate, spread, None, SLAB, 136, 8)
    differences(u1, grads, *small[0])
    stresses(grads, wflat, corners, spread, *small[1])
    update(u1, u0, u2, iflat, rate, spread, omega1, *small[2])

    pack = zero
    for i in range(BX):
        pack = second.put(i, [own_tile(u2.at[c], HALO + i, lane) for c in range(3)], pair, pack)
    second.seal(pack)
    second.send(pos, has)
    wide(second, [u2.at[c] for c in range(3)], u2)
    update(u2, u1, u0, iflat, rate, spread, omega2, SLAB, 136, 8)
    differences(u0, grads, *small[0])
    stresses(grads, wflat, corners, spread, *small[1])
    update(u0, u2, u1, iflat, rate, spread, omega3, *small[2])

    for i in range(BX):
        for c in range(3):
            out[c, i] = 4.0 * own_tile(u1.at[c], HALO + i, lane)
    first.wait_send(pos, has)
    targets.wait_send(pos, has)
    second.wait_send(pos, has)


def per_device(start_disp, inertial, material, pinned, stiffness):
    f = jnp.float32
    flat = (ROWS, 128)
    hbm = pl.BlockSpec(memory_space=pl.ANY)
    return pl.pallas_call(
        kernel,
        out_shape=jax.ShapeDtypeStruct(start_disp.shape, f),
        in_specs=[hbm, hbm, hbm, hbm, pl.BlockSpec(memory_space=pltpu.SMEM)],
        out_specs=pl.BlockSpec(memory_space=pltpu.VMEM),
        scratch_shapes=[
            pltpu.VMEM(start_disp.shape, f),
            pltpu.VMEM(inertial.shape, f),
            pltpu.VMEM(material.shape, jnp.int32),
            pltpu.VMEM(pinned.shape, jnp.int32),
            pltpu.SemaphoreType.DMA((4,)),
            pltpu.VMEM((3, 3, *flat), f),
            pltpu.VMEM(flat, f),
            pltpu.VMEM((3, *flat), f),
            pltpu.VMEM(flat, f),
            pltpu.VMEM(flat, f),
            pltpu.VMEM((9, *flat), f),
            pltpu.VMEM((12, *flat), f),
            pltpu.VMEM((12, *flat), f),
            *Group.scratch(HALO, 4),
            *Group.scratch(1, 4),
            *Group.scratch(HALO, 3),
        ],
        compiler_params=pltpu.CompilerParams(collective_id=0, has_side_effects=True),
    )(start_disp, inertial, material, pinned, stiffness)


def solution(mesh):
    placed = (
        P(None, "gx", "gy", "gz"),
        P(None, "gx", "gy", "gz"),
        P("gx", "gy", "gz"),
        P("gx", "gy", "gz"),
        P(),
    )
    return jax.shard_map(
        per_device, mesh=mesh, in_specs=placed, out_specs=P(None, "gx", "gy", "gz"), check_vma=False
    )
```

```python
import functools

import jax
import jax.numpy as jnp
from jax import lax
from jax.experimental import pallas as pl
from jax.experimental.pallas import tpu as pltpu
from jax.sharding import PartitionSpec as P

ITERS = 4
POLAR_STEPS = 6
MATS = 8

relax = 0.6
radius = 0.9

AXES = ("gx", "gy", "gz")
BX = 8
HALO = 2
EX = BX + 2 * HALO
HZ = 2 * HALO
EZ = 128 + 2 * HZ
SLAB = 13
ROWS = 176
VOFF = 16
ROLLED = 20
DIRS = [
    (dx, dy, dz)
    for dx in (-1, 0, 1)
    for dy in (-1, 0, 1)
    for dz in (-1, 0, 1)
    if (dx, dy, dz) != (0, 0, 0)
]


def every(conds):
    conds = [c for c in conds if c is not True]
    return functools.reduce(lambda p, q: p & q, conds) if conds else True


def guarded(cond, act):
    if cond is True:
        act()
    else:
        pl.when(cond)(act)


class Group:
    def __init__(self, width, dz, refs):
        self.h = width
        self.dz = dz
        self.ro, self.ry, self.sy, self.szo, self.szy, self.zo, self.zy, self.ssem, self.rsem = refs
        self.count = self.ro.shape[0]
        if dz:
            self.messages = list(DIRS)
        else:
            flat = [d for d in DIRS if d[2] == 0]
            self.messages = flat + [(*d[:2], None) for d in flat]

    @staticmethod
    def scratch(width, dz, count):
        f = jnp.float32
        sides = 2 if dz else 1
        total = len(DIRS) if dz else 16
        return [
            pltpu.VMEM((count, EX, BX, 128), f),
            pltpu.VMEM((count, EX, 2, width, 128), f),
            pltpu.VMEM((count, BX, 2, width, 128), f),
            pltpu.VMEM((2, BX, 128), f),
            pltpu.VMEM((2, 2, width, 128), f),
            pltpu.VMEM((sides, 3, 2, BX, 128), f),
            pltpu.VMEM((sides, 3, 2, 2, width, 128), f),
            pltpu.SemaphoreType.DMA((total,)),
            pltpu.SemaphoreType.DMA((total,)),
        ]

    def copy(self, index, pos):
        dx, dy, dz = self.messages[index]
        h = self.h
        src_x = {-1: (0, h), 0: (0, BX), 1: (BX - h, h)}[dx]
        dst_x = {-1: (HALO + BX, h), 0: (HALO, BX), 1: (HALO - h, h)}[dx]
        src_side, dst_side = {-1: (0, 1), 0: (0, 0), 1: (1, 0)}[dy]
        zside = 1 if dz == -1 else 0
        slot = 1 - dx
        sx, tx = pl.ds(*src_x), pl.ds(*dst_x)
        if dz == 0:
            if dy == 0:
                src = self.ro.at[:, pl.ds(HALO + src_x[0], src_x[1])]
                dst = self.ro.at[:, tx]
            else:
                src, dst = self.sy.at[:, sx, src_side], self.ry.at[:, tx, dst_side]
        elif dy == 0:
            src, dst = self.szo, self.zo.at[zside, slot]
        else:
            src, dst = self.szy.at[:, src_side], self.zy.at[zside, slot, :, dst_side]
        return pltpu.make_async_remote_copy(
            src_ref=src,
            dst_ref=dst,
            send_sem=self.ssem.at[index],
            recv_sem=self.rsem.at[index],
            device_id={a: p + d for a, p, d in zip(AXES, pos, (dx, dy, dz or 0))},
            device_id_type=pl.DeviceIdType.MESH,
        )

    def put(self, i, tiles):
        h = self.h
        for c, tile in enumerate(tiles):
            self.ro[c, HALO + i] = tile
            self.sy[c, i, 0] = tile[0:h]
            self.sy[c, i, 1] = tile[BX - h : BX]

    def seal(self, packs):
        h = self.h
        for k, pack in enumerate(packs):
            self.szo[k] = pack
            self.szy[k, 0] = pack[0:h]
            self.szy[k, 1] = pack[BX - h : BX]

    def clear(self, has):
        h = self.h
        zsides = self.zo.shape[0]

        def zero(ref, index):
            ref[index] = jnp.zeros(ref.at[index].shape, jnp.float32)

        for d in (-1, 1):
            start = HALO + BX if d == 1 else HALO - h
            side = 0 if d == -1 else 1
            slot = 1 + d

            def clear_x(start=start, slot=slot):
                for c in range(self.count):
                    for x in range(start, start + h):
                        zero(self.ro, (c, x))
                        zero(self.ry, (c, x))
                for s in range(zsides):
                    for k in range(2):
                        zero(self.zo, (s, slot, k))
                        zero(self.zy, (s, slot, k))

            pl.when(jnp.logical_not(has[0][d]))(clear_x)

            def clear_y(side=side):
                for c in range(self.count):
                    for x in range(EX):
                        zero(self.ry, (c, x, side))
                for s in range(zsides):
                    for slot in range(3):
                        for k in range(2):
                            zero(self.zy, (s, slot, k, side))

            pl.when(jnp.logical_not(has[1][d]))(clear_y)

            def clear_z(side=side):
                for slot in range(3):
                    for k in range(2):
                        zero(self.zo, (side, slot, k))
                        zero(self.zy, (side, slot, k))

            if self.dz:
                pl.when(jnp.logical_not(has[2][d]))(clear_z)

    def send(self, pos, has):
        for index, d in sorted(enumerate(self.messages), key=lambda e: e[1][1] == 0):
            guarded(every([has[a][d[a] or 0] for a in range(3)]), self.copy(index, pos).start)

    def wait_recv(self, pos, has, edges):
        for index, d in enumerate(self.messages):
            if (d[1] != 0) == edges:
                there = every([has[a][-(d[a] or 0)] for a in range(3)])
                guarded(there, self.copy(index, pos).wait_recv)

    def wait_send(self, pos, has):
        for index, d in enumerate(self.messages):
            guarded(every([has[a][d[a] or 0] for a in range(3)]), self.copy(index, pos).wait_send)

    def to_flat(self, targets, edges):
        h = self.h
        count = self.count
        rows = 2 * h if edges else BX
        lane = lax.broadcasted_iota(jnp.int32, (rows, 128), 1)
        main, zs = (self.ry, self.zy) if edges else (self.ro, self.zo)
        zero = jnp.zeros((rows, 128), jnp.float32)
        kept = not (edges or self.dz)
        before = [zero] * count
        for place in range(SLAB):
            if kept and HALO < place < HALO + BX:
                continue
            first, last = place == 0, place == SLAB - 1
            slot, before_slot = ((p >= HALO) + (p >= HALO + BX) for p in (place, place - 1))
            unit = (place - HALO) % BX

            def columns(side, slot):
                if kept and slot == 1:
                    return zero
                return zs[side, slot, unit // 4].reshape(rows, 128)

            both = jnp.where(
                (lane & 7) < HZ,
                zero if first else columns(zs.shape[0] - 1, before_slot),
                zero if last else columns(0, slot),
            )
            for c in range(count):
                if last or (kept and slot == 1):
                    now = zero
                else:
                    now = pltpu.roll(main[c, place].reshape(rows, 128), 8 * place + HZ, 1)
                ends = pltpu.roll(both, (8 * place - HZ - 32 * (unit % 4) - 8 * c) % 128, 1)
                flat = jnp.where(
                    lane >= 8 * place + HZ,
                    now,
                    jnp.where(lane < 8 * place - HZ, before[c], ends),
                )
                before[c] = now
                out = targets[c]
                if not edges:
                    span = pl.ds(HALO * SLAB + place, BX, stride=SLAB)
                    if kept and place == HALO:
                        flat = jnp.where(lane < 8 * place, flat, out[span, :])
                    if kept and place == HALO + BX:
                        flat = jnp.where(lane < 8 * place, out[span, :], flat)
                    out[span, :] = flat
                elif h == 1:
                    out[pl.ds(SLAB + place, 2, stride=9 * SLAB), :] = flat
                else:
                    out[pl.ds(place, 2, stride=SLAB), :] = flat[0:2]
                    out[pl.ds(10 * SLAB + place, 2, stride=SLAB), :] = flat[2:4]


def merge(packs, unit, field, half, tile, lane4, from_lane):
    to = 32 * (unit % 4) + 8 * field + 4 * half
    shift = (to - from_lane) % 128
    moved = pltpu.roll(tile, shift, 1) if shift else tile
    packs[unit // 4] = jnp.where(lane4 == to // 4, moved, packs[unit // 4])


def pack_block(packs, i, tiles, lane4):
    for c, tile in enumerate(tiles):
        merge(packs, (i + 1) % BX, c, 0, tile, lane4, 0)
        merge(packs, i, c, 1, tile, lane4, 128 - HZ)


def loop(start, rows, step, body, unroll=1):
    blocks = -(-rows // step)
    unroll = min(unroll, blocks)

    def trip(t, carry):
        for k in range(unroll):
            body(start + t * (unroll * step) + k * step)
        return carry

    trips = blocks // unroll
    if trips > 1:
        lax.fori_loop(0, trips, trip, 0)
    else:
        trip(0, 0)
    for k in range(trips * unroll, blocks):
        body(start + k * step)


def span(row, stride):
    return pl.ds(row, 8) if stride == 1 else pl.ds(row, 8, stride=stride)


def after(ref, row, stride, lane, shift):
    whole, part = divmod(shift, 128)
    near = ref[span(row + whole, stride), :]
    far = ref[span(row + whole + 1, stride), :]
    return pltpu.roll(jnp.where(lane < part, far, near), 128 - part, 1)


def earlier(get, row, lane, shift):
    whole, part = divmod(shift, 128)
    return pltpu.roll(jnp.where(lane >= 128 - part, get(row - whole - 1), get(row - whole)), part, 1)


def differences(u, grads, lane, row, stride=1):
    for c in range(3):
        ref = u.at[c]
        a00 = ref[span(row, stride), :]
        a01 = after(ref, row, stride, lane, 1)
        a10 = after(ref, row, stride, lane, EZ)
        a11 = after(ref, row, stride, lane, EZ + 1)
        s0, s1 = a00 + a01, a10 + a11
        grads[3 * c, span(row, stride), :] = s1 - s0
        grads[3 * c + 1, span(row, stride), :] = s0 + s1
        grads[3 * c + 2, span(row, stride), :] = (a01 - a00) + (a11 - a10)


def stresses(grads, weights, corners, row, stride=1):
    def at(k, r):
        return grads[k, span(r, stride), :]

    deform = []
    for c in range(3):
        fx = at(3 * c, row) + at(3 * c, row + SLAB)
        fy = at(3 * c + 1, row + SLAB) - at(3 * c + 1, row)
        fz = at(3 * c + 2, row) + at(3 * c + 2, row + SLAB)
        deform.append([fx, fy, fz])
    for c in range(3):
        deform[c][c] = deform[c][c] + 1.0
    rows_sq = [
        deform[c][0] * deform[c][0] + deform[c][1] * deform[c][1] + deform[c][2] * deform[c][2]
        for c in range(3)
    ]
    total = rows_sq[0] + rows_sq[1] + rows_sq[2]
    scale = jnp.minimum(lax.rsqrt(total * (2.0 / 3.0)), 0.5**0.5)
    y = [[deform[c][d] * scale for d in range(3)] for c in range(3)]
    weight = weights[span(row, stride), :]
    heavy = weight * 2.0**0.5
    for step in range(POLAR_STEPS):

        def gram(i, j):
            return y[0][i] * y[0][j] + y[1][i] * y[1][j] + y[2][i] * y[2][j]

        d0, d1, d2 = 1.5 - gram(0, 0), 1.5 - gram(1, 1), 1.5 - gram(2, 2)
        o01, o02, o12 = gram(0, 1), gram(0, 2), gram(1, 2)
        if step == POLAR_STEPS - 1:
            d0, d1, d2 = d0 * heavy, d1 * heavy, d2 * heavy
            o01, o02, o12 = o01 * heavy, o02 * heavy, o12 * heavy
        y = [
            [
                y[c][0] * d0 - (y[c][1] * o01 + y[c][2] * o02),
                y[c][1] * d1 - (y[c][0] * o01 + y[c][2] * o12),
                y[c][2] * d2 - (y[c][0] * o02 + y[c][1] * o12),
            ]
            for c in range(3)
        ]
    for c in range(3):
        px, py, pz = (weight * deform[c][d] - y[c][d] for d in range(3))
        s, t = py + px, py - px
        for k, part in enumerate((s + pz, s - pz, t + pz, t - pz)):
            corners[4 * c + k, span(row + VOFF, stride), :] = part


def update(state, u, prev, inertial, rate, corners, omega, lane, row, stride=1):
    seen = state.setdefault(stride, {})

    def spread(c, k):
        def get(r):
            if (c, k, r) not in seen:
                below = corners[4 * c + k, span(r + VOFF - SLAB, stride), :]
                seen[c, k, r] = below - corners[4 * c + 3 - k, span(r + VOFF, stride), :]
            return seen[c, k, r]

        return get

    a = rate[span(row, stride), :]
    result = []
    for c in range(3):
        force = (
            earlier(spread(c, 0), row, lane, EZ + 1) + earlier(spread(c, 1), row, lane, EZ)
        ) + (earlier(spread(c, 2), row, lane, 1) + spread(c, 3)(row))
        here = u[c, span(row, stride), :]
        new = here - a * ((here - inertial[c, span(row, stride), :]) + force)
        if omega is not None:
            old = prev[c, span(row, stride), :]
            new = omega * (new - old) + old
        result.append(new)
    return result


def kernel(
    start_hbm,
    inertial_hbm,
    material_hbm,
    pinned_hbm,
    stiffness,
    out,
    start_v,
    inertial_v,
    material_v,
    pinned_v,
    in_sems,
    ulat,
    wflat,
    iflat,
    pflat,
    rate,
    grads,
    corners,
    *group_refs,
):
    pos = [lax.axis_index(a) for a in AXES]
    sizes = [lax.axis_size(a) for a in AXES]
    has = [{-1: p > 0, 0: True, 1: p < n - 1} for p, n in zip(pos, sizes)]
    loads = [
        pltpu.make_async_copy(src, dst, in_sems.at[i])
        for i, (src, dst) in enumerate(
            (
                (start_hbm, start_v),
                (inertial_hbm, inertial_v),
                (material_hbm, material_v),
                (pinned_hbm, pinned_v),
            )
        )
    ]
    for load in loads:
        load.start()
    nine = len(group_refs) // 3
    first = Group(HALO, True, group_refs[:nine])
    targets = Group(1, True, group_refs[nine : 2 * nine])
    second = Group(HALO, False, group_refs[2 * nine :])
    barrier = pltpu.get_barrier_semaphore()
    for d in sorted(DIRS, key=lambda e: -sum(map(abs, e))):

        def greet(d=d):
            pl.semaphore_signal(
                barrier,
                inc=1,
                device_id={a: p + e for a, p, e in zip(AXES, pos, d)},
                device_id_type=pl.DeviceIdType.MESH,
            )

        guarded(every([has[a][d[a]] for a in range(3)]), greet)
    first.clear(has)
    targets.clear(has)

    for load in loads:
        load.wait()
    lane = lax.broadcasted_iota(jnp.int32, (BX, 128), 1)
    grid_y = lax.broadcasted_iota(jnp.int32, (BX, 128), 0) + pos[1] * BX
    grid_z = lane + pos[2] * 128
    inner = (grid_y < BX * sizes[1] - 1) & (grid_z < 128 * sizes[2] - 1)

    lane4 = lane >> 2
    zero = jnp.zeros((BX, 128), jnp.float32)
    packs = [[zero, zero], [zero, zero]]
    for i in range(BX):
        pins = pinned_v[i] > 0
        goal = [inertial_v[c, i] * 0.25 for c in range(3)]
        disp = [jnp.where(pins, goal[c], start_v[c, i] * 0.25) for c in range(3)]
        kinds = material_v[i]
        weight = zero
        for m in range(MATS):
            weight = jnp.where(kinds == m, stiffness[m] * 0.0625, weight)
        valid = inner & (pos[0] * BX + i < BX * sizes[0] - 1)
        fields = (disp + [jnp.where(valid, weight, 0.0)], goal + [jnp.where(pins, 1.0, 0.0)])
        for group, pack, tiles in zip((first, targets), packs, fields):
            group.put(i, tiles)
            pack_block(pack, i, tiles, lane4)
    first.seal(packs[0])
    targets.seal(packs[1])

    sides = [1 + (p > 0).astype(jnp.int32) + (p < n - 1).astype(jnp.int32) for p, n in zip(pos, sizes)]
    pl.semaphore_wait(barrier, sides[0] * sides[1] * sides[2] - 1)
    first.send(pos, has)
    targets.send(pos, has)
    second.clear(has)

    u0, u1, u2 = (ulat.at[k] for k in range(3))
    firsts = [u0.at[c] for c in range(3)] + [wflat]
    goals = [iflat.at[c] for c in range(3)] + [pflat]

    def wide(group, targets, u):
        def inside(t, carry):
            stresses(grads, wflat, corners, 26 + 8 * t)
            return carry

        def outside(t, carry):
            stresses(grads, wflat, corners, jnp.where(t < 4, 0, 82) + 8 * t)
            return carry

        group.wait_recv(pos, has, False)
        group.to_flat(targets, False)
        for r in range(26, 130, 8):
            differences(u, grads, lane, r)
        lax.fori_loop(0, 11, inside, 0)
        group.wait_recv(pos, has, True)
        group.to_flat(targets, True)
        for r in (*range(0, 32, 8), *range(130, 162, 8)):
            differences(u, grads, lane, r)
        lax.fori_loop(0, 8, outside, 0)

    def narrow(u):
        for r in range(1, 11):
            differences(u, grads, lane, SLAB + r, SLAB)
        for r in (9 * SLAB + 1, 9 * SLAB + 3, 10 * SLAB + 1, 10 * SLAB + 3):
            differences(u, grads, lane, r)

        def column(t, carry):
            stresses(grads, wflat, corners, SLAB + 1 + t, SLAB)
            return carry

        lax.fori_loop(0, 10, column, 0)
        for r in (9 * SLAB + 1, 9 * SLAB + 3):
            stresses(grads, wflat, corners, r)

    def update_wide(u, prev, fresh, omega):
        for r in range(SLAB, SLAB + 136, 8):
            new = update({}, u, prev, iflat, rate, corners, omega, lane, r)
            for c in range(3):
                fresh[c, pl.ds(r, 8), :] = new[c]

    def update_own(u, prev, omega):
        state = {}
        return [
            update(state, u, prev, iflat, rate, corners, omega, lane, HALO * SLAB + r, SLAB)
            for r in range(HALO, HALO + BX + 1)
        ]

    def own_tile(rows, i, c):
        shift = 8 * (HALO + i) + HZ
        return pltpu.roll(jnp.where(lane >= shift, rows[i][c], rows[i + 1][c]), 128 - shift, 1)

    wide(first, firsts, u0)
    for edges in (False, True):
        targets.wait_recv(pos, has, edges)
        targets.to_flat(goals, edges)

    sums = grads.at[0]
    for r in range(SLAB, SLAB + 136, 8):
        sums[pl.ds(r, 8), :] = wflat[pl.ds(r, 8), :] + wflat[pl.ds(r - SLAB, 8), :]
    for r in range(SLAB, SLAB + 136, 8):

        def get(row):
            return sums[pl.ds(row, 8), :]

        total = (earlier(get, r, lane, EZ + 1) + earlier(get, r, lane, EZ)) + (
            earlier(get, r, lane, 1) + get(r)
        )
        rate[pl.ds(r, 8), :] = jnp.where(
            pflat[pl.ds(r, 8), :] > 0.0, 0.0, relax / (1.0 + 3.0 * total)
        )

    omega1 = 2.0 / (2.0 - radius * radius)
    omega2 = 4.0 / (4.0 - radius * radius * omega1)
    omega3 = 4.0 / (4.0 - radius * radius * omega2)

    update_wide(u0, None, u1, None)
    narrow(u1)
    rows = update_own(u1, u0, omega1)
    pack = [zero, zero]
    for i in range(BX):
        second.put(i, [own_tile(rows, i, c) for c in range(3)])
    for i in range(BX + 1):
        place = HALO + i
        for c in range(3):
            if i > 0:
                merge(pack, i % BX, c, 0, rows[i][c], lane4, 8 * place - HZ)
            if i < BX:
                merge(pack, i, c, 1, rows[i][c], lane4, 8 * place)
    second.seal(pack)
    second.send(pos, has)
    for i in range(BX + 1):
        for c in range(3):
            u2[c, pl.ds(HALO * SLAB + HALO + i, BX, stride=SLAB), :] = rows[i][c]

    wide(second, [u2.at[c] for c in range(3)], u2)
    update_wide(u2, u1, u0, omega2)
    narrow(u0)
    rows = update_own(u0, u2, omega3)
    for i in range(BX):
        for c in range(3):
            out[c, i] = 4.0 * own_tile(rows, i, c)
    first.wait_send(pos, has)
    targets.wait_send(pos, has)
    second.wait_send(pos, has)


def per_device(start_disp, inertial, material, pinned, stiffness):
    f = jnp.float32
    flat = (ROWS, 128)
    hbm = pl.BlockSpec(memory_space=pl.ANY)
    return pl.pallas_call(
        kernel,
        out_shape=jax.ShapeDtypeStruct(start_disp.shape, f),
        in_specs=[hbm, hbm, hbm, hbm, pl.BlockSpec(memory_space=pltpu.SMEM)],
        out_specs=pl.BlockSpec(memory_space=pltpu.VMEM),
        scratch_shapes=[
            pltpu.VMEM(start_disp.shape, f),
            pltpu.VMEM(inertial.shape, f),
            pltpu.VMEM(material.shape, jnp.int32),
            pltpu.VMEM(pinned.shape, jnp.int32),
            pltpu.SemaphoreType.DMA((4,)),
            pltpu.VMEM((3, 3, *flat), f),
            pltpu.VMEM(flat, f),
            pltpu.VMEM((3, *flat), f),
            pltpu.VMEM(flat, f),
            pltpu.VMEM(flat, f),
            pltpu.VMEM((9, *flat), f),
            pltpu.VMEM((12, *flat), f),
            *Group.scratch(HALO, True, 4),
            *Group.scratch(1, True, 4),
            *Group.scratch(HALO, False, 3),
        ],
        compiler_params=pltpu.CompilerParams(
            collective_id=0, has_side_effects=True, vmem_limit_bytes=16 * 1024 * 1024
        ),
    )(start_disp, inertial, material, pinned, stiffness)


def solution(mesh):
    placed = (
        P(None, "gx", "gy", "gz"),
        P(None, "gx", "gy", "gz"),
        P("gx", "gy", "gz"),
        P("gx", "gy", "gz"),
        P(),
    )
    return jax.shard_map(
        per_device, mesh=mesh, in_specs=placed, out_specs=P(None, "gx", "gy", "gz"), check_vma=False
    )
```

```python
import functools

import jax
import jax.numpy as jnp
from jax import lax
from jax.experimental import pallas as pl
from jax.experimental.pallas import tpu as pltpu
from jax.sharding import PartitionSpec as P

ITERS = 4
POLAR_STEPS = 6
MATS = 8

relax = 0.6
radius = 0.9

AXES = ("gx", "gy", "gz")
BX = 8
HALO = 2
EX = BX + 2 * HALO
HZ = 2 * HALO
EZ = 128 + 2 * HZ
SLAB = 13
ROWS = 176
VOFF = 16
ROLLED = 20
DIRS = [
    (dx, dy, dz)
    for dx in (-1, 0, 1)
    for dy in (-1, 0, 1)
    for dz in (-1, 0, 1)
    if (dx, dy, dz) != (0, 0, 0)
]


def every(conds):
    conds = [c for c in conds if c is not True]
    return functools.reduce(lambda p, q: p & q, conds) if conds else True


def guarded(cond, act):
    if cond is True:
        act()
    else:
        pl.when(cond)(act)


class Group:
    def __init__(self, width, dz, refs):
        self.h = width
        self.dz = dz
        self.ro, self.ry, self.sy, self.szo, self.szy, self.zo, self.zy, self.ssem, self.rsem = refs
        self.count = self.ro.shape[0]
        if dz:
            self.messages = list(DIRS)
        else:
            flat = [d for d in DIRS if d[2] == 0]
            self.messages = flat + [(*d[:2], None) for d in flat]

    @staticmethod
    def scratch(width, dz, count):
        f = jnp.float32
        sides = 2 if dz else 1
        total = len(DIRS) if dz else 16
        return [
            pltpu.VMEM((count, EX, BX, 128), f),
            pltpu.VMEM((count, EX, 2, width, 128), f),
            pltpu.VMEM((count, BX, 2, width, 128), f),
            pltpu.VMEM((2, BX, 128), f),
            pltpu.VMEM((2, 2, width, 128), f),
            pltpu.VMEM((sides, 3, 2, BX, 128), f),
            pltpu.VMEM((sides, 3, 2, 2, width, 128), f),
            pltpu.SemaphoreType.DMA((total,)),
            pltpu.SemaphoreType.DMA((total,)),
        ]

    def copy(self, index, pos):
        dx, dy, dz = self.messages[index]
        h = self.h
        src_x = {-1: (0, h), 0: (0, BX), 1: (BX - h, h)}[dx]
        dst_x = {-1: (HALO + BX, h), 0: (HALO, BX), 1: (HALO - h, h)}[dx]
        src_side, dst_side = {-1: (0, 1), 0: (0, 0), 1: (1, 0)}[dy]
        zside = 1 if dz == -1 else 0
        slot = 1 - dx
        sx, tx = pl.ds(*src_x), pl.ds(*dst_x)
        if dz == 0:
            if dy == 0:
                src = self.ro.at[:, pl.ds(HALO + src_x[0], src_x[1])]
                dst = self.ro.at[:, tx]
            else:
                src, dst = self.sy.at[:, sx, src_side], self.ry.at[:, tx, dst_side]
        elif dy == 0:
            src, dst = self.szo, self.zo.at[zside, slot]
        else:
            src, dst = self.szy.at[:, src_side], self.zy.at[zside, slot, :, dst_side]
        return pltpu.make_async_remote_copy(
            src_ref=src,
            dst_ref=dst,
            send_sem=self.ssem.at[index],
            recv_sem=self.rsem.at[index],
            device_id={a: p + d for a, p, d in zip(AXES, pos, (dx, dy, dz or 0))},
            device_id_type=pl.DeviceIdType.MESH,
        )

    def put(self, i, tiles):
        h = self.h
        for c, tile in enumerate(tiles):
            self.ro[c, HALO + i] = tile
            self.sy[c, i, 0] = tile[0:h]
            self.sy[c, i, 1] = tile[BX - h : BX]

    def seal(self, packs):
        h = self.h
        for k, pack in enumerate(packs):
            self.szo[k] = pack
            self.szy[k, 0] = pack[0:h]
            self.szy[k, 1] = pack[BX - h : BX]

    def clear(self, has):
        h = self.h
        zsides = self.zo.shape[0]

        def zero(ref, index):
            ref[index] = jnp.zeros(ref.at[index].shape, jnp.float32)

        for d in (-1, 1):
            start = HALO + BX if d == 1 else HALO - h
            side = 0 if d == -1 else 1
            slot = 1 + d

            def clear_x(start=start, slot=slot):
                for c in range(self.count):
                    for x in range(start, start + h):
                        zero(self.ro, (c, x))
                        zero(self.ry, (c, x))
                for s in range(zsides):
                    for k in range(2):
                        zero(self.zo, (s, slot, k))
                        zero(self.zy, (s, slot, k))

            pl.when(jnp.logical_not(has[0][d]))(clear_x)

            def clear_y(side=side):
                for c in range(self.count):
                    for x in range(EX):
                        zero(self.ry, (c, x, side))
                for s in range(zsides):
                    for slot in range(3):
                        for k in range(2):
                            zero(self.zy, (s, slot, k, side))

            pl.when(jnp.logical_not(has[1][d]))(clear_y)

            def clear_z(side=side):
                for slot in range(3):
                    for k in range(2):
                        zero(self.zo, (side, slot, k))
                        zero(self.zy, (side, slot, k))

            if self.dz:
                pl.when(jnp.logical_not(has[2][d]))(clear_z)

    def send(self, pos, has):
        for index, d in sorted(enumerate(self.messages), key=lambda e: e[1][1] == 0):
            guarded(every([has[a][d[a] or 0] for a in range(3)]), self.copy(index, pos).start)

    def wait_recv(self, pos, has, edges):
        for index, d in enumerate(self.messages):
            if (d[1] != 0) == edges:
                there = every([has[a][-(d[a] or 0)] for a in range(3)])
                guarded(there, self.copy(index, pos).wait_recv)

    def wait_send(self, pos, has):
        for index, d in enumerate(self.messages):
            guarded(every([has[a][d[a] or 0] for a in range(3)]), self.copy(index, pos).wait_send)

    def to_flat(self, targets, edges):
        h = self.h
        count = self.count
        rows = 2 * h if edges else BX
        lane = lax.broadcasted_iota(jnp.int32, (rows, 128), 1)
        main, zs = (self.ry, self.zy) if edges else (self.ro, self.zo)
        zero = jnp.zeros((rows, 128), jnp.float32)
        kept = not (edges or self.dz)
        before = [zero] * count
        for place in range(SLAB):
            if kept and HALO < place < HALO + BX:
                continue
            first, last = place == 0, place == SLAB - 1
            slot, before_slot = ((p >= HALO) + (p >= HALO + BX) for p in (place, place - 1))
            unit = (place - HALO) % BX

            def columns(side, slot):
                if kept and slot == 1:
                    return zero
                return zs[side, slot, unit // 4].reshape(rows, 128)

            both = jnp.where(
                (lane & 7) < HZ,
                zero if first else columns(zs.shape[0] - 1, before_slot),
                zero if last else columns(0, slot),
            )
            for c in range(count):
                if last or (kept and slot == 1):
                    now = zero
                else:
                    now = pltpu.roll(main[c, place].reshape(rows, 128), 8 * place + HZ, 1)
                ends = pltpu.roll(both, (8 * place - HZ - 32 * (unit % 4) - 8 * c) % 128, 1)
                flat = jnp.where(
                    lane >= 8 * place + HZ,
                    now,
                    jnp.where(lane < 8 * place - HZ, before[c], ends),
                )
                before[c] = now
                out = targets[c]
                if not edges:
                    span = pl.ds(HALO * SLAB + place, BX, stride=SLAB)
                    if kept and place == HALO:
                        flat = jnp.where(lane < 8 * place, flat, out[span, :])
                    if kept and place == HALO + BX:
                        flat = jnp.where(lane < 8 * place, out[span, :], flat)
                    out[span, :] = flat
                elif h == 1:
                    out[pl.ds(SLAB + place, 2, stride=9 * SLAB), :] = flat
                else:
                    out[pl.ds(place, 2, stride=SLAB), :] = flat[0:2]
                    out[pl.ds(10 * SLAB + place, 2, stride=SLAB), :] = flat[2:4]


def merge(packs, unit, field, half, tile, lane4, from_lane):
    to = 32 * (unit % 4) + 8 * field + 4 * half
    shift = (to - from_lane) % 128
    moved = pltpu.roll(tile, shift, 1) if shift else tile
    packs[unit // 4] = jnp.where(lane4 == to // 4, moved, packs[unit // 4])


def pack_block(packs, i, tiles, lane4):
    for c, tile in enumerate(tiles):
        merge(packs, (i + 1) % BX, c, 0, tile, lane4, 0)
        merge(packs, i, c, 1, tile, lane4, 128 - HZ)


def loop(start, rows, step, body, unroll=1):
    blocks = -(-rows // step)
    unroll = min(unroll, blocks)

    def trip(t, carry):
        for k in range(unroll):
            body(start + t * (unroll * step) + k * step)
        return carry

    trips = blocks // unroll
    if trips > 1:
        lax.fori_loop(0, trips, trip, 0)
    else:
        trip(0, 0)
    for k in range(trips * unroll, blocks):
        body(start + k * step)


def span(row, stride):
    return pl.ds(row, 8) if stride == 1 else pl.ds(row, 8, stride=stride)


def after(ref, row, stride, lane, shift):
    whole, part = divmod(shift, 128)
    near = ref[span(row + whole, stride), :]
    far = ref[span(row + whole + 1, stride), :]
    return pltpu.roll(jnp.where(lane < part, far, near), 128 - part, 1)


def earlier(get, row, lane, shift):
    whole, part = divmod(shift, 128)
    return pltpu.roll(jnp.where(lane >= 128 - part, get(row - whole - 1), get(row - whole)), part, 1)


def differences(u, grads, lane, row, stride=1):
    for c in range(3):
        ref = u.at[c]
        a00 = ref[span(row, stride), :]
        a01 = after(ref, row, stride, lane, 1)
        a10 = after(ref, row, stride, lane, EZ)
        a11 = after(ref, row, stride, lane, EZ + 1)
        s0, s1 = a00 + a01, a10 + a11
        grads[3 * c, span(row, stride), :] = s1 - s0
        grads[3 * c + 1, span(row, stride), :] = s0 + s1
        grads[3 * c + 2, span(row, stride), :] = (a01 - a00) + (a11 - a10)


def stresses(grads, weights, corners, row, stride=1):
    def at(k, r):
        return grads[k, span(r, stride), :]

    deform = []
    for c in range(3):
        fx = at(3 * c, row) + at(3 * c, row + SLAB)
        fy = at(3 * c + 1, row + SLAB) - at(3 * c + 1, row)
        fz = at(3 * c + 2, row) + at(3 * c + 2, row + SLAB)
        deform.append([fx, fy, fz])
    for c in range(3):
        deform[c][c] = deform[c][c] + 1.0
    rows_sq = [
        deform[c][0] * deform[c][0] + deform[c][1] * deform[c][1] + deform[c][2] * deform[c][2]
        for c in range(3)
    ]
    total = rows_sq[0] + rows_sq[1] + rows_sq[2]
    scale = jnp.minimum(lax.rsqrt(total * (2.0 / 3.0)), 0.5**0.5)
    y = [[deform[c][d] * scale for d in range(3)] for c in range(3)]
    weight = weights[span(row, stride), :]
    heavy = weight * 2.0**0.5
    for step in range(POLAR_STEPS):

        def gram(i, j):
            return y[0][i] * y[0][j] + y[1][i] * y[1][j] + y[2][i] * y[2][j]

        d0, d1, d2 = 1.5 - gram(0, 0), 1.5 - gram(1, 1), 1.5 - gram(2, 2)
        o01, o02, o12 = gram(0, 1), gram(0, 2), gram(1, 2)
        if step == POLAR_STEPS - 1:
            d0, d1, d2 = d0 * heavy, d1 * heavy, d2 * heavy
            o01, o02, o12 = o01 * heavy, o02 * heavy, o12 * heavy
        y = [
            [
                y[c][0] * d0 - (y[c][1] * o01 + y[c][2] * o02),
                y[c][1] * d1 - (y[c][0] * o01 + y[c][2] * o12),
                y[c][2] * d2 - (y[c][0] * o02 + y[c][1] * o12),
            ]
            for c in range(3)
        ]
    for c in range(3):
        px, py, pz = (weight * deform[c][d] - y[c][d] for d in range(3))
        s, t = py + px, py - px
        for k, part in enumerate((s + pz, s - pz, t + pz, t - pz)):
            corners[4 * c + k, span(row + VOFF, stride), :] = part


def update(state, u, prev, inertial, rate, corners, omega, lane, row, stride=1):
    seen = state.setdefault(stride, {})

    def spread(c, k):
        def get(r):
            if (c, k, r) not in seen:
                below = corners[4 * c + k, span(r + VOFF - SLAB, stride), :]
                seen[c, k, r] = below - corners[4 * c + 3 - k, span(r + VOFF, stride), :]
            return seen[c, k, r]

        return get

    a = rate[span(row, stride), :]
    result = []
    for c in range(3):
        force = (
            earlier(spread(c, 0), row, lane, EZ + 1) + earlier(spread(c, 1), row, lane, EZ)
        ) + (earlier(spread(c, 2), row, lane, 1) + spread(c, 3)(row))
        here = u[c, span(row, stride), :]
        new = here - a * ((here - inertial[c, span(row, stride), :]) + force)
        if omega is not None:
            old = prev[c, span(row, stride), :]
            new = omega * (new - old) + old
        result.append(new)
    return result


def kernel(
    start_hbm,
    inertial_hbm,
    material_hbm,
    pinned_hbm,
    stiffness,
    out,
    start_v,
    inertial_v,
    material_v,
    pinned_v,
    in_sems,
    ulat,
    wflat,
    iflat,
    pflat,
    rate,
    grads,
    corners,
    *group_refs,
):
    pos = [lax.axis_index(a) for a in AXES]
    sizes = [lax.axis_size(a) for a in AXES]
    has = [{-1: p > 0, 0: True, 1: p < n - 1} for p, n in zip(pos, sizes)]
    loads = [
        pltpu.make_async_copy(src, dst, in_sems.at[i])
        for i, (src, dst) in enumerate(
            (
                (start_hbm, start_v),
                (inertial_hbm, inertial_v),
                (material_hbm, material_v),
                (pinned_hbm, pinned_v),
            )
        )
    ]
    for load in loads:
        load.start()
    nine = len(group_refs) // 3
    first = Group(HALO, True, group_refs[:nine])
    targets = Group(1, True, group_refs[nine : 2 * nine])
    second = Group(HALO, False, group_refs[2 * nine :])
    barrier = pltpu.get_barrier_semaphore()
    for d in sorted(DIRS, key=lambda e: -sum(map(abs, e))):

        def greet(d=d):
            pl.semaphore_signal(
                barrier,
                inc=1,
                device_id={a: p + e for a, p, e in zip(AXES, pos, d)},
                device_id_type=pl.DeviceIdType.MESH,
            )

        guarded(every([has[a][d[a]] for a in range(3)]), greet)
    first.clear(has)
    targets.clear(has)

    for load in loads:
        load.wait()
    lane = lax.broadcasted_iota(jnp.int32, (BX, 128), 1)
    grid_y = lax.broadcasted_iota(jnp.int32, (BX, 128), 0) + pos[1] * BX
    grid_z = lane + pos[2] * 128
    inner = (grid_y < BX * sizes[1] - 1) & (grid_z < 128 * sizes[2] - 1)

    lane4 = lane >> 2
    zero = jnp.zeros((BX, 128), jnp.float32)
    packs = [[zero, zero], [zero, zero]]
    for i in range(BX):
        pins = pinned_v[i] > 0
        goal = [inertial_v[c, i] * 0.25 for c in range(3)]
        disp = [jnp.where(pins, goal[c], start_v[c, i] * 0.25) for c in range(3)]
        kinds = material_v[i]
        weight = zero
        for m in range(MATS):
            weight = jnp.where(kinds == m, stiffness[m] * 0.0625, weight)
        valid = inner & (pos[0] * BX + i < BX * sizes[0] - 1)
        fields = (disp + [jnp.where(valid, weight, 0.0)], goal + [jnp.where(pins, 1.0, 0.0)])
        for group, pack, tiles in zip((first, targets), packs, fields):
            group.put(i, tiles)
            pack_block(pack, i, tiles, lane4)
    first.seal(packs[0])
    targets.seal(packs[1])

    sides = [1 + (p > 0).astype(jnp.int32) + (p < n - 1).astype(jnp.int32) for p, n in zip(pos, sizes)]
    pl.semaphore_wait(barrier, sides[0] * sides[1] * sides[2] - 1)
    first.send(pos, has)
    targets.send(pos, has)
    second.clear(has)

    u0, u1, u2 = (ulat.at[k] for k in range(3))
    firsts = [u0.at[c] for c in range(3)] + [wflat]
    goals = [iflat.at[c] for c in range(3)] + [pflat]

    def wide(group, targets, u):
        def inside(t, carry):
            stresses(grads, wflat, corners, 26 + 8 * t)
            return carry

        def outside(t, carry):
            stresses(grads, wflat, corners, jnp.where(t < 4, 0, 82) + 8 * t)
            return carry

        group.wait_recv(pos, has, False)
        group.to_flat(targets, False)
        for r in range(26, 130, 8):
            differences(u, grads, lane, r)
        lax.fori_loop(0, 11, inside, 0)
        group.wait_recv(pos, has, True)
        group.to_flat(targets, True)
        for r in (*range(0, 32, 8), *range(130, 162, 8)):
            differences(u, grads, lane, r)
        lax.fori_loop(0, 8, outside, 0)

    def narrow(u):
        for r in range(1, 11):
            differences(u, grads, lane, SLAB + r, SLAB)
        for r in (9 * SLAB + 1, 9 * SLAB + 3, 10 * SLAB + 1, 10 * SLAB + 3):
            differences(u, grads, lane, r)

        def column(t, carry):
            stresses(grads, wflat, corners, SLAB + 1 + t, SLAB)
            return carry

        lax.fori_loop(0, 10, column, 0)
        for r in (9 * SLAB + 1, 9 * SLAB + 3):
            stresses(grads, wflat, corners, r)

    def update_wide(u, prev, fresh, omega):
        for r in range(SLAB, SLAB + 136, 8):
            new = update({}, u, prev, iflat, rate, corners, omega, lane, r)
            for c in range(3):
                fresh[c, pl.ds(r, 8), :] = new[c]

    def update_own(u, prev, omega):
        state = {}
        return [
            update(state, u, prev, iflat, rate, corners, omega, lane, HALO * SLAB + r, SLAB)
            for r in range(HALO, HALO + BX + 1)
        ]

    def own_tile(rows, i, c):
        shift = 8 * (HALO + i) + HZ
        return pltpu.roll(jnp.where(lane >= shift, rows[i][c], rows[i + 1][c]), 128 - shift, 1)

    wide(first, firsts, u0)
    for edges in (False, True):
        targets.wait_recv(pos, has, edges)
        targets.to_flat(goals, edges)

    sums = grads.at[0]
    for r in range(SLAB, SLAB + 136, 8):
        sums[pl.ds(r, 8), :] = wflat[pl.ds(r, 8), :] + wflat[pl.ds(r - SLAB, 8), :]
    for r in range(SLAB, SLAB + 136, 8):

        def get(row):
            return sums[pl.ds(row, 8), :]

        total = (earlier(get, r, lane, EZ + 1) + earlier(get, r, lane, EZ)) + (
            earlier(get, r, lane, 1) + get(r)
        )
        rate[pl.ds(r, 8), :] = jnp.where(
            pflat[pl.ds(r, 8), :] > 0.0, 0.0, relax / (1.0 + 3.0 * total)
        )

    omega1 = 2.0 / (2.0 - radius * radius)
    omega2 = 4.0 / (4.0 - radius * radius * omega1)
    omega3 = 4.0 / (4.0 - radius * radius * omega2)

    update_wide(u0, None, u1, None)
    narrow(u1)
    rows = update_own(u1, u0, omega1)
    pack = [zero, zero]
    for i in range(BX):
        second.put(i, [own_tile(rows, i, c) for c in range(3)])
    for i in range(BX + 1):
        place = HALO + i
        for c in range(3):
            if i > 0:
                merge(pack, i % BX, c, 0, rows[i][c], lane4, 8 * place - HZ)
            if i < BX:
                merge(pack, i, c, 1, rows[i][c], lane4, 8 * place)
    second.seal(pack)
    second.send(pos, has)
    for i in range(BX + 1):
        for c in range(3):
            u2[c, pl.ds(HALO * SLAB + HALO + i, BX, stride=SLAB), :] = rows[i][c]

    wide(second, [u2.at[c] for c in range(3)], u2)
    update_wide(u2, u1, u0, omega2)
    narrow(u0)
    rows = update_own(u0, u2, omega3)
    for i in range(BX):
        for c in range(3):
            out[c, i] = 4.0 * own_tile(rows, i, c)
    first.wait_send(pos, has)
    targets.wait_send(pos, has)
    second.wait_send(pos, has)


def per_device(start_disp, inertial, material, pinned, stiffness):
    f = jnp.float32
    flat = (ROWS, 128)
    hbm = pl.BlockSpec(memory_space=pl.ANY)
    return pl.pallas_call(
        kernel,
        out_shape=jax.ShapeDtypeStruct(start_disp.shape, f),
        in_specs=[hbm, hbm, hbm, hbm, pl.BlockSpec(memory_space=pltpu.SMEM)],
        out_specs=pl.BlockSpec(memory_space=pltpu.VMEM),
        scratch_shapes=[
            pltpu.VMEM(start_disp.shape, f),
            pltpu.VMEM(inertial.shape, f),
            pltpu.VMEM(material.shape, jnp.int32),
            pltpu.VMEM(pinned.shape, jnp.int32),
            pltpu.SemaphoreType.DMA((4,)),
            pltpu.VMEM((3, 3, *flat), f),
            pltpu.VMEM(flat, f),
            pltpu.VMEM((3, *flat), f),
            pltpu.VMEM(flat, f),
            pltpu.VMEM(flat, f),
            pltpu.VMEM((9, *flat), f),
            pltpu.VMEM((12, *flat), f),
            *Group.scratch(HALO, True, 4),
            *Group.scratch(1, True, 4),
            *Group.scratch(HALO, False, 3),
        ],
        compiler_params=pltpu.CompilerParams(collective_id=0, has_side_effects=True),
    )(start_disp, inertial, material, pinned, stiffness)


def solution(mesh):
    placed = (
        P(None, "gx", "gy", "gz"),
        P(None, "gx", "gy", "gz"),
        P("gx", "gy", "gz"),
        P("gx", "gy", "gz"),
        P(),
    )
    return jax.shard_map(
        per_device, mesh=mesh, in_specs=placed, out_specs=P(None, "gx", "gy", "gz"), check_vma=False
    )
```

```python
import functools

import jax
import jax.numpy as jnp
from jax import lax
from jax.experimental import pallas as pl
from jax.experimental.pallas import tpu as pltpu
from jax.sharding import PartitionSpec as P

ITERS = 4
POLAR_STEPS = 6
MATS = 8

relax = 0.6
radius = 0.9

AXES = ("gx", "gy", "gz")
BX = 8
HALO = 2
EX = BX + 2 * HALO
HZ = 2 * HALO
EZ = 128 + 2 * HZ
SLAB = 13
ROWS = 176
VOFF = 16
TOGETHER = 2
DIRS = [
    (dx, dy, dz)
    for dx in (-1, 0, 1)
    for dy in (-1, 0, 1)
    for dz in (-1, 0, 1)
    if (dx, dy, dz) != (0, 0, 0)
]


def every(conds):
    conds = [c for c in conds if c is not True]
    return functools.reduce(lambda p, q: p & q, conds) if conds else True


def guarded(cond, act):
    if cond is True:
        act()
    else:
        pl.when(cond)(act)


class Group:
    def __init__(self, width, dz, refs):
        self.h = width
        self.dz = dz
        self.ro, self.ry, self.sy, self.szo, self.szy, self.zo, self.zy, self.ssem, self.rsem = refs
        self.count = self.ro.shape[0]
        if dz:
            self.messages = list(DIRS)
        else:
            flat = [d for d in DIRS if d[2] == 0]
            self.messages = flat + [(*d[:2], None) for d in flat]

    @staticmethod
    def scratch(width, dz, count):
        f = jnp.float32
        sides = 2 if dz else 1
        total = len(DIRS) if dz else 16
        return [
            pltpu.VMEM((count, EX, BX, 128), f),
            pltpu.VMEM((count, EX, 2, width, 128), f),
            pltpu.VMEM((count, BX, 2, width, 128), f),
            pltpu.VMEM((2, BX, 128), f),
            pltpu.VMEM((2, 2, width, 128), f),
            pltpu.VMEM((sides, 3, 2, BX, 128), f),
            pltpu.VMEM((sides, 3, 2, 2, width, 128), f),
            pltpu.SemaphoreType.DMA((total,)),
            pltpu.SemaphoreType.DMA((total,)),
        ]

    def copy(self, index, pos):
        dx, dy, dz = self.messages[index]
        h = self.h
        src_x = {-1: (0, h), 0: (0, BX), 1: (BX - h, h)}[dx]
        dst_x = {-1: (HALO + BX, h), 0: (HALO, BX), 1: (HALO - h, h)}[dx]
        src_side, dst_side = {-1: (0, 1), 0: (0, 0), 1: (1, 0)}[dy]
        zside = 1 if dz == -1 else 0
        slot = 1 - dx
        sx, tx = pl.ds(*src_x), pl.ds(*dst_x)
        if dz == 0:
            if dy == 0:
                src = self.ro.at[:, pl.ds(HALO + src_x[0], src_x[1])]
                dst = self.ro.at[:, tx]
            else:
                src, dst = self.sy.at[:, sx, src_side], self.ry.at[:, tx, dst_side]
        elif dy == 0:
            src, dst = self.szo, self.zo.at[zside, slot]
        else:
            src, dst = self.szy.at[:, src_side], self.zy.at[zside, slot, :, dst_side]
        return pltpu.make_async_remote_copy(
            src_ref=src,
            dst_ref=dst,
            send_sem=self.ssem.at[index],
            recv_sem=self.rsem.at[index],
            device_id={a: p + d for a, p, d in zip(AXES, pos, (dx, dy, dz or 0))},
            device_id_type=pl.DeviceIdType.MESH,
        )

    def put(self, i, tiles):
        h = self.h
        for c, tile in enumerate(tiles):
            self.ro[c, HALO + i] = tile
            self.sy[c, i, 0] = tile[0:h]
            self.sy[c, i, 1] = tile[BX - h : BX]

    def seal(self, packs):
        h = self.h
        for k, pack in enumerate(packs):
            self.szo[k] = pack
            self.szy[k, 0] = pack[0:h]
            self.szy[k, 1] = pack[BX - h : BX]

    def clear(self, has):
        h = self.h
        zsides = self.zo.shape[0]

        def zero(ref, index):
            ref[index] = jnp.zeros(ref.at[index].shape, jnp.float32)

        for d in (-1, 1):
            start = HALO + BX if d == 1 else HALO - h
            side = 0 if d == -1 else 1
            slot = 1 + d

            def clear_x(start=start, slot=slot):
                for c in range(self.count):
                    for x in range(start, start + h):
                        zero(self.ro, (c, x))
                        zero(self.ry, (c, x))
                for s in range(zsides):
                    for k in range(2):
                        zero(self.zo, (s, slot, k))
                        zero(self.zy, (s, slot, k))

            pl.when(jnp.logical_not(has[0][d]))(clear_x)

            def clear_y(side=side):
                for c in range(self.count):
                    for x in range(EX):
                        zero(self.ry, (c, x, side))
                for s in range(zsides):
                    for slot in range(3):
                        for k in range(2):
                            zero(self.zy, (s, slot, k, side))

            pl.when(jnp.logical_not(has[1][d]))(clear_y)

            def clear_z(side=side):
                for slot in range(3):
                    for k in range(2):
                        zero(self.zo, (side, slot, k))
                        zero(self.zy, (side, slot, k))

            if self.dz:
                pl.when(jnp.logical_not(has[2][d]))(clear_z)

    def send(self, pos, has):
        for index, d in sorted(enumerate(self.messages), key=lambda e: e[1][1] == 0):
            guarded(every([has[a][d[a] or 0] for a in range(3)]), self.copy(index, pos).start)

    def wait_recv(self, pos, has, edges):
        for index, d in enumerate(self.messages):
            if (d[1] != 0) == edges:
                there = every([has[a][-(d[a] or 0)] for a in range(3)])
                guarded(there, self.copy(index, pos).wait_recv)

    def wait_send(self, pos, has):
        for index, d in enumerate(self.messages):
            guarded(every([has[a][d[a] or 0] for a in range(3)]), self.copy(index, pos).wait_send)

    def to_flat(self, targets, edges):
        h = self.h
        count = self.count
        rows = 2 * h if edges else BX
        lane = lax.broadcasted_iota(jnp.int32, (rows, 128), 1)
        main, zs = (self.ry, self.zy) if edges else (self.ro, self.zo)
        zero = jnp.zeros((rows, 128), jnp.float32)
        kept = not (edges or self.dz)
        before = [zero] * count
        for place in range(SLAB):
            if kept and HALO < place < HALO + BX:
                continue
            first, last = place == 0, place == SLAB - 1
            slot, before_slot = ((p >= HALO) + (p >= HALO + BX) for p in (place, place - 1))
            unit = (place - HALO) % BX

            def columns(side, slot):
                if kept and slot == 1:
                    return zero
                return zs[side, slot, unit // 4].reshape(rows, 128)

            both = jnp.where(
                (lane & 7) < HZ,
                zero if first else columns(zs.shape[0] - 1, before_slot),
                zero if last else columns(0, slot),
            )
            for c in range(count):
                if last or (kept and slot == 1):
                    now = zero
                else:
                    now = pltpu.roll(main[c, place].reshape(rows, 128), 8 * place + HZ, 1)
                ends = pltpu.roll(both, (8 * place - HZ - 32 * (unit % 4) - 8 * c) % 128, 1)
                flat = jnp.where(
                    lane >= 8 * place + HZ,
                    now,
                    jnp.where(lane < 8 * place - HZ, before[c], ends),
                )
                before[c] = now
                out = targets[c]
                if not edges:
                    span = pl.ds(HALO * SLAB + place, BX, stride=SLAB)
                    if kept and place == HALO:
                        flat = jnp.where(lane < 8 * place, flat, out[span, :])
                    if kept and place == HALO + BX:
                        flat = jnp.where(lane < 8 * place, out[span, :], flat)
                    out[span, :] = flat
                elif h == 1:
                    out[pl.ds(SLAB + place, 2, stride=9 * SLAB), :] = flat
                else:
                    out[pl.ds(place, 2, stride=SLAB), :] = flat[0:2]
                    out[pl.ds(10 * SLAB + place, 2, stride=SLAB), :] = flat[2:4]


def merge(packs, unit, field, half, tile, lane4, from_lane):
    to = 32 * (unit % 4) + 8 * field + 4 * half
    shift = (to - from_lane) % 128
    moved = pltpu.roll(tile, shift, 1) if shift else tile
    packs[unit // 4] = jnp.where(lane4 == to // 4, moved, packs[unit // 4])


def pack_block(packs, i, tiles, lane4):
    for c, tile in enumerate(tiles):
        merge(packs, (i + 1) % BX, c, 0, tile, lane4, 0)
        merge(packs, i, c, 1, tile, lane4, 128 - HZ)


def loop(count, body):
    def trip(t, carry):
        for k in range(TOGETHER):
            body(t * TOGETHER + k)
        return carry

    lax.fori_loop(0, count // TOGETHER, trip, 0)
    for k in range(count - count % TOGETHER, count):
        body(k)


def span(row, stride):
    return pl.ds(row, 8) if stride == 1 else pl.ds(row, 8, stride=stride)


def after(ref, row, stride, lane, shift):
    whole, part = divmod(shift, 128)
    near = ref[span(row + whole, stride), :]
    far = ref[span(row + whole + 1, stride), :]
    return pltpu.roll(jnp.where(lane < part, far, near), 128 - part, 1)


def earlier(get, row, lane, shift):
    whole, part = divmod(shift, 128)
    return pltpu.roll(jnp.where(lane >= 128 - part, get(row - whole - 1), get(row - whole)), part, 1)


def differences(u, grads, lane, row, stride=1):
    for c in range(3):
        ref = u.at[c]
        a00 = ref[span(row, stride), :]
        a01 = after(ref, row, stride, lane, 1)
        a10 = after(ref, row, stride, lane, EZ)
        a11 = after(ref, row, stride, lane, EZ + 1)
        s0, s1 = a00 + a01, a10 + a11
        grads[3 * c, span(row, stride), :] = s1 - s0
        grads[3 * c + 1, span(row, stride), :] = s0 + s1
        grads[3 * c + 2, span(row, stride), :] = (a01 - a00) + (a11 - a10)


def stresses(grads, weights, corners, row, stride=1):
    def at(k, r):
        return grads[k, span(r, stride), :]

    deform = []
    for c in range(3):
        fx = at(3 * c, row) + at(3 * c, row + SLAB)
        fy = at(3 * c + 1, row + SLAB) - at(3 * c + 1, row)
        fz = at(3 * c + 2, row) + at(3 * c + 2, row + SLAB)
        deform.append([fx, fy, fz])
    for c in range(3):
        deform[c][c] = deform[c][c] + 1.0
    def dot(i, j):
        return deform[0][i] * deform[0][j] + deform[1][i] * deform[1][j] + deform[2][i] * deform[2][j]

    grams = [dot(0, 0), dot(1, 1), dot(2, 2)]
    total = grams[0] + grams[1] + grams[2]
    scale = jnp.minimum(lax.rsqrt(total * (1.0 / 3.0)), 1.0)
    half = scale * scale * 0.5
    mean = half * total * (1.0 / 3.0)
    d0, d1, d2 = (grams[k] * half - mean for k in range(3))
    d01, d02, d12 = dot(0, 1) * half, dot(0, 2) * half, dot(1, 2) * half
    sq01, sq02, sq12 = d01 * d01, d02 * d02, d12 * d12
    e0, e1, e2 = d0 * d0 + (sq01 + sq02), d1 * d1 + (sq01 + sq12), d2 * d2 + (sq02 + sq12)
    e01, e02, e12 = d02 * d12 - d2 * d01, d01 * d12 - d1 * d02, d01 * d02 - d0 * d12
    p = 0.5 * (e0 + e1 + e2)
    q = d0 * (d1 * d2 - sq12) + (d01 * e01 + d02 * e02)

    def reduced(c0, c1, c2, c3, c4):
        return c0 + q * c3, c1 + (p * c3 + q * c4), c2 + p * c4

    def times_linear(k, c):
        return k * c[0] + q * c[2], (k * c[1] + c[0]) + p * c[2], k * c[2] + c[1]

    low = mean - 1.5
    square = low * low
    t = mean * square + q, 2.0 * (mean * low) + (square + p), mean + 2.0 * low
    poly = times_linear(low, (t[0] - 1.5, t[1], t[2]))
    for step in range(2, POLAR_STEPS):
        c0, c1, c2 = poly
        twice0, twice1 = c0 + c0, c1 + c1
        square = reduced(c0 * c0, twice0 * c1, twice0 * c2 + c1 * c1, twice1 * c2, c2 * c2)
        t0, t1, t2 = times_linear(mean, square)
        t0 = t0 - 1.5
        poly = reduced(
            c0 * t0,
            c0 * t1 + c1 * t0,
            c0 * t2 + c1 * t1 + c2 * t0,
            c1 * t2 + c2 * t1,
            c2 * t2,
        )
    weight = weights[span(row, stride), :]
    heavy = weight * scale
    c0, c1, c2 = weight - heavy * poly[0], heavy * poly[1], heavy * poly[2]
    w0, w1, w2 = (c0 - (c1 * d + c2 * e) for d, e in ((d0, e0), (d1, e1), (d2, e2)))
    w01, w02, w12 = (c1 * d + c2 * e for d, e in ((d01, e01), (d02, e02), (d12, e12)))
    for c in range(3):
        fx, fy, fz = deform[c]
        px = fx * w0 - (fy * w01 + fz * w02)
        py = fy * w1 - (fx * w01 + fz * w12)
        pz = fz * w2 - (fx * w02 + fy * w12)
        s, t = py + px, py - px
        for k, part in enumerate((s + pz, s - pz, t + pz, t - pz)):
            corners[4 * c + k, span(row + VOFF, stride), :] = part


def update(state, u, prev, inertial, rate, corners, omega, lane, row, stride=1):
    seen = state.setdefault(stride, {})

    def spread(c, k):
        def get(r):
            if (c, k, r) not in seen:
                below = corners[4 * c + k, span(r + VOFF - SLAB, stride), :]
                seen[c, k, r] = below - corners[4 * c + 3 - k, span(r + VOFF, stride), :]
            return seen[c, k, r]

        return get

    a = rate[span(row, stride), :]
    result = []
    for c in range(3):
        force = (
            earlier(spread(c, 0), row, lane, EZ + 1) + earlier(spread(c, 1), row, lane, EZ)
        ) + (earlier(spread(c, 2), row, lane, 1) + spread(c, 3)(row))
        here = u[c, span(row, stride), :]
        new = here - a * ((here - inertial[c, span(row, stride), :]) + force)
        if omega is not None:
            old = prev[c, span(row, stride), :]
            new = omega * (new - old) + old
        result.append(new)
    return result


def kernel(
    start_hbm,
    inertial_hbm,
    material_hbm,
    pinned_hbm,
    stiffness,
    out,
    start_v,
    inertial_v,
    material_v,
    pinned_v,
    in_sems,
    ulat,
    wflat,
    iflat,
    pflat,
    rate,
    grads,
    corners,
    *group_refs,
):
    pos = [lax.axis_index(a) for a in AXES]
    sizes = [lax.axis_size(a) for a in AXES]
    has = [{-1: p > 0, 0: True, 1: p < n - 1} for p, n in zip(pos, sizes)]
    loads = [
        pltpu.make_async_copy(src, dst, in_sems.at[i])
        for i, (src, dst) in enumerate(
            (
                (start_hbm, start_v),
                (inertial_hbm, inertial_v),
                (material_hbm, material_v),
                (pinned_hbm, pinned_v),
            )
        )
    ]
    for load in loads:
        load.start()
    nine = len(group_refs) // 3
    first = Group(HALO, True, group_refs[:nine])
    targets = Group(1, True, group_refs[nine : 2 * nine])
    second = Group(HALO, False, group_refs[2 * nine :])
    barrier = pltpu.get_barrier_semaphore()
    for d in sorted(DIRS, key=lambda e: -sum(map(abs, e))):

        def greet(d=d):
            pl.semaphore_signal(
                barrier,
                inc=1,
                device_id={a: p + e for a, p, e in zip(AXES, pos, d)},
                device_id_type=pl.DeviceIdType.MESH,
            )

        guarded(every([has[a][d[a]] for a in range(3)]), greet)
    first.clear(has)
    targets.clear(has)

    for load in loads:
        load.wait()
    lane = lax.broadcasted_iota(jnp.int32, (BX, 128), 1)
    grid_y = lax.broadcasted_iota(jnp.int32, (BX, 128), 0) + pos[1] * BX
    grid_z = lane + pos[2] * 128
    inner = (grid_y < BX * sizes[1] - 1) & (grid_z < 128 * sizes[2] - 1)

    lane4 = lane >> 2
    zero = jnp.zeros((BX, 128), jnp.float32)
    packs = [[zero, zero], [zero, zero]]
    for i in range(BX):
        pins = pinned_v[i] > 0
        goal = [inertial_v[c, i] * 0.25 for c in range(3)]
        disp = [jnp.where(pins, goal[c], start_v[c, i] * 0.25) for c in range(3)]
        kinds = material_v[i]
        weight = zero
        for m in range(MATS):
            weight = jnp.where(kinds == m, stiffness[m] * 0.0625, weight)
        valid = inner & (pos[0] * BX + i < BX * sizes[0] - 1)
        fields = (disp + [jnp.where(valid, weight, 0.0)], goal + [jnp.where(pins, 1.0, 0.0)])
        for group, pack, tiles in zip((first, targets), packs, fields):
            group.put(i, tiles)
            pack_block(pack, i, tiles, lane4)
    first.seal(packs[0])
    targets.seal(packs[1])

    sides = [1 + (p > 0).astype(jnp.int32) + (p < n - 1).astype(jnp.int32) for p, n in zip(pos, sizes)]
    pl.semaphore_wait(barrier, sides[0] * sides[1] * sides[2] - 1)
    first.send(pos, has)
    targets.send(pos, has)
    second.clear(has)

    u0, u1, u2 = (ulat.at[k] for k in range(3))
    firsts = [u0.at[c] for c in range(3)] + [wflat]
    goals = [iflat.at[c] for c in range(3)] + [pflat]

    def wide(group, targets, u):
        def inside(t):
            stresses(grads, wflat, corners, 26 + 8 * t)

        def outside(t):
            stresses(grads, wflat, corners, jnp.where(t < 4, 0, 82) + 8 * t)

        group.wait_recv(pos, has, False)
        group.to_flat(targets, False)
        for r in range(26, 130, 8):
            differences(u, grads, lane, r)
        loop(12, inside)
        group.wait_recv(pos, has, True)
        group.to_flat(targets, True)
        for r in (*range(0, 32, 8), *range(130, 162, 8)):
            differences(u, grads, lane, r)
        loop(8, outside)

    def narrow(u):
        for r in range(1, 11):
            differences(u, grads, lane, SLAB + r, SLAB)
        for r in (9 * SLAB + 1, 9 * SLAB + 3, 10 * SLAB + 1, 10 * SLAB + 3):
            differences(u, grads, lane, r)

        def column(t):
            stresses(grads, wflat, corners, SLAB + 1 + t, SLAB)

        loop(10, column)
        for r in (9 * SLAB + 1, 9 * SLAB + 3):
            stresses(grads, wflat, corners, r)

    def update_wide(u, prev, fresh, omega):
        for r in range(SLAB, SLAB + 136, 8):
            new = update({}, u, prev, iflat, rate, corners, omega, lane, r)
            for c in range(3):
                fresh[c, pl.ds(r, 8), :] = new[c]

    def update_own(u, prev, omega):
        state = {}
        return [
            update(state, u, prev, iflat, rate, corners, omega, lane, HALO * SLAB + r, SLAB)
            for r in range(HALO, HALO + BX + 1)
        ]

    def own_tile(rows, i, c):
        shift = 8 * (HALO + i) + HZ
        return pltpu.roll(jnp.where(lane >= shift, rows[i][c], rows[i + 1][c]), 128 - shift, 1)

    wide(first, firsts, u0)
    for edges in (False, True):
        targets.wait_recv(pos, has, edges)
        targets.to_flat(goals, edges)

    sums = grads.at[0]
    for r in range(SLAB, SLAB + 136, 8):
        sums[pl.ds(r, 8), :] = wflat[pl.ds(r, 8), :] + wflat[pl.ds(r - SLAB, 8), :]
    for r in range(SLAB, SLAB + 136, 8):

        def get(row):
            return sums[pl.ds(row, 8), :]

        total = (earlier(get, r, lane, EZ + 1) + earlier(get, r, lane, EZ)) + (
            earlier(get, r, lane, 1) + get(r)
        )
        rate[pl.ds(r, 8), :] = jnp.where(
            pflat[pl.ds(r, 8), :] > 0.0, 0.0, relax / (1.0 + 3.0 * total)
        )

    omega1 = 2.0 / (2.0 - radius * radius)
    omega2 = 4.0 / (4.0 - radius * radius * omega1)
    omega3 = 4.0 / (4.0 - radius * radius * omega2)

    update_wide(u0, None, u1, None)
    narrow(u1)
    rows = update_own(u1, u0, omega1)
    pack = [zero, zero]
    for i in range(BX):
        second.put(i, [own_tile(rows, i, c) for c in range(3)])
    for i in range(BX + 1):
        place = HALO + i
        for c in range(3):
            if i > 0:
                merge(pack, i % BX, c, 0, rows[i][c], lane4, 8 * place - HZ)
            if i < BX:
                merge(pack, i, c, 1, rows[i][c], lane4, 8 * place)
    second.seal(pack)
    second.send(pos, has)
    for i in range(BX + 1):
        for c in range(3):
            u2[c, pl.ds(HALO * SLAB + HALO + i, BX, stride=SLAB), :] = rows[i][c]

    wide(second, [u2.at[c] for c in range(3)], u2)
    update_wide(u2, u1, u0, omega2)
    narrow(u0)
    rows = update_own(u0, u2, omega3)
    for i in range(BX):
        for c in range(3):
            out[c, i] = 4.0 * own_tile(rows, i, c)
    first.wait_send(pos, has)
    targets.wait_send(pos, has)
    second.wait_send(pos, has)


def per_device(start_disp, inertial, material, pinned, stiffness):
    f = jnp.float32
    flat = (ROWS, 128)
    hbm = pl.BlockSpec(memory_space=pl.ANY)
    return pl.pallas_call(
        kernel,
        out_shape=jax.ShapeDtypeStruct(start_disp.shape, f),
        in_specs=[hbm, hbm, hbm, hbm, pl.BlockSpec(memory_space=pltpu.SMEM)],
        out_specs=pl.BlockSpec(memory_space=pltpu.VMEM),
        scratch_shapes=[
            pltpu.VMEM(start_disp.shape, f),
            pltpu.VMEM(inertial.shape, f),
            pltpu.VMEM(material.shape, jnp.int32),
            pltpu.VMEM(pinned.shape, jnp.int32),
            pltpu.SemaphoreType.DMA((4,)),
            pltpu.VMEM((3, 3, *flat), f),
            pltpu.VMEM(flat, f),
            pltpu.VMEM((3, *flat), f),
            pltpu.VMEM(flat, f),
            pltpu.VMEM(flat, f),
            pltpu.VMEM((9, *flat), f),
            pltpu.VMEM((12, *flat), f),
            *Group.scratch(HALO, True, 4),
            *Group.scratch(1, True, 4),
            *Group.scratch(HALO, False, 3),
        ],
        compiler_params=pltpu.CompilerParams(collective_id=0, has_side_effects=True),
    )(start_disp, inertial, material, pinned, stiffness)


def solution(mesh):
    placed = (
        P(None, "gx", "gy", "gz"),
        P(None, "gx", "gy", "gz"),
        P("gx", "gy", "gz"),
        P("gx", "gy", "gz"),
        P(),
    )
    return jax.shard_map(
        per_device, mesh=mesh, in_specs=placed, out_specs=P(None, "gx", "gy", "gz"), check_vma=False
    )
```

```python
import functools

import jax
import jax.numpy as jnp
from jax import lax
from jax.experimental import pallas as pl
from jax.experimental.pallas import tpu as pltpu
from jax.sharding import PartitionSpec as P

ITERS = 4
POLAR_STEPS = 6
MATS = 8

relax = 0.6
radius = 0.9

AXES = ("gx", "gy", "gz")
BX = 8
HALO = 2
EX = BX + 2 * HALO
HZ = 2 * HALO
EZ = 128 + 2 * HZ
SLAB = 13
ROWS = 176
VOFF = 16
TOGETHER = 2
DIRS = [
    (dx, dy, dz)
    for dx in (-1, 0, 1)
    for dy in (-1, 0, 1)
    for dz in (-1, 0, 1)
    if (dx, dy, dz) != (0, 0, 0)
]


def every(conds):
    conds = [c for c in conds if c is not True]
    return functools.reduce(lambda p, q: p & q, conds) if conds else True


def guarded(cond, act):
    if cond is True:
        act()
    else:
        pl.when(cond)(act)


def zero(ref, index):
    ref[index] = jnp.zeros(ref.at[index].shape, jnp.float32)


class Group:
    fields = 4

    def __init__(self, width, refs):
        self.h = width
        self.ro, self.ry, self.sy, self.ssem, self.rsem, *self.extra = refs
        self.messages = [d for d in DIRS if d[2] == 0]

    @staticmethod
    def scratch(width, total, extra=()):
        f = jnp.float32
        return [
            pltpu.VMEM((4, EX, BX, 128), f),
            pltpu.VMEM((4, EX, 2, width, 128), f),
            pltpu.VMEM((4, BX, 2, width, 128), f),
            pltpu.SemaphoreType.DMA((total,)),
            pltpu.SemaphoreType.DMA((total,)),
            *(pltpu.VMEM(shape, f) for shape in extra),
        ]

    def parts(self, d):
        dx, dy, _ = d
        h = self.h
        src_x = {-1: (0, h), 0: (0, BX), 1: (BX - h, h)}[dx]
        dst_x = {-1: (HALO + BX, h), 0: (HALO, BX), 1: (HALO - h, h)}[dx]
        count = self.fields if dx == 0 else 4
        fields, sx, tx = pl.ds(0, count), pl.ds(*src_x), pl.ds(*dst_x)
        if dy == 0:
            return self.ro.at[:, pl.ds(HALO + src_x[0], src_x[1])], self.ro.at[:, tx]
        src_side, dst_side = (0, 1) if dy == -1 else (1, 0)
        return self.sy.at[fields, sx, src_side], self.ry.at[fields, tx, dst_side]

    def copy(self, index, pos):
        d = self.messages[index]
        src, dst = self.parts(d)
        return pltpu.make_async_remote_copy(
            src_ref=src,
            dst_ref=dst,
            send_sem=self.ssem.at[index],
            recv_sem=self.rsem.at[index],
            device_id={a: p + (e or 0) for a, p, e in zip(AXES, pos, d)},
            device_id_type=pl.DeviceIdType.MESH,
        )

    def put(self, i, tiles, field=0):
        h = self.h
        for c, tile in enumerate(tiles):
            self.ro[field + c, HALO + i] = tile
            self.sy[field + c, i, 0] = tile[0:h]
            self.sy[field + c, i, 1] = tile[BX - h : BX]

    def clear(self, has):
        for d in (-1, 1):
            start = HALO + BX if d == 1 else HALO - self.h
            side = 0 if d == -1 else 1

            def clear_x(start=start, slot=1 + d):
                for c in range(4):
                    for x in range(start, start + self.h):
                        zero(self.ro, (c, x))
                        zero(self.ry, (c, x))
                self.clear_columns(0, slot)

            pl.when(jnp.logical_not(has[0][d]))(clear_x)

            def clear_y(side=side):
                for c in range(4):
                    for x in range(EX):
                        zero(self.ry, (c, x, side))
                self.clear_columns(1, side)

            pl.when(jnp.logical_not(has[1][d]))(clear_y)

    def clear_columns(self, axis, which):
        pass

    def send(self, pos, has):
        for index, d in sorted(enumerate(self.messages), key=lambda e: e[1][1] == 0):
            guarded(every([has[a][d[a] or 0] for a in range(3)]), self.copy(index, pos).start)

    def wait_recv(self, pos, has, edges):
        for index, d in enumerate(self.messages):
            if (d[1] != 0) == edges:
                there = every([has[a][-(d[a] or 0)] for a in range(3)])
                guarded(there, self.copy(index, pos).wait_recv)

    def wait_send(self, pos, has):
        for index, d in enumerate(self.messages):
            guarded(every([has[a][d[a] or 0] for a in range(3)]), self.copy(index, pos).wait_send)

    def to_flat(self, targets, edges, kept=False):
        h = self.h
        rows = 2 * h if edges else BX
        lane = lax.broadcasted_iota(jnp.int32, (rows, 128), 1)
        main = self.ry if edges else self.ro
        nothing = jnp.zeros((rows, 128), jnp.float32)
        before = [nothing] * len(targets)
        for place in range(SLAB):
            if kept and HALO < place < HALO + BX:
                continue
            first, last = place == 0, place == SLAB - 1
            slot, before_slot = ((p >= HALO) + (p >= HALO + BX) for p in (place, place - 1))
            unit = (place - HALO) % BX

            def columns(side, slot):
                if kept and slot == 1:
                    return nothing
                return self.columns(edges, side, slot, unit // 4)

            both = jnp.where(
                (lane & 7) < HZ,
                nothing if first else columns(1, before_slot),
                nothing if last else columns(0, slot),
            )
            for c, out in enumerate(targets):
                if last or (kept and slot == 1):
                    now = nothing
                else:
                    now = pltpu.roll(main[c, place].reshape(rows, 128), 8 * place + HZ, 1)
                ends = pltpu.roll(both, (8 * place - HZ - 32 * (unit % 4) - 8 * c) % 128, 1)
                flat = jnp.where(
                    lane >= 8 * place + HZ,
                    now,
                    jnp.where(lane < 8 * place - HZ, before[c], ends),
                )
                before[c] = now
                if not edges:
                    where = pl.ds(HALO * SLAB + place, BX, stride=SLAB)
                    if kept and place == HALO:
                        flat = jnp.where(lane < 8 * place, flat, out[where, :])
                    if kept and place == HALO + BX:
                        flat = jnp.where(lane < 8 * place, out[where, :], flat)
                    out[where, :] = flat
                elif h == 1:
                    out[pl.ds(SLAB + place, 2, stride=9 * SLAB), :] = flat
                else:
                    out[pl.ds(place, 2, stride=SLAB), :] = flat[0:2]
                    out[pl.ds(10 * SLAB + place, 2, stride=SLAB), :] = flat[2:4]


class First(Group):
    extra_shapes = [
        (4, BX, 128),
        (4, 2, HALO, 128),
        (2, 3, 4, BX, 128),
        (2, 3, 4, 2, HALO, 128),
    ]

    def __init__(self, refs):
        super().__init__(HALO, refs)
        self.messages = list(DIRS)
        self.szo, self.szy, self.zo, self.zy = self.extra

    def parts(self, d):
        dx, dy, dz = d
        if dz == 0:
            return super().parts(d)
        side, slot = (0 if dz == 1 else 1), 1 - dx
        if dy == 0:
            return self.szo, self.zo.at[side, slot]
        src_side, dst_side = (0, 1) if dy == -1 else (1, 0)
        return self.szy.at[:, src_side], self.zy.at[side, slot, :, dst_side]

    def seal(self, packs):
        for k, pack in enumerate(packs):
            self.szo[k] = pack
            self.szy[k, 0] = pack[0:HALO]
            self.szy[k, 1] = pack[BX - HALO : BX]

    def clear(self, has):
        super().clear(has)
        for d in (-1, 1):

            def clear_z(side=(0 if d == -1 else 1)):
                self.clear_columns(2, side)

            pl.when(jnp.logical_not(has[2][d]))(clear_z)

    def clear_columns(self, axis, which):
        for side in range(2):
            for slot in range(3):
                for k in range(4):
                    if axis == 1:
                        zero(self.zy, (side, slot, k, which))
                    elif which == (slot if axis == 0 else side):
                        zero(self.zo, (side, slot, k))
                        zero(self.zy, (side, slot, k))

    def columns(self, edges, side, slot, k):
        if not edges:
            return self.zo[side, slot, k]
        return self.zy[side, slot, k].reshape(2 * HALO, 128)


class Targets(Group):
    def __init__(self, refs, first):
        super().__init__(1, refs)
        self.first = first

    def columns(self, edges, side, slot, k):
        found = self.first.columns(edges, side, slot, 2 + k)
        return found[1:3] if edges else found


class Second(Group):
    fields = 3
    extra_shapes = [(2, 2, HALO, 128), (2, 2, HALO, 128)]

    def __init__(self, refs):
        super().__init__(HALO, refs)
        self.messages = self.messages + [(0, -1, None), (0, 1, None)]
        self.szy, self.zy = self.extra

    def parts(self, d):
        if d[2] == 0:
            return super().parts(d)
        src_side, dst_side = (0, 1) if d[1] == -1 else (1, 0)
        return self.szy.at[:, src_side], self.zy.at[:, dst_side]

    def seal(self, packs):
        for k, pack in enumerate(packs):
            self.put(k, [pack], 3)
            self.put(BX - HALO + k, [pack], 3)
            self.szy[k, 0] = pack[0:HALO]
            self.szy[k, 1] = pack[BX - HALO : BX]

    def clear_columns(self, axis, which):
        if axis == 1:
            for k in range(2):
                zero(self.zy, (k, which))

    def columns(self, edges, side, slot, k):
        if slot == 1:
            return self.zy[k].reshape(2 * HALO, 128)
        x = k if slot == 0 else HALO + BX + k
        return self.ry[3, x].reshape(2 * HALO, 128) if edges else self.ro[3, x]


def merge(packs, unit, field, half, tile, lane4, from_lane):
    to = 32 * (unit % 4) + 8 * field + 4 * half
    shift = (to - from_lane) % 128
    moved = pltpu.roll(tile, shift, 1) if shift else tile
    packs[unit // 4] = jnp.where(lane4 == to // 4, moved, packs[unit // 4])


def pack_block(packs, i, tiles, lane4):
    for c, tile in enumerate(tiles):
        merge(packs, (i + 1) % BX, c, 0, tile, lane4, 0)
        merge(packs, i, c, 1, tile, lane4, 128 - HZ)


def loop(count, body):
    def trip(t, carry):
        for k in range(TOGETHER):
            body(t * TOGETHER + k)
        return carry

    lax.fori_loop(0, count // TOGETHER, trip, 0)
    for k in range(count - count % TOGETHER, count):
        body(k)


def span(row, stride):
    return pl.ds(row, 8) if stride == 1 else pl.ds(row, 8, stride=stride)


def after(ref, row, stride, lane, shift):
    whole, part = divmod(shift, 128)
    near = ref[span(row + whole, stride), :]
    far = ref[span(row + whole + 1, stride), :]
    return pltpu.roll(jnp.where(lane < part, far, near), 128 - part, 1)


def earlier(get, row, lane, shift):
    whole, part = divmod(shift, 128)
    return pltpu.roll(jnp.where(lane >= 128 - part, get(row - whole - 1), get(row - whole)), part, 1)


def differences(u, grads, lane, row, stride=1):
    for c in range(3):
        ref = u.at[c]
        a00 = ref[span(row, stride), :]
        a01 = after(ref, row, stride, lane, 1)
        a10 = after(ref, row, stride, lane, EZ)
        a11 = after(ref, row, stride, lane, EZ + 1)
        s0, s1 = a00 + a01, a10 + a11
        grads[3 * c, span(row, stride), :] = s1 - s0
        grads[3 * c + 1, span(row, stride), :] = s0 + s1
        grads[3 * c + 2, span(row, stride), :] = (a01 - a00) + (a11 - a10)


def stresses(grads, weights, corners, row, stride=1):
    def at(k, r):
        return grads[k, span(r, stride), :]

    deform = []
    for c in range(3):
        fx = at(3 * c, row) + at(3 * c, row + SLAB)
        fy = at(3 * c + 1, row + SLAB) - at(3 * c + 1, row)
        fz = at(3 * c + 2, row) + at(3 * c + 2, row + SLAB)
        deform.append([fx, fy, fz])
    for c in range(3):
        deform[c][c] = deform[c][c] + 1.0
    def dot(i, j):
        return deform[0][i] * deform[0][j] + deform[1][i] * deform[1][j] + deform[2][i] * deform[2][j]

    grams = [dot(0, 0), dot(1, 1), dot(2, 2)]
    total = grams[0] + grams[1] + grams[2]
    scale = jnp.minimum(lax.rsqrt(total * (1.0 / 3.0)), 1.0)
    half = scale * scale * 0.5
    mean = half * total * (1.0 / 3.0)
    d0, d1, d2 = (grams[k] * half - mean for k in range(3))
    d01, d02, d12 = dot(0, 1) * half, dot(0, 2) * half, dot(1, 2) * half
    sq01, sq02, sq12 = d01 * d01, d02 * d02, d12 * d12
    e0, e1, e2 = d0 * d0 + (sq01 + sq02), d1 * d1 + (sq01 + sq12), d2 * d2 + (sq02 + sq12)
    e01, e02, e12 = d02 * d12 - d2 * d01, d01 * d12 - d1 * d02, d01 * d02 - d0 * d12
    p = 0.5 * (e0 + e1 + e2)
    q = d0 * (d1 * d2 - sq12) + (d01 * e01 + d02 * e02)

    def reduced(c0, c1, c2, c3, c4):
        return c0 + q * c3, c1 + (p * c3 + q * c4), c2 + p * c4

    def times_linear(k, c):
        return k * c[0] + q * c[2], (k * c[1] + c[0]) + p * c[2], k * c[2] + c[1]

    low = mean - 1.5
    square = low * low
    t = mean * square + q, 2.0 * (mean * low) + (square + p), mean + 2.0 * low
    poly = times_linear(low, (t[0] - 1.5, t[1], t[2]))
    for step in range(2, POLAR_STEPS):
        c0, c1, c2 = poly
        twice0, twice1 = c0 + c0, c1 + c1
        square = reduced(c0 * c0, twice0 * c1, twice0 * c2 + c1 * c1, twice1 * c2, c2 * c2)
        t0, t1, t2 = times_linear(mean, square)
        t0 = t0 - 1.5
        poly = reduced(
            c0 * t0,
            c0 * t1 + c1 * t0,
            c0 * t2 + c1 * t1 + c2 * t0,
            c1 * t2 + c2 * t1,
            c2 * t2,
        )
    weight = weights[span(row, stride), :]
    heavy = weight * scale
    c0, c1, c2 = weight - heavy * poly[0], heavy * poly[1], heavy * poly[2]
    w0, w1, w2 = (c0 - (c1 * d + c2 * e) for d, e in ((d0, e0), (d1, e1), (d2, e2)))
    w01, w02, w12 = (c1 * d + c2 * e for d, e in ((d01, e01), (d02, e02), (d12, e12)))
    for c in range(3):
        fx, fy, fz = deform[c]
        px = fx * w0 - (fy * w01 + fz * w02)
        py = fy * w1 - (fx * w01 + fz * w12)
        pz = fz * w2 - (fx * w02 + fy * w12)
        s, t = py + px, py - px
        for k, part in enumerate((s + pz, s - pz, t + pz, t - pz)):
            corners[4 * c + k, span(row + VOFF, stride), :] = part


def update(state, u, prev, inertial, rate, corners, omega, lane, row, stride=1):
    seen = state.setdefault(stride, {})

    def spread(c, k):
        def get(r):
            if (c, k, r) not in seen:
                below = corners[4 * c + k, span(r + VOFF - SLAB, stride), :]
                seen[c, k, r] = below - corners[4 * c + 3 - k, span(r + VOFF, stride), :]
            return seen[c, k, r]

        return get

    a = rate[span(row, stride), :]
    result = []
    for c in range(3):
        force = (
            earlier(spread(c, 0), row, lane, EZ + 1) + earlier(spread(c, 1), row, lane, EZ)
        ) + (earlier(spread(c, 2), row, lane, 1) + spread(c, 3)(row))
        here = u[c, span(row, stride), :]
        new = here - a * ((here - inertial[c, span(row, stride), :]) + force)
        if omega is not None:
            old = prev[c, span(row, stride), :]
            new = omega * (new - old) + old
        result.append(new)
    return result


def kernel(
    start_hbm,
    inertial_hbm,
    material_hbm,
    pinned_hbm,
    stiffness,
    out,
    start_v,
    inertial_v,
    material_v,
    pinned_v,
    in_sems,
    ulat,
    wflat,
    iflat,
    pflat,
    rate,
    grads,
    corners,
    *group_refs,
):
    pos = [lax.axis_index(a) for a in AXES]
    sizes = [lax.axis_size(a) for a in AXES]
    has = [{-1: p > 0, 0: True, 1: p < n - 1} for p, n in zip(pos, sizes)]
    loads = [
        pltpu.make_async_copy(src, dst, in_sems.at[i])
        for i, (src, dst) in enumerate(
            (
                (start_hbm, start_v),
                (inertial_hbm, inertial_v),
                (material_hbm, material_v),
                (pinned_hbm, pinned_v),
            )
        )
    ]
    for load in loads:
        load.start()
    ends = [5 + len(First.extra_shapes), 10 + len(First.extra_shapes)]
    first = First(group_refs[: ends[0]])
    targets = Targets(group_refs[ends[0] : ends[1]], first)
    second = Second(group_refs[ends[1] :])
    barrier = pltpu.get_barrier_semaphore()
    for d in sorted(DIRS, key=lambda e: -sum(map(abs, e))):

        def greet(d=d):
            pl.semaphore_signal(
                barrier,
                inc=1,
                device_id={a: p + e for a, p, e in zip(AXES, pos, d)},
                device_id_type=pl.DeviceIdType.MESH,
            )

        guarded(every([has[a][d[a]] for a in range(3)]), greet)
    first.clear(has)
    targets.clear(has)

    for load in loads:
        load.wait()
    lane = lax.broadcasted_iota(jnp.int32, (BX, 128), 1)
    grid_y = lax.broadcasted_iota(jnp.int32, (BX, 128), 0) + pos[1] * BX
    grid_z = lane + pos[2] * 128
    inner = (grid_y < BX * sizes[1] - 1) & (grid_z < 128 * sizes[2] - 1)

    lane4 = lane >> 2
    nothing = jnp.zeros((BX, 128), jnp.float32)
    packs = [[nothing, nothing], [nothing, nothing]]
    for i in range(BX):
        pins = pinned_v[i] > 0
        goal = [inertial_v[c, i] * 0.25 for c in range(3)]
        disp = [jnp.where(pins, goal[c], start_v[c, i] * 0.25) for c in range(3)]
        kinds = material_v[i]
        weight = nothing
        for m in range(MATS):
            weight = jnp.where(kinds == m, stiffness[m] * 0.0625, weight)
        valid = inner & (pos[0] * BX + i < BX * sizes[0] - 1)
        fields = (disp + [jnp.where(valid, weight, 0.0)], goal + [jnp.where(pins, 1.0, 0.0)])
        for group, pack, tiles in zip((first, targets), packs, fields):
            group.put(i, tiles)
            pack_block(pack, i, tiles, lane4)
    first.seal(packs[0] + packs[1])

    sides = [1 + (p > 0).astype(jnp.int32) + (p < n - 1).astype(jnp.int32) for p, n in zip(pos, sizes)]
    pl.semaphore_wait(barrier, sides[0] * sides[1] * sides[2] - 1)
    first.send(pos, has)
    targets.send(pos, has)
    second.clear(has)

    u0, u1, u2 = (ulat.at[k] for k in range(3))
    firsts = [u0.at[c] for c in range(3)] + [wflat]
    goals = [iflat.at[c] for c in range(3)] + [pflat]

    def wide(group, fields, u, between):
        def inside(t):
            stresses(grads, wflat, corners, 26 + 8 * t)

        def outside(t):
            stresses(grads, wflat, corners, jnp.where(t < 4, 0, 82) + 8 * t)

        group.wait_recv(pos, has, False)
        group.to_flat(fields, False, group is second)
        for r in range(26, 130, 8):
            differences(u, grads, lane, r)
        loop(12, inside)
        between()
        group.wait_recv(pos, has, True)
        group.to_flat(fields, True)
        for r in (*range(0, 32, 8), *range(130, 162, 8)):
            differences(u, grads, lane, r)
        loop(8, outside)

    def narrow(u):
        for r in range(1, 11):
            differences(u, grads, lane, SLAB + r, SLAB)
        for r in (9 * SLAB + 1, 9 * SLAB + 3, 10 * SLAB + 1, 10 * SLAB + 3):
            differences(u, grads, lane, r)

        def column(t):
            stresses(grads, wflat, corners, SLAB + 1 + t, SLAB)

        loop(10, column)
        for r in (9 * SLAB + 1, 9 * SLAB + 3):
            stresses(grads, wflat, corners, r)

    def update_wide(u, prev, fresh, omega):
        for r in range(SLAB, SLAB + 136, 8):
            new = update({}, u, prev, iflat, rate, corners, omega, lane, r)
            for c in range(3):
                fresh[c, pl.ds(r, 8), :] = new[c]

    def update_own(u, prev, omega):
        state = {}
        return [
            update(state, u, prev, iflat, rate, corners, omega, lane, HALO * SLAB + r, SLAB)
            for r in range(HALO, HALO + BX + 1)
        ]

    def own_tile(rows, i, c):
        shift = 8 * (HALO + i) + HZ
        return pltpu.roll(jnp.where(lane >= shift, rows[i][c], rows[i + 1][c]), 128 - shift, 1)

    def goals_inside():
        targets.wait_recv(pos, has, False)
        targets.to_flat(goals, False)

    wide(first, firsts, u0, goals_inside)
    targets.wait_recv(pos, has, True)
    targets.to_flat(goals, True)

    sums = grads.at[0]
    for r in range(SLAB, SLAB + 136, 8):
        sums[pl.ds(r, 8), :] = wflat[pl.ds(r, 8), :] + wflat[pl.ds(r - SLAB, 8), :]
    for r in range(SLAB, SLAB + 136, 8):

        def get(row):
            return sums[pl.ds(row, 8), :]

        total = (earlier(get, r, lane, EZ + 1) + earlier(get, r, lane, EZ)) + (
            earlier(get, r, lane, 1) + get(r)
        )
        rate[pl.ds(r, 8), :] = jnp.where(
            pflat[pl.ds(r, 8), :] > 0.0, 0.0, relax / (1.0 + 3.0 * total)
        )

    omega1 = 2.0 / (2.0 - radius * radius)
    omega2 = 4.0 / (4.0 - radius * radius * omega1)
    omega3 = 4.0 / (4.0 - radius * radius * omega2)

    update_wide(u0, None, u1, None)
    narrow(u1)
    rows = update_own(u1, u0, omega1)
    pack = [nothing, nothing]
    for i in range(BX):
        second.put(i, [own_tile(rows, i, c) for c in range(3)])
    for i in range(BX + 1):
        place = HALO + i
        for c in range(3):
            if i > 0:
                merge(pack, i % BX, c, 0, rows[i][c], lane4, 8 * place - HZ)
            if i < BX:
                merge(pack, i, c, 1, rows[i][c], lane4, 8 * place)
    second.seal(pack)
    second.send(pos, has)
    for i in range(BX + 1):
        for c in range(3):
            u2[c, pl.ds(HALO * SLAB + HALO + i, BX, stride=SLAB), :] = rows[i][c]

    first.wait_send(pos, has)
    targets.wait_send(pos, has)
    wide(second, [u2.at[c] for c in range(3)], u2, lambda: None)
    second.wait_send(pos, has)
    update_wide(u2, u1, u0, omega2)
    narrow(u0)
    rows = update_own(u0, u2, omega3)
    for i in range(BX):
        for c in range(3):
            out[c, i] = 4.0 * own_tile(rows, i, c)


def per_device(start_disp, inertial, material, pinned, stiffness):
    f = jnp.float32
    flat = (ROWS, 128)
    hbm = pl.BlockSpec(memory_space=pl.ANY)
    return pl.pallas_call(
        kernel,
        out_shape=pltpu.VMEM(start_disp.shape, f),
        in_specs=[hbm, hbm, hbm, hbm, pl.BlockSpec(memory_space=pltpu.SMEM)],
        out_specs=pl.BlockSpec(memory_space=pltpu.VMEM),
        scratch_shapes=[
            pltpu.VMEM(start_disp.shape, f),
            pltpu.VMEM(inertial.shape, f),
            pltpu.VMEM(material.shape, jnp.int32),
            pltpu.VMEM(pinned.shape, jnp.int32),
            pltpu.SemaphoreType.DMA((4,)),
            pltpu.VMEM((3, 3, *flat), f),
            pltpu.VMEM(flat, f),
            pltpu.VMEM((3, *flat), f),
            pltpu.VMEM(flat, f),
            pltpu.VMEM(flat, f),
            pltpu.VMEM((9, *flat), f),
            pltpu.VMEM((12, *flat), f),
            *Group.scratch(HALO, len(DIRS), First.extra_shapes),
            *Group.scratch(1, 8),
            *Group.scratch(HALO, 10, Second.extra_shapes),
        ],
        compiler_params=pltpu.CompilerParams(collective_id=0, has_side_effects=True),
    )(start_disp, inertial, material, pinned, stiffness)


def solution(mesh):
    placed = (
        P(None, "gx", "gy", "gz"),
        P(None, "gx", "gy", "gz"),
        P("gx", "gy", "gz"),
        P("gx", "gy", "gz"),
        P(),
    )
    return jax.shard_map(
        per_device, mesh=mesh, in_specs=placed, out_specs=P(None, "gx", "gy", "gz"), check_vma=False
    )
```

```python
import functools

import jax
import jax.numpy as jnp
from jax import lax
from jax.experimental import pallas as pl
from jax.experimental.pallas import tpu as pltpu
from jax.sharding import PartitionSpec as P

ITERS = 4
POLAR_STEPS = 6
MATS = 8

relax = 0.6
radius = 0.9

AXES = ("gx", "gy", "gz")
BX = 8
HALO = 2
EX = BX + 2 * HALO
HZ = 2 * HALO
EZ = 128 + 2 * HZ
SLAB = 13
ROWS = 176
VOFF = 16
TOGETHER = 2
DIRS = [
    (dx, dy, dz)
    for dx in (-1, 0, 1)
    for dy in (-1, 0, 1)
    for dz in (-1, 0, 1)
    if (dx, dy, dz) != (0, 0, 0)
]


def every(conds):
    conds = [c for c in conds if c is not True]
    return functools.reduce(lambda p, q: p & q, conds) if conds else True


def guarded(cond, act):
    if cond is True:
        act()
    else:
        pl.when(cond)(act)


def zero(ref, index):
    ref[index] = jnp.zeros(ref.at[index].shape, jnp.float32)


class Group:
    fields = 4

    def __init__(self, width, refs):
        self.h = width
        self.ro, self.ry, self.sy, self.ssem, self.rsem, *self.extra = refs
        self.messages = [d for d in DIRS if d[2] == 0]

    @staticmethod
    def scratch(width, total, extra=()):
        f = jnp.float32
        return [
            pltpu.VMEM((4, EX, BX, 128), f),
            pltpu.VMEM((4, EX, 2, width, 128), f),
            pltpu.VMEM((4, BX, 2, width, 128), f),
            pltpu.SemaphoreType.DMA((total,)),
            pltpu.SemaphoreType.DMA((total,)),
            *(pltpu.VMEM(shape, f) for shape in extra),
        ]

    def parts(self, d):
        dx, dy, _ = d
        h = self.h
        src_x = {-1: (0, h), 0: (0, BX), 1: (BX - h, h)}[dx]
        dst_x = {-1: (HALO + BX, h), 0: (HALO, BX), 1: (HALO - h, h)}[dx]
        count = self.fields if dx == 0 else 4
        fields, sx, tx = pl.ds(0, count), pl.ds(*src_x), pl.ds(*dst_x)
        if dy == 0:
            return self.ro.at[:, pl.ds(HALO + src_x[0], src_x[1])], self.ro.at[:, tx]
        src_side, dst_side = (0, 1) if dy == -1 else (1, 0)
        return self.sy.at[fields, sx, src_side], self.ry.at[fields, tx, dst_side]

    def copy(self, index, pos):
        d = self.messages[index]
        src, dst = self.parts(d)
        return pltpu.make_async_remote_copy(
            src_ref=src,
            dst_ref=dst,
            send_sem=self.ssem.at[index],
            recv_sem=self.rsem.at[index],
            device_id={a: p + (e or 0) for a, p, e in zip(AXES, pos, d)},
            device_id_type=pl.DeviceIdType.MESH,
        )

    def put(self, i, tiles, field=0):
        h = self.h
        for c, tile in enumerate(tiles):
            self.ro[field + c, HALO + i] = tile
            self.sy[field + c, i, 0] = tile[0:h]
            self.sy[field + c, i, 1] = tile[BX - h : BX]

    def clear(self, has):
        for d in (-1, 1):
            start = HALO + BX if d == 1 else HALO - self.h
            side = 0 if d == -1 else 1

            def clear_x(start=start, slot=1 + d):
                for c in range(4):
                    for x in range(start, start + self.h):
                        zero(self.ro, (c, x))
                        zero(self.ry, (c, x))
                self.clear_columns(0, slot)

            pl.when(jnp.logical_not(has[0][d]))(clear_x)

            def clear_y(side=side):
                for c in range(4):
                    for x in range(EX):
                        zero(self.ry, (c, x, side))
                self.clear_columns(1, side)

            pl.when(jnp.logical_not(has[1][d]))(clear_y)

    def clear_columns(self, axis, which):
        pass

    def send(self, pos, has):
        for index, d in sorted(
            enumerate(self.messages), key=lambda e: (e[1][1] == 0, -sum(abs(a or 0) for a in e[1]))
        ):
            guarded(every([has[a][d[a] or 0] for a in range(3)]), self.copy(index, pos).start)

    def wait_recv(self, pos, has, edges):
        for index, d in enumerate(self.messages):
            if (d[1] != 0) == edges:
                there = every([has[a][-(d[a] or 0)] for a in range(3)])
                guarded(there, self.copy(index, pos).wait_recv)

    def wait_send(self, pos, has):
        for index, d in enumerate(self.messages):
            guarded(every([has[a][d[a] or 0] for a in range(3)]), self.copy(index, pos).wait_send)

    def to_flat(self, targets, edges, kept=False):
        h = self.h
        rows = 2 * h if edges else BX
        lane = lax.broadcasted_iota(jnp.int32, (rows, 128), 1)
        main = self.ry if edges else self.ro
        nothing = jnp.zeros((rows, 128), jnp.float32)
        before = [nothing] * len(targets)
        for place in range(SLAB):
            if kept and HALO < place < HALO + BX:
                continue
            first, last = place == 0, place == SLAB - 1
            slot, before_slot = ((p >= HALO) + (p >= HALO + BX) for p in (place, place - 1))
            unit = (place - HALO) % BX

            def columns(side, slot):
                if kept and slot == 1:
                    return nothing
                return self.columns(edges, side, slot, unit // 4)

            both = jnp.where(
                (lane & 7) < HZ,
                nothing if first else columns(1, before_slot),
                nothing if last else columns(0, slot),
            )
            for c, out in enumerate(targets):
                if last or (kept and slot == 1):
                    now = nothing
                else:
                    now = pltpu.roll(main[c, place].reshape(rows, 128), 8 * place + HZ, 1)
                ends = pltpu.roll(both, (8 * place - HZ - 32 * (unit % 4) - 8 * c) % 128, 1)
                flat = jnp.where(
                    lane >= 8 * place + HZ,
                    now,
                    jnp.where(lane < 8 * place - HZ, before[c], ends),
                )
                before[c] = now
                if not edges:
                    where = pl.ds(HALO * SLAB + place, BX, stride=SLAB)
                    if kept and place == HALO:
                        flat = jnp.where(lane < 8 * place, flat, out[where, :])
                    if kept and place == HALO + BX:
                        flat = jnp.where(lane < 8 * place, out[where, :], flat)
                    out[where, :] = flat
                elif h == 1:
                    out[pl.ds(SLAB + place, 2, stride=9 * SLAB), :] = flat
                else:
                    out[pl.ds(place, 2, stride=SLAB), :] = flat[0:2]
                    out[pl.ds(10 * SLAB + place, 2, stride=SLAB), :] = flat[2:4]


class First(Group):
    extra_shapes = [
        (4, BX, 128),
        (4, 2, HALO, 128),
        (2, 3, 4, BX, 128),
        (2, 3, 4, 2, HALO, 128),
    ]

    def __init__(self, refs):
        super().__init__(HALO, refs)
        self.messages = list(DIRS)
        self.szo, self.szy, self.zo, self.zy = self.extra

    def parts(self, d):
        dx, dy, dz = d
        if dz == 0:
            return super().parts(d)
        side, slot = (0 if dz == 1 else 1), 1 - dx
        if dy == 0:
            return self.szo, self.zo.at[side, slot]
        src_side, dst_side = (0, 1) if dy == -1 else (1, 0)
        return self.szy.at[:, src_side], self.zy.at[side, slot, :, dst_side]

    def seal(self, packs):
        for k, pack in enumerate(packs):
            self.szo[k] = pack
            self.szy[k, 0] = pack[0:HALO]
            self.szy[k, 1] = pack[BX - HALO : BX]

    def clear(self, has):
        super().clear(has)
        for d in (-1, 1):

            def clear_z(side=(0 if d == -1 else 1)):
                self.clear_columns(2, side)

            pl.when(jnp.logical_not(has[2][d]))(clear_z)

    def clear_columns(self, axis, which):
        for side in range(2):
            for slot in range(3):
                for k in range(4):
                    if axis == 1:
                        zero(self.zy, (side, slot, k, which))
                    elif which == (slot if axis == 0 else side):
                        zero(self.zo, (side, slot, k))
                        zero(self.zy, (side, slot, k))

    def columns(self, edges, side, slot, k):
        if not edges:
            return self.zo[side, slot, k]
        return self.zy[side, slot, k].reshape(2 * HALO, 128)


class Targets(Group):
    def __init__(self, refs, first):
        super().__init__(1, refs)
        self.first = first

    def columns(self, edges, side, slot, k):
        found = self.first.columns(edges, side, slot, 2 + k)
        return found[1:3] if edges else found


class Second(Group):
    fields = 3
    extra_shapes = [(2, 2, HALO, 128), (2, 2, HALO, 128)]

    def __init__(self, refs):
        super().__init__(HALO, refs)
        self.messages = self.messages + [(0, -1, None), (0, 1, None)]
        self.szy, self.zy = self.extra

    def parts(self, d):
        if d[2] == 0:
            return super().parts(d)
        src_side, dst_side = (0, 1) if d[1] == -1 else (1, 0)
        return self.szy.at[:, src_side], self.zy.at[:, dst_side]

    def seal(self, packs):
        for k, pack in enumerate(packs):
            self.put(k, [pack], 3)
            self.put(BX - HALO + k, [pack], 3)
            self.szy[k, 0] = pack[0:HALO]
            self.szy[k, 1] = pack[BX - HALO : BX]

    def clear_columns(self, axis, which):
        if axis == 1:
            for k in range(2):
                zero(self.zy, (k, which))

    def columns(self, edges, side, slot, k):
        if slot == 1:
            return self.zy[k].reshape(2 * HALO, 128)
        x = k if slot == 0 else HALO + BX + k
        return self.ry[3, x].reshape(2 * HALO, 128) if edges else self.ro[3, x]


def merge(packs, unit, field, half, tile, lane4, from_lane):
    to = 32 * (unit % 4) + 8 * field + 4 * half
    shift = (to - from_lane) % 128
    moved = pltpu.roll(tile, shift, 1) if shift else tile
    packs[unit // 4] = jnp.where(lane4 == to // 4, moved, packs[unit // 4])


def pack_block(packs, i, tiles, lane4):
    for c, tile in enumerate(tiles):
        merge(packs, (i + 1) % BX, c, 0, tile, lane4, 0)
        merge(packs, i, c, 1, tile, lane4, 128 - HZ)


def loop(count, body):
    def trip(t, carry):
        for k in range(TOGETHER):
            body(t * TOGETHER + k)
        return carry

    lax.fori_loop(0, count // TOGETHER, trip, 0)
    for k in range(count - count % TOGETHER, count):
        body(k)


def span(row, stride):
    return pl.ds(row, 8) if stride == 1 else pl.ds(row, 8, stride=stride)


def after(ref, row, stride, lane, shift):
    whole, part = divmod(shift, 128)
    near = ref[span(row + whole, stride), :]
    far = ref[span(row + whole + 1, stride), :]
    return pltpu.roll(jnp.where(lane < part, far, near), 128 - part, 1)


def earlier(get, row, lane, shift):
    whole, part = divmod(shift, 128)
    return pltpu.roll(jnp.where(lane >= 128 - part, get(row - whole - 1), get(row - whole)), part, 1)


def differences(u, grads, lane, row, stride=1):
    for c in range(3):
        ref = u.at[c]
        a00 = ref[span(row, stride), :]
        a01 = after(ref, row, stride, lane, 1)
        a10 = after(ref, row, stride, lane, EZ)
        a11 = after(ref, row, stride, lane, EZ + 1)
        s0, s1 = a00 + a01, a10 + a11
        grads[3 * c, span(row, stride), :] = s1 - s0
        grads[3 * c + 1, span(row, stride), :] = s0 + s1
        grads[3 * c + 2, span(row, stride), :] = (a01 - a00) + (a11 - a10)


def stresses(grads, weights, corners, row, stride=1):
    def at(k, r):
        return grads[k, span(r, stride), :]

    deform = []
    for c in range(3):
        fx = at(3 * c, row) + at(3 * c, row + SLAB)
        fy = at(3 * c + 1, row + SLAB) - at(3 * c + 1, row)
        fz = at(3 * c + 2, row) + at(3 * c + 2, row + SLAB)
        deform.append([fx, fy, fz])
    for c in range(3):
        deform[c][c] = deform[c][c] + 1.0
    def dot(i, j):
        return deform[0][i] * deform[0][j] + deform[1][i] * deform[1][j] + deform[2][i] * deform[2][j]

    grams = [dot(0, 0), dot(1, 1), dot(2, 2)]
    total = grams[0] + grams[1] + grams[2]
    scale = jnp.minimum(lax.rsqrt(total * (1.0 / 3.0)), 1.0)
    half = scale * scale * 0.5
    mean = half * total * (1.0 / 3.0)
    d0, d1, d2 = (grams[k] * half - mean for k in range(3))
    d01, d02, d12 = dot(0, 1) * half, dot(0, 2) * half, dot(1, 2) * half
    sq01, sq02, sq12 = d01 * d01, d02 * d02, d12 * d12
    e0, e1, e2 = d0 * d0 + (sq01 + sq02), d1 * d1 + (sq01 + sq12), d2 * d2 + (sq02 + sq12)
    e01, e02, e12 = d02 * d12 - d2 * d01, d01 * d12 - d1 * d02, d01 * d02 - d0 * d12
    p = 0.5 * (e0 + e1 + e2)
    q = d0 * (d1 * d2 - sq12) + (d01 * e01 + d02 * e02)

    def reduced(c0, c1, c2, c3, c4):
        return c0 + q * c3, c1 + (p * c3 + q * c4), c2 + p * c4

    def times_linear(k, c):
        return k * c[0] + q * c[2], (k * c[1] + c[0]) + p * c[2], k * c[2] + c[1]

    low = mean - 1.5
    square = low * low
    t = mean * square + q, 2.0 * (mean * low) + (square + p), mean + 2.0 * low
    poly = times_linear(low, (t[0] - 1.5, t[1], t[2]))
    for step in range(2, POLAR_STEPS):
        c0, c1, c2 = poly
        twice0, twice1 = c0 + c0, c1 + c1
        square = reduced(c0 * c0, twice0 * c1, twice0 * c2 + c1 * c1, twice1 * c2, c2 * c2)
        t0, t1, t2 = times_linear(mean, square)
        t0 = t0 - 1.5
        poly = reduced(
            c0 * t0,
            c0 * t1 + c1 * t0,
            c0 * t2 + c1 * t1 + c2 * t0,
            c1 * t2 + c2 * t1,
            c2 * t2,
        )
    weight = weights[span(row, stride), :]
    heavy = weight * scale
    c0, c1, c2 = weight - heavy * poly[0], heavy * poly[1], heavy * poly[2]
    w0, w1, w2 = (c0 - (c1 * d + c2 * e) for d, e in ((d0, e0), (d1, e1), (d2, e2)))
    w01, w02, w12 = (c1 * d + c2 * e for d, e in ((d01, e01), (d02, e02), (d12, e12)))
    for c in range(3):
        fx, fy, fz = deform[c]
        px = fx * w0 - (fy * w01 + fz * w02)
        py = fy * w1 - (fx * w01 + fz * w12)
        pz = fz * w2 - (fx * w02 + fy * w12)
        s, t = py + px, py - px
        for k, part in enumerate((s + pz, s - pz, t + pz, t - pz)):
            corners[4 * c + k, span(row + VOFF, stride), :] = part


def update(state, u, prev, inertial, rate, corners, omega, lane, row, stride=1):
    seen = state.setdefault(stride, {})

    def spread(c, k):
        def get(r):
            if (c, k, r) not in seen:
                below = corners[4 * c + k, span(r + VOFF - SLAB, stride), :]
                seen[c, k, r] = below - corners[4 * c + 3 - k, span(r + VOFF, stride), :]
            return seen[c, k, r]

        return get

    a = rate[span(row, stride), :]
    result = []
    for c in range(3):
        force = (
            earlier(spread(c, 0), row, lane, EZ + 1) + earlier(spread(c, 1), row, lane, EZ)
        ) + (earlier(spread(c, 2), row, lane, 1) + spread(c, 3)(row))
        here = u[c, span(row, stride), :]
        new = here - a * ((here - inertial[c, span(row, stride), :]) + force)
        if omega is not None:
            old = prev[c, span(row, stride), :]
            new = omega * (new - old) + old
        result.append(new)
    return result


def kernel(
    start_hbm,
    inertial_hbm,
    material_hbm,
    pinned_hbm,
    stiffness,
    out,
    start_v,
    inertial_v,
    material_v,
    pinned_v,
    in_sems,
    ulat,
    wflat,
    iflat,
    pflat,
    rate,
    grads,
    corners,
    *group_refs,
):
    pos = [lax.axis_index(a) for a in AXES]
    sizes = [lax.axis_size(a) for a in AXES]
    has = [{-1: p > 0, 0: True, 1: p < n - 1} for p, n in zip(pos, sizes)]
    loads = [
        pltpu.make_async_copy(src, dst, in_sems.at[i])
        for i, (src, dst) in enumerate(
            (
                (start_hbm, start_v),
                (inertial_hbm, inertial_v),
                (material_hbm, material_v),
                (pinned_hbm, pinned_v),
            )
        )
    ]
    for load in loads:
        load.start()
    ends = [5 + len(First.extra_shapes), 10 + len(First.extra_shapes)]
    first = First(group_refs[: ends[0]])
    targets = Targets(group_refs[ends[0] : ends[1]], first)
    second = Second(group_refs[ends[1] :])
    barrier = pltpu.get_barrier_semaphore()
    for d in sorted(DIRS, key=lambda e: -sum(map(abs, e))):

        def greet(d=d):
            pl.semaphore_signal(
                barrier,
                inc=1,
                device_id={a: p + e for a, p, e in zip(AXES, pos, d)},
                device_id_type=pl.DeviceIdType.MESH,
            )

        guarded(every([has[a][d[a]] for a in range(3)]), greet)
    first.clear(has)
    targets.clear(has)

    for load in loads:
        load.wait()
    lane = lax.broadcasted_iota(jnp.int32, (BX, 128), 1)
    grid_y = lax.broadcasted_iota(jnp.int32, (BX, 128), 0) + pos[1] * BX
    grid_z = lane + pos[2] * 128
    inner = (grid_y < BX * sizes[1] - 1) & (grid_z < 128 * sizes[2] - 1)

    lane4 = lane >> 2
    nothing = jnp.zeros((BX, 128), jnp.float32)
    packs = [[nothing, nothing], [nothing, nothing]]
    for i in range(BX):
        pins = pinned_v[i] > 0
        goal = [inertial_v[c, i] * 0.25 for c in range(3)]
        disp = [jnp.where(pins, goal[c], start_v[c, i] * 0.25) for c in range(3)]
        kinds = material_v[i]
        weight = nothing
        for m in range(MATS):
            weight = jnp.where(kinds == m, stiffness[m] * 0.0625, weight)
        valid = inner & (pos[0] * BX + i < BX * sizes[0] - 1)
        fields = (disp + [jnp.where(valid, weight, 0.0)], goal + [jnp.where(pins, 1.0, 0.0)])
        for group, pack, tiles in zip((first, targets), packs, fields):
            group.put(i, tiles)
            pack_block(pack, i, tiles, lane4)
    first.seal(packs[0] + packs[1])

    sides = [1 + (p > 0).astype(jnp.int32) + (p < n - 1).astype(jnp.int32) for p, n in zip(pos, sizes)]
    pl.semaphore_wait(barrier, sides[0] * sides[1] * sides[2] - 1)
    first.send(pos, has)
    targets.send(pos, has)
    second.clear(has)

    u0, u1, u2 = (ulat.at[k] for k in range(3))
    firsts = [u0.at[c] for c in range(3)] + [wflat]
    goals = [iflat.at[c] for c in range(3)] + [pflat]

    def wide(group, fields, u, between):
        def inside(t):
            stresses(grads, wflat, corners, 26 + 8 * t)

        def outside(t):
            stresses(grads, wflat, corners, jnp.where(t < 4, 0, 82) + 8 * t)

        def columns(numbers, shift):
            for r in numbers:
                differences(u, grads, lane, HALO * SLAB + r, SLAB)
            loop(6, lambda t: stresses(grads, wflat, corners, HALO * SLAB + shift(t), SLAB))

        if group is second:
            columns(range(3, 9), lambda t: 3 + t)
            group.wait_recv(pos, has, False)
            group.to_flat(fields, False, True)
            columns((0, 1, 2, 9, 10, 11), lambda t: t + jnp.where(t < 3, 0, 6))
        else:
            group.wait_recv(pos, has, False)
            group.to_flat(fields, False)
            for r in range(26, 130, 8):
                differences(u, grads, lane, r)
            loop(12, inside)
        between()
        group.wait_recv(pos, has, True)
        group.to_flat(fields, True)
        for r in (*range(0, 32, 8), *range(130, 162, 8)):
            differences(u, grads, lane, r)
        loop(8, outside)

    def narrow(u):
        for r in range(1, 11):
            differences(u, grads, lane, SLAB + r, SLAB)
        for r in (9 * SLAB + 1, 9 * SLAB + 3, 10 * SLAB + 1, 10 * SLAB + 3):
            differences(u, grads, lane, r)

        def column(t):
            stresses(grads, wflat, corners, SLAB + 1 + t, SLAB)

        loop(10, column)
        for r in (9 * SLAB + 1, 9 * SLAB + 3):
            stresses(grads, wflat, corners, r)

    def update_wide(u, prev, fresh, omega):
        for r in range(SLAB, SLAB + 136, 8):
            new = update({}, u, prev, iflat, rate, corners, omega, lane, r)
            for c in range(3):
                fresh[c, pl.ds(r, 8), :] = new[c]

    def update_own(u, prev, omega):
        state = {}
        return [
            update(state, u, prev, iflat, rate, corners, omega, lane, HALO * SLAB + r, SLAB)
            for r in range(HALO, HALO + BX + 1)
        ]

    def own_tile(rows, i, c):
        shift = 8 * (HALO + i) + HZ
        return pltpu.roll(jnp.where(lane >= shift, rows[i][c], rows[i + 1][c]), 128 - shift, 1)

    def goals_inside():
        targets.wait_recv(pos, has, False)
        targets.to_flat(goals, False)

    wide(first, firsts, u0, goals_inside)
    targets.wait_recv(pos, has, True)
    targets.to_flat(goals, True)

    sums = grads.at[0]
    for r in range(SLAB, SLAB + 136, 8):
        sums[pl.ds(r, 8), :] = wflat[pl.ds(r, 8), :] + wflat[pl.ds(r - SLAB, 8), :]
    for r in range(SLAB, SLAB + 136, 8):

        def get(row):
            return sums[pl.ds(row, 8), :]

        total = (earlier(get, r, lane, EZ + 1) + earlier(get, r, lane, EZ)) + (
            earlier(get, r, lane, 1) + get(r)
        )
        rate[pl.ds(r, 8), :] = jnp.where(
            pflat[pl.ds(r, 8), :] > 0.0, 0.0, relax / (1.0 + 3.0 * total)
        )

    omega1 = 2.0 / (2.0 - radius * radius)
    omega2 = 4.0 / (4.0 - radius * radius * omega1)
    omega3 = 4.0 / (4.0 - radius * radius * omega2)

    update_wide(u0, None, u1, None)
    narrow(u1)
    rows = update_own(u1, u0, omega1)
    pack = [nothing, nothing]
    for i in range(BX):
        second.put(i, [own_tile(rows, i, c) for c in range(3)])
    for i in range(BX + 1):
        place = HALO + i
        for c in range(3):
            if i > 0:
                merge(pack, i % BX, c, 0, rows[i][c], lane4, 8 * place - HZ)
            if i < BX:
                merge(pack, i, c, 1, rows[i][c], lane4, 8 * place)
    second.seal(pack)
    second.send(pos, has)
    for i in range(BX + 1):
        for c in range(3):
            u2[c, pl.ds(HALO * SLAB + HALO + i, BX, stride=SLAB), :] = rows[i][c]

    first.wait_send(pos, has)
    targets.wait_send(pos, has)
    wide(second, [u2.at[c] for c in range(3)], u2, lambda: None)
    second.wait_send(pos, has)
    update_wide(u2, u1, u0, omega2)
    narrow(u0)
    rows = update_own(u0, u2, omega3)
    for i in range(BX):
        for c in range(3):
            out[c, i] = 4.0 * own_tile(rows, i, c)


def per_device(start_disp, inertial, material, pinned, stiffness):
    f = jnp.float32
    flat = (ROWS, 128)
    hbm = pl.BlockSpec(memory_space=pl.ANY)
    return pl.pallas_call(
        kernel,
        out_shape=pltpu.VMEM(start_disp.shape, f),
        in_specs=[hbm, hbm, hbm, hbm, pl.BlockSpec(memory_space=pltpu.SMEM)],
        out_specs=pl.BlockSpec(memory_space=pltpu.VMEM),
        scratch_shapes=[
            pltpu.VMEM(start_disp.shape, f),
            pltpu.VMEM(inertial.shape, f),
            pltpu.VMEM(material.shape, jnp.int32),
            pltpu.VMEM(pinned.shape, jnp.int32),
            pltpu.SemaphoreType.DMA((4,)),
            pltpu.VMEM((3, 3, *flat), f),
            pltpu.VMEM(flat, f),
            pltpu.VMEM((3, *flat), f),
            pltpu.VMEM(flat, f),
            pltpu.VMEM(flat, f),
            pltpu.VMEM((9, *flat), f),
            pltpu.VMEM((12, *flat), f),
            *Group.scratch(HALO, len(DIRS), First.extra_shapes),
            *Group.scratch(1, 8),
            *Group.scratch(HALO, 10, Second.extra_shapes),
        ],
        compiler_params=pltpu.CompilerParams(collective_id=0, has_side_effects=True),
    )(start_disp, inertial, material, pinned, stiffness)


def solution(mesh):
    placed = (
        P(None, "gx", "gy", "gz"),
        P(None, "gx", "gy", "gz"),
        P("gx", "gy", "gz"),
        P("gx", "gy", "gz"),
        P(),
    )
    return jax.shard_map(
        per_device, mesh=mesh, in_specs=placed, out_specs=P(None, "gx", "gy", "gz"), check_vma=False
    )
```

```python
import functools

import jax
import jax.numpy as jnp
from jax import lax
from jax.experimental import pallas as pl
from jax.experimental.pallas import tpu as pltpu
from jax.sharding import PartitionSpec as P

ITERS = 4
POLAR_STEPS = 6
MATS = 8

relax = 0.6
radius = 0.9

AXES = ("gx", "gy", "gz")
BX = 8
HALO = 2
EX = BX + 2 * HALO
HZ = 2 * HALO
EZ = 128 + 2 * HZ
SLAB = 13
ROWS = 176
VOFF = 16
TOGETHER = 2
DIRS = [
    (dx, dy, dz)
    for dx in (-1, 0, 1)
    for dy in (-1, 0, 1)
    for dz in (-1, 0, 1)
    if (dx, dy, dz) != (0, 0, 0)
]


def every(conds):
    conds = [c for c in conds if c is not True]
    return functools.reduce(lambda p, q: p & q, conds) if conds else True


def guarded(cond, act):
    if cond is True:
        act()
    else:
        pl.when(cond)(act)


def zero(ref, index):
    ref[index] = jnp.zeros(ref.at[index].shape, jnp.float32)


class Group:
    fields = 4

    def __init__(self, width, refs):
        self.h = width
        self.ro, self.ry, self.sy, self.ssem, self.rsem, *self.extra = refs
        self.messages = [d for d in DIRS if d[2] == 0]

    @staticmethod
    def scratch(width, total, extra=()):
        f = jnp.float32
        return [
            pltpu.VMEM((4, EX, BX, 128), f),
            pltpu.VMEM((4, EX, 2, width, 128), f),
            pltpu.VMEM((4, BX, 2, width, 128), f),
            pltpu.SemaphoreType.DMA((total,)),
            pltpu.SemaphoreType.DMA((total,)),
            *(pltpu.VMEM(shape, f) for shape in extra),
        ]

    def parts(self, d):
        dx, dy, _ = d
        h = self.h
        src_x = {-1: (0, h), 0: (0, BX), 1: (BX - h, h)}[dx]
        dst_x = {-1: (HALO + BX, h), 0: (HALO, BX), 1: (HALO - h, h)}[dx]
        count = self.fields if dx == 0 else 4
        fields, sx, tx = pl.ds(0, count), pl.ds(*src_x), pl.ds(*dst_x)
        if dy == 0:
            return self.ro.at[:, pl.ds(HALO + src_x[0], src_x[1])], self.ro.at[:, tx]
        src_side, dst_side = (0, 1) if dy == -1 else (1, 0)
        return self.sy.at[fields, sx, src_side], self.ry.at[fields, tx, dst_side]

    def copy(self, index, pos):
        d = self.messages[index]
        src, dst = self.parts(d)
        return pltpu.make_async_remote_copy(
            src_ref=src,
            dst_ref=dst,
            send_sem=self.ssem.at[index],
            recv_sem=self.rsem.at[index],
            device_id={a: p + (e or 0) for a, p, e in zip(AXES, pos, d)},
            device_id_type=pl.DeviceIdType.MESH,
        )

    def put(self, i, tiles, field=0):
        h = self.h
        for c, tile in enumerate(tiles):
            self.ro[field + c, HALO + i] = tile
            self.sy[field + c, i, 0] = tile[0:h]
            self.sy[field + c, i, 1] = tile[BX - h : BX]

    def clear(self, has):
        for d in (-1, 1):
            start = HALO + BX if d == 1 else HALO - self.h
            side = 0 if d == -1 else 1

            def clear_x(start=start, slot=1 + d):
                for c in range(4):
                    for x in range(start, start + self.h):
                        zero(self.ro, (c, x))
                        zero(self.ry, (c, x))
                self.clear_columns(0, slot)

            pl.when(jnp.logical_not(has[0][d]))(clear_x)

            def clear_y(side=side):
                for c in range(4):
                    for x in range(EX):
                        zero(self.ry, (c, x, side))
                self.clear_columns(1, side)

            pl.when(jnp.logical_not(has[1][d]))(clear_y)

    def clear_columns(self, axis, which):
        pass

    def send(self, pos, has):
        for index, d in sorted(
            enumerate(self.messages), key=lambda e: (e[1][1] == 0, -sum(abs(a or 0) for a in e[1]))
        ):
            guarded(every([has[a][d[a] or 0] for a in range(3)]), self.copy(index, pos).start)

    def wait_recv(self, pos, has, edges):
        for index, d in enumerate(self.messages):
            if (d[1] != 0) == edges:
                there = every([has[a][-(d[a] or 0)] for a in range(3)])
                guarded(there, self.copy(index, pos).wait_recv)

    def wait_send(self, pos, has):
        for index, d in enumerate(self.messages):
            guarded(every([has[a][d[a] or 0] for a in range(3)]), self.copy(index, pos).wait_send)

    def to_flat(self, targets, edges, kept=False):
        h = self.h
        rows = 2 * h if edges else BX
        lane = lax.broadcasted_iota(jnp.int32, (rows, 128), 1)
        main = self.ry if edges else self.ro
        nothing = jnp.zeros((rows, 128), jnp.float32)
        before = [nothing] * len(targets)
        for place in range(SLAB):
            if kept and HALO < place < HALO + BX:
                continue
            first, last = place == 0, place == SLAB - 1
            slot, before_slot = ((p >= HALO) + (p >= HALO + BX) for p in (place, place - 1))
            unit = (place - HALO) % BX

            def columns(side, slot):
                if kept and slot == 1:
                    return nothing
                return self.columns(edges, side, slot, unit // 4)

            both = jnp.where(
                (lane & 7) < HZ,
                nothing if first else columns(1, before_slot),
                nothing if last else columns(0, slot),
            )
            for c, out in enumerate(targets):
                if last or (kept and slot == 1):
                    now = nothing
                else:
                    now = pltpu.roll(main[c, place].reshape(rows, 128), 8 * place + HZ, 1)
                ends = pltpu.roll(both, (8 * place - HZ - 32 * (unit % 4) - 8 * c) % 128, 1)
                flat = jnp.where(
                    lane >= 8 * place + HZ,
                    now,
                    jnp.where(lane < 8 * place - HZ, before[c], ends),
                )
                before[c] = now
                if not edges:
                    where = pl.ds(HALO * SLAB + place, BX, stride=SLAB)
                    if kept and place == HALO:
                        flat = jnp.where(lane < 8 * place, flat, out[where, :])
                    if kept and place == HALO + BX:
                        flat = jnp.where(lane < 8 * place, out[where, :], flat)
                    out[where, :] = flat
                elif h == 1:
                    out[pl.ds(SLAB + place, 2, stride=9 * SLAB), :] = flat
                else:
                    out[pl.ds(place, 2, stride=SLAB), :] = flat[0:2]
                    out[pl.ds(10 * SLAB + place, 2, stride=SLAB), :] = flat[2:4]


class First(Group):
    extra_shapes = [
        (4, BX, 128),
        (4, 2, HALO, 128),
        (2, 3, 4, BX, 128),
        (2, 3, 4, 2, HALO, 128),
    ]

    def __init__(self, refs):
        super().__init__(HALO, refs)
        self.messages = list(DIRS)
        self.szo, self.szy, self.zo, self.zy = self.extra

    def parts(self, d):
        dx, dy, dz = d
        if dz == 0:
            return super().parts(d)
        side, slot = (0 if dz == 1 else 1), 1 - dx
        if dy == 0:
            return self.szo, self.zo.at[side, slot]
        src_side, dst_side = (0, 1) if dy == -1 else (1, 0)
        return self.szy.at[:, src_side], self.zy.at[side, slot, :, dst_side]

    def seal(self, packs):
        for k, pack in enumerate(packs):
            self.szo[k] = pack
            self.szy[k, 0] = pack[0:HALO]
            self.szy[k, 1] = pack[BX - HALO : BX]

    def clear(self, has):
        super().clear(has)
        for d in (-1, 1):

            def clear_z(side=(0 if d == -1 else 1)):
                self.clear_columns(2, side)

            pl.when(jnp.logical_not(has[2][d]))(clear_z)

    def clear_columns(self, axis, which):
        for side in range(2):
            for slot in range(3):
                for k in range(4):
                    if axis == 1:
                        zero(self.zy, (side, slot, k, which))
                    elif which == (slot if axis == 0 else side):
                        zero(self.zo, (side, slot, k))
                        zero(self.zy, (side, slot, k))

    def columns(self, edges, side, slot, k):
        if not edges:
            return self.zo[side, slot, k]
        return self.zy[side, slot, k].reshape(2 * HALO, 128)


class Targets(Group):
    def __init__(self, refs, first):
        super().__init__(1, refs)
        self.first = first

    def columns(self, edges, side, slot, k):
        found = self.first.columns(edges, side, slot, 2 + k)
        return found[1:3] if edges else found


class Second(Group):
    fields = 3
    extra_shapes = [(2, 2, HALO, 128), (2, 2, HALO, 128)]

    def __init__(self, refs):
        super().__init__(HALO, refs)
        self.messages = self.messages + [(0, -1, None), (0, 1, None)]
        self.szy, self.zy = self.extra

    def parts(self, d):
        if d[2] == 0:
            return super().parts(d)
        src_side, dst_side = (0, 1) if d[1] == -1 else (1, 0)
        return self.szy.at[:, src_side], self.zy.at[:, dst_side]

    def seal(self, packs):
        for k, pack in enumerate(packs):
            self.put(k, [pack], 3)
            self.put(BX - HALO + k, [pack], 3)
            self.szy[k, 0] = pack[0:HALO]
            self.szy[k, 1] = pack[BX - HALO : BX]

    def clear_columns(self, axis, which):
        if axis == 1:
            for k in range(2):
                zero(self.zy, (k, which))

    def columns(self, edges, side, slot, k):
        if slot == 1:
            return self.zy[k].reshape(2 * HALO, 128)
        x = k if slot == 0 else HALO + BX + k
        return self.ry[3, x].reshape(2 * HALO, 128) if edges else self.ro[3, x]


def merge(packs, unit, field, half, tile, lane4, from_lane):
    to = 32 * (unit % 4) + 8 * field + 4 * half
    shift = (to - from_lane) % 128
    moved = pltpu.roll(tile, shift, 1) if shift else tile
    packs[unit // 4] = jnp.where(lane4 == to // 4, moved, packs[unit // 4])


def pack_block(packs, i, tiles, lane4):
    for c, tile in enumerate(tiles):
        merge(packs, (i + 1) % BX, c, 0, tile, lane4, 0)
        merge(packs, i, c, 1, tile, lane4, 128 - HZ)


def loop(count, body):
    def trip(t, carry):
        for k in range(TOGETHER):
            body(t * TOGETHER + k)
        return carry

    lax.fori_loop(0, count // TOGETHER, trip, 0)
    for k in range(count - count % TOGETHER, count):
        body(k)


def span(row, stride):
    return pl.ds(row, 8) if stride == 1 else pl.ds(row, 8, stride=stride)


def after(ref, row, stride, lane, shift):
    whole, part = divmod(shift, 128)
    near = ref[span(row + whole, stride), :]
    far = ref[span(row + whole + 1, stride), :]
    return pltpu.roll(jnp.where(lane < part, far, near), 128 - part, 1)


def earlier(get, row, lane, shift):
    whole, part = divmod(shift, 128)
    return pltpu.roll(jnp.where(lane >= 128 - part, get(row - whole - 1), get(row - whole)), part, 1)


def differences(u, grads, lane, row, stride=1):
    for c in range(3):
        ref = u.at[c]
        a00 = ref[span(row, stride), :]
        a01 = after(ref, row, stride, lane, 1)
        a10 = after(ref, row, stride, lane, EZ)
        a11 = after(ref, row, stride, lane, EZ + 1)
        s0, s1 = a00 + a01, a10 + a11
        grads[3 * c, span(row, stride), :] = s1 - s0
        grads[3 * c + 1, span(row, stride), :] = s0 + s1
        grads[3 * c + 2, span(row, stride), :] = (a01 - a00) + (a11 - a10)


def stresses(grads, weights, corners, row, stride=1):
    def at(k, r):
        return grads[k, span(r, stride), :]

    deform = []
    for c in range(3):
        fx = at(3 * c, row) + at(3 * c, row + SLAB)
        fy = at(3 * c + 1, row + SLAB) - at(3 * c + 1, row)
        fz = at(3 * c + 2, row) + at(3 * c + 2, row + SLAB)
        deform.append([fx, fy, fz])
    for c in range(3):
        deform[c][c] = deform[c][c] + 1.0
    def dot(i, j):
        return deform[0][i] * deform[0][j] + deform[1][i] * deform[1][j] + deform[2][i] * deform[2][j]

    grams = [dot(0, 0), dot(1, 1), dot(2, 2)]
    total = grams[0] + grams[1] + grams[2]
    scale = jnp.minimum(lax.rsqrt(total * (1.0 / 3.0)), 1.0)
    half = scale * scale * 0.5
    mean = half * total * (1.0 / 3.0)
    d0, d1, d2 = (grams[k] * half - mean for k in range(3))
    d01, d02, d12 = dot(0, 1) * half, dot(0, 2) * half, dot(1, 2) * half
    sq01, sq02, sq12 = d01 * d01, d02 * d02, d12 * d12
    e0, e1, e2 = d0 * d0 + (sq01 + sq02), d1 * d1 + (sq01 + sq12), d2 * d2 + (sq02 + sq12)
    e01, e02, e12 = d02 * d12 - d2 * d01, d01 * d12 - d1 * d02, d01 * d02 - d0 * d12
    p = 0.5 * (e0 + e1 + e2)
    q = d0 * (d1 * d2 - sq12) + (d01 * e01 + d02 * e02)

    def reduced(c0, c1, c2, c3, c4):
        return c0 + q * c3, c1 + (p * c3 + q * c4), c2 + p * c4

    def times_linear(k, c):
        return k * c[0] + q * c[2], (k * c[1] + c[0]) + p * c[2], k * c[2] + c[1]

    low = mean - 1.5
    square = low * low
    t = mean * square + q, 2.0 * (mean * low) + (square + p), mean + 2.0 * low
    poly = times_linear(low, (t[0] - 1.5, t[1], t[2]))
    for step in range(2, POLAR_STEPS):
        c0, c1, c2 = poly
        twice0, twice1 = c0 + c0, c1 + c1
        square = reduced(c0 * c0, twice0 * c1, twice0 * c2 + c1 * c1, twice1 * c2, c2 * c2)
        t0, t1, t2 = times_linear(mean, square)
        t0 = t0 - 1.5
        poly = reduced(
            c0 * t0,
            c0 * t1 + c1 * t0,
            c0 * t2 + c1 * t1 + c2 * t0,
            c1 * t2 + c2 * t1,
            c2 * t2,
        )
    weight = weights[span(row, stride), :]
    heavy = weight * scale
    c0, c1, c2 = weight - heavy * poly[0], heavy * poly[1], heavy * poly[2]
    w0, w1, w2 = (c0 - (c1 * d + c2 * e) for d, e in ((d0, e0), (d1, e1), (d2, e2)))
    w01, w02, w12 = (c1 * d + c2 * e for d, e in ((d01, e01), (d02, e02), (d12, e12)))
    for c in range(3):
        fx, fy, fz = deform[c]
        px = fx * w0 - (fy * w01 + fz * w02)
        py = fy * w1 - (fx * w01 + fz * w12)
        pz = fz * w2 - (fx * w02 + fy * w12)
        s, t = py + px, py - px
        for k, part in enumerate((s + pz, s - pz, t + pz, t - pz)):
            corners[4 * c + k, span(row + VOFF, stride), :] = part


def update(state, u, prev, inertial, rate, corners, omega, lane, row, stride=1):
    seen = state.setdefault(stride, {})

    def spread(c, k):
        def get(r):
            if (c, k, r) not in seen:
                below = corners[4 * c + k, span(r + VOFF - SLAB, stride), :]
                seen[c, k, r] = below - corners[4 * c + 3 - k, span(r + VOFF, stride), :]
            return seen[c, k, r]

        return get

    a = rate[span(row, stride), :]
    result = []
    for c in range(3):
        force = (
            earlier(spread(c, 0), row, lane, EZ + 1) + earlier(spread(c, 1), row, lane, EZ)
        ) + (earlier(spread(c, 2), row, lane, 1) + spread(c, 3)(row))
        here = u[c, span(row, stride), :]
        new = here - a * ((here - inertial[c, span(row, stride), :]) + force)
        if omega is not None:
            old = prev[c, span(row, stride), :]
            new = omega * (new - old) + old
        result.append(new)
    return result


def kernel(
    start_hbm,
    inertial_hbm,
    material_hbm,
    pinned_hbm,
    stiffness,
    out,
    start_v,
    inertial_v,
    material_v,
    pinned_v,
    in_sems,
    ulat,
    wflat,
    iflat,
    pflat,
    rate,
    sums,
    grads,
    corners,
    *group_refs,
):
    pos = [lax.axis_index(a) for a in AXES]
    sizes = [lax.axis_size(a) for a in AXES]
    has = [{-1: p > 0, 0: True, 1: p < n - 1} for p, n in zip(pos, sizes)]
    loads = [
        pltpu.make_async_copy(src, dst, in_sems.at[i])
        for i, (src, dst) in enumerate(
            (
                (start_hbm, start_v),
                (inertial_hbm, inertial_v),
                (material_hbm, material_v),
                (pinned_hbm, pinned_v),
            )
        )
    ]
    for load in loads:
        load.start()
    ends = [5 + len(First.extra_shapes), 10 + len(First.extra_shapes)]
    first = First(group_refs[: ends[0]])
    targets = Targets(group_refs[ends[0] : ends[1]], first)
    second = Second(group_refs[ends[1] :])
    barrier = pltpu.get_barrier_semaphore()
    for d in sorted(DIRS, key=lambda e: -sum(map(abs, e))):

        def greet(d=d):
            pl.semaphore_signal(
                barrier,
                inc=1,
                device_id={a: p + e for a, p, e in zip(AXES, pos, d)},
                device_id_type=pl.DeviceIdType.MESH,
            )

        guarded(every([has[a][d[a]] for a in range(3)]), greet)
    first.clear(has)
    targets.clear(has)

    for load in loads:
        load.wait()
    lane = lax.broadcasted_iota(jnp.int32, (BX, 128), 1)
    grid_y = lax.broadcasted_iota(jnp.int32, (BX, 128), 0) + pos[1] * BX
    grid_z = lane + pos[2] * 128
    inner = (grid_y < BX * sizes[1] - 1) & (grid_z < 128 * sizes[2] - 1)

    lane4 = lane >> 2
    nothing = jnp.zeros((BX, 128), jnp.float32)
    packs = [[nothing, nothing], [nothing, nothing]]
    for i in range(BX):
        pins = pinned_v[i] > 0
        goal = [inertial_v[c, i] * 0.25 for c in range(3)]
        disp = [jnp.where(pins, goal[c], start_v[c, i] * 0.25) for c in range(3)]
        kinds = material_v[i]
        weight = nothing
        for m in range(MATS):
            weight = jnp.where(kinds == m, stiffness[m] * 0.0625, weight)
        valid = inner & (pos[0] * BX + i < BX * sizes[0] - 1)
        fields = (disp + [jnp.where(valid, weight, 0.0)], goal + [jnp.where(pins, 1.0, 0.0)])
        for group, pack, tiles in zip((first, targets), packs, fields):
            group.put(i, tiles)
            pack_block(pack, i, tiles, lane4)
    first.seal(packs[0] + packs[1])

    sides = [1 + (p > 0).astype(jnp.int32) + (p < n - 1).astype(jnp.int32) for p, n in zip(pos, sizes)]
    pl.semaphore_wait(barrier, sides[0] * sides[1] * sides[2] - 1)
    first.send(pos, has)
    targets.send(pos, has)
    second.clear(has)

    u0, u1, u2 = (ulat.at[k] for k in range(3))
    firsts = [u0.at[c] for c in range(3)] + [wflat]
    goals = [iflat.at[c] for c in range(3)] + [pflat]

    def wide(group, fields, u, between):
        def inside(t):
            stresses(grads, wflat, corners, 26 + 8 * t)

        def outside(t):
            stresses(grads, wflat, corners, jnp.where(t < 4, 0, 82) + 8 * t)

        def columns(numbers, shift):
            for r in numbers:
                differences(u, grads, lane, HALO * SLAB + r, SLAB)
            loop(6, lambda t: stresses(grads, wflat, corners, HALO * SLAB + shift(t), SLAB))

        if group is second:
            columns(range(3, 9), lambda t: 3 + t)
            group.wait_recv(pos, has, False)
            group.to_flat(fields, False, True)
            columns((0, 1, 2, 9, 10, 11), lambda t: t + jnp.where(t < 3, 0, 6))
        else:
            group.wait_recv(pos, has, False)
            group.to_flat(fields, False)
            for r in range(26, 130, 8):
                differences(u, grads, lane, r)
            loop(12, inside)
        between()
        group.wait_recv(pos, has, True)
        group.to_flat(fields, True)
        for r in (*range(0, 32, 8), *range(130, 162, 8)):
            differences(u, grads, lane, r)
        loop(8, outside)

    def narrow(u):
        for r in range(1, 11):
            differences(u, grads, lane, SLAB + r, SLAB)
        for r in (9 * SLAB + 1, 9 * SLAB + 3, 10 * SLAB + 1, 10 * SLAB + 3):
            differences(u, grads, lane, r)

        def column(t):
            stresses(grads, wflat, corners, SLAB + 1 + t, SLAB)

        loop(10, column)
        for r in (9 * SLAB + 1, 9 * SLAB + 3):
            stresses(grads, wflat, corners, r)

    inner = range(3 * SLAB, 9 * SLAB, 8)
    outer = (*range(SLAB, 3 * SLAB, 8), *range(9 * SLAB, 11 * SLAB, 8))

    def update_rows(blocks, u, prev, fresh, omega):
        for r in blocks:
            new = update({}, u, prev, iflat, rate, corners, omega, lane, r)
            for c in range(3):
                fresh[c, pl.ds(r, 8), :] = new[c]

    def rates(blocks):
        for r in blocks:
            sums[pl.ds(r, 8), :] = wflat[pl.ds(r, 8), :] + wflat[pl.ds(r - SLAB, 8), :]

        def get(row):
            return sums[pl.ds(row, 8), :]

        for r in blocks:
            total = (earlier(get, r, lane, EZ + 1) + earlier(get, r, lane, EZ)) + (
                earlier(get, r, lane, 1) + get(r)
            )
            rate[pl.ds(r, 8), :] = jnp.where(
                pflat[pl.ds(r, 8), :] > 0.0, 0.0, relax / (1.0 + 3.0 * total)
            )

    def update_own(u, prev, omega):
        state = {}
        return [
            update(state, u, prev, iflat, rate, corners, omega, lane, HALO * SLAB + r, SLAB)
            for r in range(HALO, HALO + BX + 1)
        ]

    def own_tile(rows, i, c):
        shift = 8 * (HALO + i) + HZ
        return pltpu.roll(jnp.where(lane >= shift, rows[i][c], rows[i + 1][c]), 128 - shift, 1)

    omega1 = 2.0 / (2.0 - radius * radius)
    omega2 = 4.0 / (4.0 - radius * radius * omega1)
    omega3 = 4.0 / (4.0 - radius * radius * omega2)

    def inner_first():
        targets.wait_recv(pos, has, False)
        targets.to_flat(goals, False)
        rates(inner)
        update_rows(inner, u0, None, u1, None)

    wide(first, firsts, u0, inner_first)
    targets.wait_recv(pos, has, True)
    targets.to_flat(goals, True)
    rates(outer)
    update_rows(outer, u0, None, u1, None)
    narrow(u1)
    rows = update_own(u1, u0, omega1)
    pack = [nothing, nothing]
    for i in range(BX):
        second.put(i, [own_tile(rows, i, c) for c in range(3)])
    for i in range(BX + 1):
        place = HALO + i
        for c in range(3):
            if i > 0:
                merge(pack, i % BX, c, 0, rows[i][c], lane4, 8 * place - HZ)
            if i < BX:
                merge(pack, i, c, 1, rows[i][c], lane4, 8 * place)
    second.seal(pack)
    second.send(pos, has)
    for i in range(BX + 1):
        for c in range(3):
            u2[c, pl.ds(HALO * SLAB + HALO + i, BX, stride=SLAB), :] = rows[i][c]

    first.wait_send(pos, has)
    targets.wait_send(pos, has)
    wide(
        second,
        [u2.at[c] for c in range(3)],
        u2,
        lambda: update_rows(inner, u2, u1, u0, omega2),
    )
    second.wait_send(pos, has)
    update_rows(outer, u2, u1, u0, omega2)
    narrow(u0)
    rows = update_own(u0, u2, omega3)
    for i in range(BX):
        for c in range(3):
            out[c, i] = 4.0 * own_tile(rows, i, c)


def per_device(start_disp, inertial, material, pinned, stiffness):
    f = jnp.float32
    flat = (ROWS, 128)
    hbm = pl.BlockSpec(memory_space=pl.ANY)
    return pl.pallas_call(
        kernel,
        out_shape=pltpu.VMEM(start_disp.shape, f),
        in_specs=[hbm, hbm, hbm, hbm, pl.BlockSpec(memory_space=pltpu.SMEM)],
        out_specs=pl.BlockSpec(memory_space=pltpu.VMEM),
        scratch_shapes=[
            pltpu.VMEM(start_disp.shape, f),
            pltpu.VMEM(inertial.shape, f),
            pltpu.VMEM(material.shape, jnp.int32),
            pltpu.VMEM(pinned.shape, jnp.int32),
            pltpu.SemaphoreType.DMA((4,)),
            pltpu.VMEM((3, 3, *flat), f),
            pltpu.VMEM(flat, f),
            pltpu.VMEM((3, *flat), f),
            pltpu.VMEM(flat, f),
            pltpu.VMEM(flat, f),
            pltpu.VMEM(flat, f),
            pltpu.VMEM((9, *flat), f),
            pltpu.VMEM((12, *flat), f),
            *Group.scratch(HALO, len(DIRS), First.extra_shapes),
            *Group.scratch(1, 8),
            *Group.scratch(HALO, 10, Second.extra_shapes),
        ],
        compiler_params=pltpu.CompilerParams(collective_id=0, has_side_effects=True),
    )(start_disp, inertial, material, pinned, stiffness)


def solution(mesh):
    placed = (
        P(None, "gx", "gy", "gz"),
        P(None, "gx", "gy", "gz"),
        P("gx", "gy", "gz"),
        P("gx", "gy", "gz"),
        P(),
    )
    return jax.shard_map(
        per_device, mesh=mesh, in_specs=placed, out_specs=P(None, "gx", "gy", "gz"), check_vma=False
    )
```

```python
import functools

import jax
import jax.numpy as jnp
from jax import lax
from jax.experimental import pallas as pl
from jax.experimental.pallas import tpu as pltpu
from jax.sharding import PartitionSpec as P

ITERS = 4
POLAR_STEPS = 6
MATS = 8

relax = 0.6
radius = 0.9

AXES = ("gx", "gy", "gz")
BX = 8
HALO = 2
EX = BX + 2 * HALO
HZ = 2 * HALO
EZ = 128 + 2 * HZ
SLAB = 13
ROWS = 176
VOFF = 16
TOGETHER = 2
DIRS = [
    (dx, dy, dz)
    for dx in (-1, 0, 1)
    for dy in (-1, 0, 1)
    for dz in (-1, 0, 1)
    if (dx, dy, dz) != (0, 0, 0)
]


def every(conds):
    conds = [c for c in conds if c is not True]
    return functools.reduce(lambda p, q: p & q, conds) if conds else True


def guarded(cond, act):
    if cond is True:
        act()
    else:
        pl.when(cond)(act)


def zero(ref, index):
    ref[index] = jnp.zeros(ref.at[index].shape, jnp.float32)


class Group:
    fields = 4

    def __init__(self, width, refs):
        self.h = width
        self.ro, self.ry, self.sy, self.ssem, self.rsem, *self.extra = refs
        self.messages = [d for d in DIRS if d[2] == 0]

    @staticmethod
    def scratch(width, total, extra=()):
        f = jnp.float32
        return [
            pltpu.VMEM((4, EX, BX, 128), f),
            pltpu.VMEM((4, EX, 2, width, 128), f),
            pltpu.VMEM((4, BX, 2, width, 128), f),
            pltpu.SemaphoreType.DMA((total,)),
            pltpu.SemaphoreType.DMA((total,)),
            *(pltpu.VMEM(shape, f) for shape in extra),
        ]

    def parts(self, d):
        dx, dy, _ = d
        h = self.h
        src_x = {-1: (0, h), 0: (0, BX), 1: (BX - h, h)}[dx]
        dst_x = {-1: (HALO + BX, h), 0: (HALO, BX), 1: (HALO - h, h)}[dx]
        count = self.fields if dx == 0 else 4
        fields, sx, tx = pl.ds(0, count), pl.ds(*src_x), pl.ds(*dst_x)
        if dy == 0:
            return self.ro.at[:, pl.ds(HALO + src_x[0], src_x[1])], self.ro.at[:, tx]
        src_side, dst_side = (0, 1) if dy == -1 else (1, 0)
        return self.sy.at[fields, sx, src_side], self.ry.at[fields, tx, dst_side]

    def copy(self, index, pos):
        d = self.messages[index]
        src, dst = self.parts(d)
        return pltpu.make_async_remote_copy(
            src_ref=src,
            dst_ref=dst,
            send_sem=self.ssem.at[index],
            recv_sem=self.rsem.at[index],
            device_id={a: p + (e or 0) for a, p, e in zip(AXES, pos, d)},
            device_id_type=pl.DeviceIdType.MESH,
        )

    def put(self, i, tiles, field=0):
        h = self.h
        for c, tile in enumerate(tiles):
            self.ro[field + c, HALO + i] = tile
            self.sy[field + c, i, 0] = tile[0:h]
            self.sy[field + c, i, 1] = tile[BX - h : BX]

    def clear(self, has):
        for d in (-1, 1):
            start = HALO + BX if d == 1 else HALO - self.h
            side = 0 if d == -1 else 1

            def clear_x(start=start, slot=1 + d):
                for c in range(4):
                    for x in range(start, start + self.h):
                        zero(self.ro, (c, x))
                        zero(self.ry, (c, x))
                self.clear_columns(0, slot)

            pl.when(jnp.logical_not(has[0][d]))(clear_x)

            def clear_y(side=side):
                for c in range(4):
                    for x in range(EX):
                        zero(self.ry, (c, x, side))
                self.clear_columns(1, side)

            pl.when(jnp.logical_not(has[1][d]))(clear_y)

    def clear_columns(self, axis, which):
        pass

    def send(self, pos, has):
        for index, d in sorted(
            enumerate(self.messages), key=lambda e: (e[1][1] != 0, -sum(abs(a or 0) for a in e[1]))
        ):
            guarded(every([has[a][d[a] or 0] for a in range(3)]), self.copy(index, pos).start)

    def wait_recv(self, pos, has, edges):
        for index, d in enumerate(self.messages):
            if (d[1] != 0) == edges:
                there = every([has[a][-(d[a] or 0)] for a in range(3)])
                guarded(there, self.copy(index, pos).wait_recv)

    def wait_send(self, pos, has):
        for index, d in enumerate(self.messages):
            guarded(every([has[a][d[a] or 0] for a in range(3)]), self.copy(index, pos).wait_send)

    def to_flat(self, targets, edges, kept=False):
        h = self.h
        rows = 2 * h if edges else BX
        lane = lax.broadcasted_iota(jnp.int32, (rows, 128), 1)
        main = self.ry if edges else self.ro
        nothing = jnp.zeros((rows, 128), jnp.float32)
        before = [nothing] * len(targets)
        for place in range(SLAB):
            if kept and HALO < place < HALO + BX:
                continue
            first, last = place == 0, place == SLAB - 1
            slot, before_slot = ((p >= HALO) + (p >= HALO + BX) for p in (place, place - 1))
            unit = (place - HALO) % BX

            def columns(side, slot):
                if kept and slot == 1:
                    return nothing
                return self.columns(edges, side, slot, unit // 4)

            both = jnp.where(
                (lane & 7) < HZ,
                nothing if first else columns(1, before_slot),
                nothing if last else columns(0, slot),
            )
            for c, out in enumerate(targets):
                if last or (kept and slot == 1):
                    now = nothing
                else:
                    now = pltpu.roll(main[c, place].reshape(rows, 128), 8 * place + HZ, 1)
                ends = pltpu.roll(both, (8 * place - HZ - 32 * (unit % 4) - 8 * c) % 128, 1)
                flat = jnp.where(
                    lane >= 8 * place + HZ,
                    now,
                    jnp.where(lane < 8 * place - HZ, before[c], ends),
                )
                before[c] = now
                if not edges:
                    where = pl.ds(HALO * SLAB + place, BX, stride=SLAB)
                    if kept and place == HALO:
                        flat = jnp.where(lane < 8 * place, flat, out[where, :])
                    if kept and place == HALO + BX:
                        flat = jnp.where(lane < 8 * place, out[where, :], flat)
                    out[where, :] = flat
                elif h == 1:
                    out[pl.ds(SLAB + place, 2, stride=9 * SLAB), :] = flat
                else:
                    out[pl.ds(place, 2, stride=SLAB), :] = flat[0:2]
                    out[pl.ds(10 * SLAB + place, 2, stride=SLAB), :] = flat[2:4]


class First(Group):
    extra_shapes = [
        (4, BX, 128),
        (4, 2, HALO, 128),
        (2, 3, 4, BX, 128),
        (2, 3, 4, 2, HALO, 128),
    ]

    def __init__(self, refs):
        super().__init__(HALO, refs)
        self.messages = list(DIRS)
        self.szo, self.szy, self.zo, self.zy = self.extra

    def parts(self, d):
        dx, dy, dz = d
        if dz == 0:
            return super().parts(d)
        side, slot = (0 if dz == 1 else 1), 1 - dx
        if dy == 0:
            return self.szo, self.zo.at[side, slot]
        src_side, dst_side = (0, 1) if dy == -1 else (1, 0)
        return self.szy.at[:, src_side], self.zy.at[side, slot, :, dst_side]

    def seal(self, packs):
        for k, pack in enumerate(packs):
            self.szo[k] = pack
            self.szy[k, 0] = pack[0:HALO]
            self.szy[k, 1] = pack[BX - HALO : BX]

    def clear(self, has):
        super().clear(has)
        for d in (-1, 1):

            def clear_z(side=(0 if d == -1 else 1)):
                self.clear_columns(2, side)

            pl.when(jnp.logical_not(has[2][d]))(clear_z)

    def clear_columns(self, axis, which):
        for side in range(2):
            for slot in range(3):
                for k in range(4):
                    if axis == 1:
                        zero(self.zy, (side, slot, k, which))
                    elif which == (slot if axis == 0 else side):
                        zero(self.zo, (side, slot, k))
                        zero(self.zy, (side, slot, k))

    def columns(self, edges, side, slot, k):
        if not edges:
            return self.zo[side, slot, k]
        return self.zy[side, slot, k].reshape(2 * HALO, 128)


class Targets(Group):
    def __init__(self, refs, first):
        super().__init__(1, refs)
        self.first = first

    def columns(self, edges, side, slot, k):
        found = self.first.columns(edges, side, slot, 2 + k)
        return found[1:3] if edges else found


class Second(Group):
    fields = 3
    extra_shapes = [(2, 2, HALO, 128), (2, 2, HALO, 128)]

    def __init__(self, refs):
        super().__init__(HALO, refs)
        self.messages = self.messages + [(0, -1, None), (0, 1, None)]
        self.szy, self.zy = self.extra

    def parts(self, d):
        if d[2] == 0:
            return super().parts(d)
        src_side, dst_side = (0, 1) if d[1] == -1 else (1, 0)
        return self.szy.at[:, src_side], self.zy.at[:, dst_side]

    def seal(self, packs):
        for k, pack in enumerate(packs):
            self.put(k, [pack], 3)
            self.put(BX - HALO + k, [pack], 3)
            self.szy[k, 0] = pack[0:HALO]
            self.szy[k, 1] = pack[BX - HALO : BX]

    def clear_columns(self, axis, which):
        if axis == 1:
            for k in range(2):
                zero(self.zy, (k, which))

    def columns(self, edges, side, slot, k):
        if slot == 1:
            return self.zy[k].reshape(2 * HALO, 128)
        x = k if slot == 0 else HALO + BX + k
        return self.ry[3, x].reshape(2 * HALO, 128) if edges else self.ro[3, x]


def merge(packs, unit, field, half, tile, lane4, from_lane):
    to = 32 * (unit % 4) + 8 * field + 4 * half
    shift = (to - from_lane) % 128
    moved = pltpu.roll(tile, shift, 1) if shift else tile
    packs[unit // 4] = jnp.where(lane4 == to // 4, moved, packs[unit // 4])


def pack_block(packs, i, tiles, lane4):
    for c, tile in enumerate(tiles):
        merge(packs, (i + 1) % BX, c, 0, tile, lane4, 0)
        merge(packs, i, c, 1, tile, lane4, 128 - HZ)


def loop(count, body):
    def trip(t, carry):
        for k in range(TOGETHER):
            body(t * TOGETHER + k)
        return carry

    lax.fori_loop(0, count // TOGETHER, trip, 0)
    for k in range(count - count % TOGETHER, count):
        body(k)


def span(row, stride):
    return pl.ds(row, 8) if stride == 1 else pl.ds(row, 8, stride=stride)


def after(ref, row, stride, lane, shift):
    whole, part = divmod(shift, 128)
    near = ref[span(row + whole, stride), :]
    far = ref[span(row + whole + 1, stride), :]
    return pltpu.roll(jnp.where(lane < part, far, near), 128 - part, 1)


def earlier(get, row, lane, shift):
    whole, part = divmod(shift, 128)
    return pltpu.roll(jnp.where(lane >= 128 - part, get(row - whole - 1), get(row - whole)), part, 1)


def differences(u, grads, lane, row, stride=1):
    for c in range(3):
        ref = u.at[c]
        a00 = ref[span(row, stride), :]
        a01 = after(ref, row, stride, lane, 1)
        a10 = after(ref, row, stride, lane, EZ)
        a11 = after(ref, row, stride, lane, EZ + 1)
        s0, s1 = a00 + a01, a10 + a11
        grads[3 * c, span(row, stride), :] = s1 - s0
        grads[3 * c + 1, span(row, stride), :] = s0 + s1
        grads[3 * c + 2, span(row, stride), :] = (a01 - a00) + (a11 - a10)


def stresses(grads, weights, corners, row, stride=1):
    def at(k, r):
        return grads[k, span(r, stride), :]

    deform = []
    for c in range(3):
        fx = at(3 * c, row) + at(3 * c, row + SLAB)
        fy = at(3 * c + 1, row + SLAB) - at(3 * c + 1, row)
        fz = at(3 * c + 2, row) + at(3 * c + 2, row + SLAB)
        deform.append([fx, fy, fz])
    for c in range(3):
        deform[c][c] = deform[c][c] + 1.0
    def dot(i, j):
        return deform[0][i] * deform[0][j] + deform[1][i] * deform[1][j] + deform[2][i] * deform[2][j]

    grams = [dot(0, 0), dot(1, 1), dot(2, 2)]
    total = grams[0] + grams[1] + grams[2]
    scale = jnp.minimum(lax.rsqrt(total * (1.0 / 3.0)), 1.0)
    half = scale * scale * 0.5
    mean = half * total * (1.0 / 3.0)
    d0, d1, d2 = (grams[k] * half - mean for k in range(3))
    d01, d02, d12 = dot(0, 1) * half, dot(0, 2) * half, dot(1, 2) * half
    sq01, sq02, sq12 = d01 * d01, d02 * d02, d12 * d12
    e0, e1, e2 = d0 * d0 + (sq01 + sq02), d1 * d1 + (sq01 + sq12), d2 * d2 + (sq02 + sq12)
    e01, e02, e12 = d02 * d12 - d2 * d01, d01 * d12 - d1 * d02, d01 * d02 - d0 * d12
    p = 0.5 * (e0 + e1 + e2)
    q = d0 * (d1 * d2 - sq12) + (d01 * e01 + d02 * e02)

    def reduced(c0, c1, c2, c3, c4):
        return c0 + q * c3, c1 + (p * c3 + q * c4), c2 + p * c4

    def times_linear(k, c):
        return k * c[0] + q * c[2], (k * c[1] + c[0]) + p * c[2], k * c[2] + c[1]

    low = mean - 1.5
    square = low * low
    t = mean * square + q, 2.0 * (mean * low) + (square + p), mean + 2.0 * low
    poly = times_linear(low, (t[0] - 1.5, t[1], t[2]))
    for step in range(2, POLAR_STEPS):
        c0, c1, c2 = poly
        twice0, twice1 = c0 + c0, c1 + c1
        square = reduced(c0 * c0, twice0 * c1, twice0 * c2 + c1 * c1, twice1 * c2, c2 * c2)
        t0, t1, t2 = times_linear(mean, square)
        t0 = t0 - 1.5
        poly = reduced(
            c0 * t0,
            c0 * t1 + c1 * t0,
            c0 * t2 + c1 * t1 + c2 * t0,
            c1 * t2 + c2 * t1,
            c2 * t2,
        )
    weight = weights[span(row, stride), :]
    heavy = weight * scale
    c0, c1, c2 = weight - heavy * poly[0], heavy * poly[1], heavy * poly[2]
    w0, w1, w2 = (c0 - (c1 * d + c2 * e) for d, e in ((d0, e0), (d1, e1), (d2, e2)))
    w01, w02, w12 = (c1 * d + c2 * e for d, e in ((d01, e01), (d02, e02), (d12, e12)))
    for c in range(3):
        fx, fy, fz = deform[c]
        px = fx * w0 - (fy * w01 + fz * w02)
        py = fy * w1 - (fx * w01 + fz * w12)
        pz = fz * w2 - (fx * w02 + fy * w12)
        s, t = py + px, py - px
        for k, part in enumerate((s + pz, s - pz, t + pz, t - pz)):
            corners[4 * c + k, span(row + VOFF, stride), :] = part


def update(state, u, prev, inertial, rate, corners, omega, lane, row, stride=1):
    seen = state.setdefault(stride, {})

    def spread(c, k):
        def get(r):
            if (c, k, r) not in seen:
                below = corners[4 * c + k, span(r + VOFF - SLAB, stride), :]
                seen[c, k, r] = below - corners[4 * c + 3 - k, span(r + VOFF, stride), :]
            return seen[c, k, r]

        return get

    a = rate[span(row, stride), :]
    result = []
    for c in range(3):
        force = (
            earlier(spread(c, 0), row, lane, EZ + 1) + earlier(spread(c, 1), row, lane, EZ)
        ) + (earlier(spread(c, 2), row, lane, 1) + spread(c, 3)(row))
        here = u[c, span(row, stride), :]
        new = here - a * ((here - inertial[c, span(row, stride), :]) + force)
        if omega is not None:
            old = prev[c, span(row, stride), :]
            new = omega * (new - old) + old
        result.append(new)
    return result


def kernel(
    start_hbm,
    inertial_hbm,
    material_hbm,
    pinned_hbm,
    stiffness,
    out,
    start_v,
    inertial_v,
    material_v,
    pinned_v,
    in_sems,
    ulat,
    wflat,
    iflat,
    pflat,
    rate,
    sums,
    grads,
    corners,
    *group_refs,
):
    pos = [lax.axis_index(a) for a in AXES]
    sizes = [lax.axis_size(a) for a in AXES]
    has = [{-1: p > 0, 0: True, 1: p < n - 1} for p, n in zip(pos, sizes)]
    loads = [
        pltpu.make_async_copy(src, dst, in_sems.at[i])
        for i, (src, dst) in enumerate(
            (
                (start_hbm, start_v),
                (inertial_hbm, inertial_v),
                (material_hbm, material_v),
                (pinned_hbm, pinned_v),
            )
        )
    ]
    for load in loads:
        load.start()
    ends = [5 + len(First.extra_shapes), 10 + len(First.extra_shapes)]
    first = First(group_refs[: ends[0]])
    targets = Targets(group_refs[ends[0] : ends[1]], first)
    second = Second(group_refs[ends[1] :])
    barrier = pltpu.get_barrier_semaphore()
    for d in sorted(DIRS, key=lambda e: -sum(map(abs, e))):

        def greet(d=d):
            pl.semaphore_signal(
                barrier,
                inc=1,
                device_id={a: p + e for a, p, e in zip(AXES, pos, d)},
                device_id_type=pl.DeviceIdType.MESH,
            )

        guarded(every([has[a][d[a]] for a in range(3)]), greet)
    first.clear(has)
    targets.clear(has)

    for load in loads:
        load.wait()
    lane = lax.broadcasted_iota(jnp.int32, (BX, 128), 1)
    grid_y = lax.broadcasted_iota(jnp.int32, (BX, 128), 0) + pos[1] * BX
    grid_z = lane + pos[2] * 128
    inner = (grid_y < BX * sizes[1] - 1) & (grid_z < 128 * sizes[2] - 1)

    lane4 = lane >> 2
    nothing = jnp.zeros((BX, 128), jnp.float32)
    packs = [[nothing, nothing], [nothing, nothing]]
    for i in range(BX):
        pins = pinned_v[i] > 0
        goal = [inertial_v[c, i] * 0.25 for c in range(3)]
        disp = [jnp.where(pins, goal[c], start_v[c, i] * 0.25) for c in range(3)]
        kinds = material_v[i]
        weight = nothing
        for m in range(MATS):
            weight = jnp.where(kinds == m, stiffness[m] * 0.0625, weight)
        valid = inner & (pos[0] * BX + i < BX * sizes[0] - 1)
        fields = (disp + [jnp.where(valid, weight, 0.0)], goal + [jnp.where(pins, 1.0, 0.0)])
        for group, pack, tiles in zip((first, targets), packs, fields):
            group.put(i, tiles)
            pack_block(pack, i, tiles, lane4)
    first.seal(packs[0] + packs[1])

    sides = [1 + (p > 0).astype(jnp.int32) + (p < n - 1).astype(jnp.int32) for p, n in zip(pos, sizes)]
    pl.semaphore_wait(barrier, sides[0] * sides[1] * sides[2] - 1)
    first.send(pos, has)
    targets.send(pos, has)
    second.clear(has)

    u0, u1, u2 = (ulat.at[k] for k in range(3))
    firsts = [u0.at[c] for c in range(3)] + [wflat]
    goals = [iflat.at[c] for c in range(3)] + [pflat]

    def wide(group, fields, u, between):
        def inside(t):
            stresses(grads, wflat, corners, 26 + 8 * t)

        def outside(t):
            stresses(grads, wflat, corners, jnp.where(t < 4, 0, 82) + 8 * t)

        def columns(numbers, shift):
            for r in numbers:
                differences(u, grads, lane, HALO * SLAB + r, SLAB)
            loop(6, lambda t: stresses(grads, wflat, corners, HALO * SLAB + shift(t), SLAB))

        if group is second:
            columns(range(3, 9), lambda t: 3 + t)
            group.wait_recv(pos, has, False)
            group.to_flat(fields, False, True)
            columns((0, 1, 2, 9, 10, 11), lambda t: t + jnp.where(t < 3, 0, 6))
        else:
            group.wait_recv(pos, has, False)
            group.to_flat(fields, False)
            for r in range(26, 130, 8):
                differences(u, grads, lane, r)
            loop(12, inside)
        between()
        group.wait_recv(pos, has, True)
        group.to_flat(fields, True)
        for r in (*range(0, 32, 8), *range(130, 162, 8)):
            differences(u, grads, lane, r)
        loop(8, outside)

    def narrow(u):
        for r in range(1, 11):
            differences(u, grads, lane, SLAB + r, SLAB)
        for r in (9 * SLAB + 1, 9 * SLAB + 3, 10 * SLAB + 1, 10 * SLAB + 3):
            differences(u, grads, lane, r)

        def column(t):
            stresses(grads, wflat, corners, SLAB + 1 + t, SLAB)

        loop(10, column)
        for r in (9 * SLAB + 1, 9 * SLAB + 3):
            stresses(grads, wflat, corners, r)

    inner = range(3 * SLAB, 9 * SLAB, 8)
    outer = (*range(SLAB, 3 * SLAB, 8), *range(9 * SLAB, 11 * SLAB, 8))

    def update_rows(blocks, u, prev, fresh, omega):
        for r in blocks:
            new = update({}, u, prev, iflat, rate, corners, omega, lane, r)
            for c in range(3):
                fresh[c, pl.ds(r, 8), :] = new[c]

    def rates(blocks):
        for r in blocks:
            sums[pl.ds(r, 8), :] = wflat[pl.ds(r, 8), :] + wflat[pl.ds(r - SLAB, 8), :]

        def get(row):
            return sums[pl.ds(row, 8), :]

        for r in blocks:
            total = (earlier(get, r, lane, EZ + 1) + earlier(get, r, lane, EZ)) + (
                earlier(get, r, lane, 1) + get(r)
            )
            rate[pl.ds(r, 8), :] = jnp.where(
                pflat[pl.ds(r, 8), :] > 0.0, 0.0, relax / (1.0 + 3.0 * total)
            )

    def update_own(u, prev, omega):
        state = {}
        return [
            update(state, u, prev, iflat, rate, corners, omega, lane, HALO * SLAB + r, SLAB)
            for r in range(HALO, HALO + BX + 1)
        ]

    def own_tile(rows, i, c):
        shift = 8 * (HALO + i) + HZ
        return pltpu.roll(jnp.where(lane >= shift, rows[i][c], rows[i + 1][c]), 128 - shift, 1)

    omega1 = 2.0 / (2.0 - radius * radius)
    omega2 = 4.0 / (4.0 - radius * radius * omega1)
    omega3 = 4.0 / (4.0 - radius * radius * omega2)

    def inner_first():
        targets.wait_recv(pos, has, False)
        targets.to_flat(goals, False)
        rates(inner)
        update_rows(inner, u0, None, u1, None)

    wide(first, firsts, u0, inner_first)
    targets.wait_recv(pos, has, True)
    targets.to_flat(goals, True)
    rates(outer)
    update_rows(outer, u0, None, u1, None)
    narrow(u1)
    rows = update_own(u1, u0, omega1)
    pack = [nothing, nothing]
    for i in range(BX):
        second.put(i, [own_tile(rows, i, c) for c in range(3)])
    for i in range(BX + 1):
        place = HALO + i
        for c in range(3):
            if i > 0:
                merge(pack, i % BX, c, 0, rows[i][c], lane4, 8 * place - HZ)
            if i < BX:
                merge(pack, i, c, 1, rows[i][c], lane4, 8 * place)
    second.seal(pack)
    second.send(pos, has)
    for i in range(BX + 1):
        for c in range(3):
            u2[c, pl.ds(HALO * SLAB + HALO + i, BX, stride=SLAB), :] = rows[i][c]

    first.wait_send(pos, has)
    targets.wait_send(pos, has)
    wide(
        second,
        [u2.at[c] for c in range(3)],
        u2,
        lambda: update_rows(inner, u2, u1, u0, omega2),
    )
    second.wait_send(pos, has)
    update_rows(outer, u2, u1, u0, omega2)
    narrow(u0)
    rows = update_own(u0, u2, omega3)
    for i in range(BX):
        for c in range(3):
            out[c, i] = 4.0 * own_tile(rows, i, c)


def per_device(start_disp, inertial, material, pinned, stiffness):
    f = jnp.float32
    flat = (ROWS, 128)
    hbm = pl.BlockSpec(memory_space=pl.ANY)
    return pl.pallas_call(
        kernel,
        out_shape=pltpu.VMEM(start_disp.shape, f),
        in_specs=[hbm, hbm, hbm, hbm, pl.BlockSpec(memory_space=pltpu.SMEM)],
        out_specs=pl.BlockSpec(memory_space=pltpu.VMEM),
        scratch_shapes=[
            pltpu.VMEM(start_disp.shape, f),
            pltpu.VMEM(inertial.shape, f),
            pltpu.VMEM(material.shape, jnp.int32),
            pltpu.VMEM(pinned.shape, jnp.int32),
            pltpu.SemaphoreType.DMA((4,)),
            pltpu.VMEM((3, 3, *flat), f),
            pltpu.VMEM(flat, f),
            pltpu.VMEM((3, *flat), f),
            pltpu.VMEM(flat, f),
            pltpu.VMEM(flat, f),
            pltpu.VMEM(flat, f),
            pltpu.VMEM((9, *flat), f),
            pltpu.VMEM((12, *flat), f),
            *Group.scratch(HALO, len(DIRS), First.extra_shapes),
            *Group.scratch(1, 8),
            *Group.scratch(HALO, 10, Second.extra_shapes),
        ],
        compiler_params=pltpu.CompilerParams(collective_id=0, has_side_effects=True),
    )(start_disp, inertial, material, pinned, stiffness)


def solution(mesh):
    placed = (
        P(None, "gx", "gy", "gz"),
        P(None, "gx", "gy", "gz"),
        P("gx", "gy", "gz"),
        P("gx", "gy", "gz"),
        P(),
    )
    return jax.shard_map(
        per_device, mesh=mesh, in_specs=placed, out_specs=P(None, "gx", "gy", "gz"), check_vma=False
    )
```

```python
import functools

import jax
import jax.numpy as jnp
from jax import lax
from jax.experimental import pallas as pl
from jax.experimental.pallas import tpu as pltpu
from jax.sharding import PartitionSpec as P

ITERS = 4
POLAR_STEPS = 6
MATS = 8

relax = 0.6
radius = 0.9

AXES = ("gx", "gy", "gz")
BX = 8
HALO = 2
EX = BX + 2 * HALO
HZ = 2 * HALO
EZ = 128 + 2 * HZ
SLAB = 13
ROWS = 176
VOFF = 16
TOGETHER = 2
DIRS = [
    (dx, dy, dz)
    for dx in (-1, 0, 1)
    for dy in (-1, 0, 1)
    for dz in (-1, 0, 1)
    if (dx, dy, dz) != (0, 0, 0)
]


def every(conds):
    conds = [c for c in conds if c is not True]
    return functools.reduce(lambda p, q: p & q, conds) if conds else True


def guarded(cond, act):
    if cond is True:
        act()
    else:
        pl.when(cond)(act)


def zero(ref, index):
    ref[index] = jnp.zeros(ref.at[index].shape, jnp.float32)


class Group:
    fields = 4

    def __init__(self, width, refs):
        self.h = width
        self.ro, self.ry, self.sy, self.ssem, self.rsem, *self.extra = refs
        self.messages = [d for d in DIRS if d[2] == 0]

    @staticmethod
    def scratch(width, total, extra=()):
        f = jnp.float32
        return [
            pltpu.VMEM((4, EX, BX, 128), f),
            pltpu.VMEM((4, EX, 2, width, 128), f),
            pltpu.VMEM((4, BX, 2, width, 128), f),
            pltpu.SemaphoreType.DMA((total,)),
            pltpu.SemaphoreType.DMA((total,)),
            *(pltpu.VMEM(shape, f) for shape in extra),
        ]

    def parts(self, d):
        dx, dy, _ = d
        h = self.h
        src_x = {-1: (0, h), 0: (0, BX), 1: (BX - h, h)}[dx]
        dst_x = {-1: (HALO + BX, h), 0: (HALO, BX), 1: (HALO - h, h)}[dx]
        count = self.fields if dx == 0 else 4
        fields, sx, tx = pl.ds(0, count), pl.ds(*src_x), pl.ds(*dst_x)
        if dy == 0:
            return self.ro.at[:, pl.ds(HALO + src_x[0], src_x[1])], self.ro.at[:, tx]
        src_side, dst_side = (0, 1) if dy == -1 else (1, 0)
        return self.sy.at[fields, sx, src_side], self.ry.at[fields, tx, dst_side]

    def copy(self, index, pos):
        d = self.messages[index]
        src, dst = self.parts(d)
        return pltpu.make_async_remote_copy(
            src_ref=src,
            dst_ref=dst,
            send_sem=self.ssem.at[index],
            recv_sem=self.rsem.at[index],
            device_id={a: p + (e or 0) for a, p, e in zip(AXES, pos, d)},
            device_id_type=pl.DeviceIdType.MESH,
        )

    def put(self, i, tiles, field=0):
        h = self.h
        for c, tile in enumerate(tiles):
            self.ro[field + c, HALO + i] = tile
            self.sy[field + c, i, 0] = tile[0:h]
            self.sy[field + c, i, 1] = tile[BX - h : BX]

    def clear(self, has):
        for d in (-1, 1):
            start = HALO + BX if d == 1 else HALO - self.h
            side = 0 if d == -1 else 1

            def clear_x(start=start, slot=1 + d):
                for c in range(4):
                    for x in range(start, start + self.h):
                        zero(self.ro, (c, x))
                        zero(self.ry, (c, x))
                self.clear_columns(0, slot)

            pl.when(jnp.logical_not(has[0][d]))(clear_x)

            def clear_y(side=side):
                for c in range(4):
                    for x in range(EX):
                        zero(self.ry, (c, x, side))
                self.clear_columns(1, side)

            pl.when(jnp.logical_not(has[1][d]))(clear_y)

    def clear_columns(self, axis, which):
        pass

    def send(self, pos, has):
        for index, d in sorted(
            enumerate(self.messages), key=lambda e: (e[1][1] != 0, -sum(abs(a or 0) for a in e[1]))
        ):
            guarded(every([has[a][d[a] or 0] for a in range(3)]), self.copy(index, pos).start)

    def wait_recv(self, pos, has, edges):
        for index, d in enumerate(self.messages):
            if (d[1] != 0) == edges:
                there = every([has[a][-(d[a] or 0)] for a in range(3)])
                guarded(there, self.copy(index, pos).wait_recv)

    def wait_send(self, pos, has):
        for index, d in enumerate(self.messages):
            guarded(every([has[a][d[a] or 0] for a in range(3)]), self.copy(index, pos).wait_send)

    def to_flat(self, targets, edges, kept=False):
        h = self.h
        rows = 2 * h if edges else BX
        lane = lax.broadcasted_iota(jnp.int32, (rows, 128), 1)
        main = self.ry if edges else self.ro
        nothing = jnp.zeros((rows, 128), jnp.float32)
        before = [nothing] * len(targets)
        for place in range(SLAB):
            if kept and HALO < place < HALO + BX:
                continue
            first, last = place == 0, place == SLAB - 1
            slot, before_slot = ((p >= HALO) + (p >= HALO + BX) for p in (place, place - 1))
            unit = (place - HALO) % BX

            def columns(side, slot):
                if kept and slot == 1:
                    return nothing
                return self.columns(edges, side, slot, unit // 4)

            both = jnp.where(
                (lane & 7) < HZ,
                nothing if first else columns(1, before_slot),
                nothing if last else columns(0, slot),
            )
            for c, out in enumerate(targets):
                if last or (kept and slot == 1):
                    now = nothing
                else:
                    now = pltpu.roll(main[c, place].reshape(rows, 128), 8 * place + HZ, 1)
                ends = pltpu.roll(both, (8 * place - HZ - 32 * (unit % 4) - 8 * c) % 128, 1)
                flat = jnp.where(
                    lane >= 8 * place + HZ,
                    now,
                    jnp.where(lane < 8 * place - HZ, before[c], ends),
                )
                before[c] = now
                if not edges:
                    where = pl.ds(HALO * SLAB + place, BX, stride=SLAB)
                    if kept and place == HALO:
                        flat = jnp.where(lane < 8 * place, flat, out[where, :])
                    if kept and place == HALO + BX:
                        flat = jnp.where(lane < 8 * place, out[where, :], flat)
                    out[where, :] = flat
                elif h == 1:
                    out[pl.ds(SLAB + place, 2, stride=9 * SLAB), :] = flat
                else:
                    out[pl.ds(place, 2, stride=SLAB), :] = flat[0:2]
                    out[pl.ds(10 * SLAB + place, 2, stride=SLAB), :] = flat[2:4]


class First(Group):
    extra_shapes = [
        (4, BX, 128),
        (4, 2, HALO, 128),
        (2, 3, 4, BX, 128),
        (2, 3, 4, 2, HALO, 128),
    ]

    def __init__(self, refs):
        super().__init__(HALO, refs)
        self.messages = list(DIRS)
        self.szo, self.szy, self.zo, self.zy = self.extra

    def parts(self, d):
        dx, dy, dz = d
        if dz == 0:
            return super().parts(d)
        side, slot = (0 if dz == 1 else 1), 1 - dx
        tiles = pl.ds(0, 2 if dx == -1 else 4)
        if dy == 0:
            return self.szo.at[tiles], self.zo.at[side, slot, tiles]
        src_side, dst_side = (0, 1) if dy == -1 else (1, 0)
        return self.szy.at[tiles, src_side], self.zy.at[side, slot, tiles, dst_side]

    def seal(self, packs):
        for k, pack in enumerate(packs):
            self.szo[k] = pack
            self.szy[k, 0] = pack[0:HALO]
            self.szy[k, 1] = pack[BX - HALO : BX]

    def clear(self, has):
        super().clear(has)
        for d in (-1, 1):

            def clear_z(side=(0 if d == -1 else 1)):
                self.clear_columns(2, side)

            pl.when(jnp.logical_not(has[2][d]))(clear_z)

    def clear_columns(self, axis, which):
        for side in range(2):
            for slot in range(3):
                for k in range(4):
                    if axis == 1:
                        zero(self.zy, (side, slot, k, which))
                    elif which == (slot if axis == 0 else side):
                        zero(self.zo, (side, slot, k))
                        zero(self.zy, (side, slot, k))

    def columns(self, edges, side, slot, k, group=0):
        if not edges:
            return self.zo[side, slot, 2 * k + group]
        return self.zy[side, slot, 2 * k + group].reshape(2 * HALO, 128)


class Targets(Group):
    def __init__(self, refs, first):
        super().__init__(1, refs)
        self.first = first

    def columns(self, edges, side, slot, k):
        found = self.first.columns(edges, side, slot, k, 1)
        return found[1:3] if edges else found


class Second(Group):
    fields = 3
    extra_shapes = [(2, 2, HALO, 128), (2, 2, HALO, 128)]

    def __init__(self, refs):
        super().__init__(HALO, refs)
        self.messages = self.messages + [(0, -1, None), (0, 1, None)]
        self.szy, self.zy = self.extra

    def parts(self, d):
        if d[2] == 0:
            return super().parts(d)
        src_side, dst_side = (0, 1) if d[1] == -1 else (1, 0)
        return self.szy.at[:, src_side], self.zy.at[:, dst_side]

    def seal(self, packs):
        for k, pack in enumerate(packs):
            self.put(k, [pack], 3)
            self.put(BX - HALO + k, [pack], 3)
            self.szy[k, 0] = pack[0:HALO]
            self.szy[k, 1] = pack[BX - HALO : BX]

    def clear_columns(self, axis, which):
        if axis == 1:
            for k in range(2):
                zero(self.zy, (k, which))

    def columns(self, edges, side, slot, k):
        if slot == 1:
            return self.zy[k].reshape(2 * HALO, 128)
        x = k if slot == 0 else HALO + BX + k
        return self.ry[3, x].reshape(2 * HALO, 128) if edges else self.ro[3, x]


def merge(packs, unit, field, half, tile, lane4, from_lane):
    to = 32 * (unit % 4) + 8 * field + 4 * half
    shift = (to - from_lane) % 128
    moved = pltpu.roll(tile, shift, 1) if shift else tile
    packs[unit // 4] = jnp.where(lane4 == to // 4, moved, packs[unit // 4])


def pack_block(packs, i, tiles, lane4):
    for c, tile in enumerate(tiles):
        merge(packs, (i + 1) % BX, c, 0, tile, lane4, 0)
        merge(packs, i, c, 1, tile, lane4, 128 - HZ)


def loop(count, body):
    def trip(t, carry):
        for k in range(TOGETHER):
            body(t * TOGETHER + k)
        return carry

    lax.fori_loop(0, count // TOGETHER, trip, 0)
    for k in range(count - count % TOGETHER, count):
        body(k)


def span(row, stride):
    return pl.ds(row, 8) if stride == 1 else pl.ds(row, 8, stride=stride)


def after(ref, row, stride, lane, shift):
    whole, part = divmod(shift, 128)
    near = ref[span(row + whole, stride), :]
    far = ref[span(row + whole + 1, stride), :]
    return pltpu.roll(jnp.where(lane < part, far, near), 128 - part, 1)


def earlier(get, row, lane, shift):
    whole, part = divmod(shift, 128)
    return pltpu.roll(jnp.where(lane >= 128 - part, get(row - whole - 1), get(row - whole)), part, 1)


def differences(u, grads, lane, row, stride=1):
    for c in range(3):
        ref = u.at[c]
        a00 = ref[span(row, stride), :]
        a01 = after(ref, row, stride, lane, 1)
        a10 = after(ref, row, stride, lane, EZ)
        a11 = after(ref, row, stride, lane, EZ + 1)
        s0, s1 = a00 + a01, a10 + a11
        grads[3 * c, span(row, stride), :] = s1 - s0
        grads[3 * c + 1, span(row, stride), :] = s0 + s1
        grads[3 * c + 2, span(row, stride), :] = (a01 - a00) + (a11 - a10)


def stresses(grads, weights, corners, row, stride=1):
    def at(k, r):
        return grads[k, span(r, stride), :]

    deform = []
    for c in range(3):
        fx = at(3 * c, row) + at(3 * c, row + SLAB)
        fy = at(3 * c + 1, row + SLAB) - at(3 * c + 1, row)
        fz = at(3 * c + 2, row) + at(3 * c + 2, row + SLAB)
        deform.append([fx, fy, fz])
    for c in range(3):
        deform[c][c] = deform[c][c] + 1.0
    def dot(i, j):
        return deform[0][i] * deform[0][j] + deform[1][i] * deform[1][j] + deform[2][i] * deform[2][j]

    grams = [dot(0, 0), dot(1, 1), dot(2, 2)]
    total = grams[0] + grams[1] + grams[2]
    scale = jnp.minimum(lax.rsqrt(total * (1.0 / 3.0)), 1.0)
    half = scale * scale * 0.5
    mean = half * total * (1.0 / 3.0)
    d0, d1, d2 = (grams[k] * half - mean for k in range(3))
    d01, d02, d12 = dot(0, 1) * half, dot(0, 2) * half, dot(1, 2) * half
    sq01, sq02, sq12 = d01 * d01, d02 * d02, d12 * d12
    e0, e1, e2 = d0 * d0 + (sq01 + sq02), d1 * d1 + (sq01 + sq12), d2 * d2 + (sq02 + sq12)
    e01, e02, e12 = d02 * d12 - d2 * d01, d01 * d12 - d1 * d02, d01 * d02 - d0 * d12
    p = 0.5 * (e0 + e1 + e2)
    q = d0 * (d1 * d2 - sq12) + (d01 * e01 + d02 * e02)

    def reduced(c0, c1, c2, c3, c4):
        return c0 + q * c3, c1 + (p * c3 + q * c4), c2 + p * c4

    def times_linear(k, c):
        return k * c[0] + q * c[2], (k * c[1] + c[0]) + p * c[2], k * c[2] + c[1]

    low = mean - 1.5
    square = low * low
    t = mean * square + q, 2.0 * (mean * low) + (square + p), mean + 2.0 * low
    poly = times_linear(low, (t[0] - 1.5, t[1], t[2]))
    for step in range(2, POLAR_STEPS):
        c0, c1, c2 = poly
        twice0, twice1 = c0 + c0, c1 + c1
        square = reduced(c0 * c0, twice0 * c1, twice0 * c2 + c1 * c1, twice1 * c2, c2 * c2)
        t0, t1, t2 = times_linear(mean, square)
        t0 = t0 - 1.5
        poly = reduced(
            c0 * t0,
            c0 * t1 + c1 * t0,
            c0 * t2 + c1 * t1 + c2 * t0,
            c1 * t2 + c2 * t1,
            c2 * t2,
        )
    weight = weights[span(row, stride), :]
    heavy = weight * scale
    c0, c1, c2 = weight - heavy * poly[0], heavy * poly[1], heavy * poly[2]
    w0, w1, w2 = (c0 - (c1 * d + c2 * e) for d, e in ((d0, e0), (d1, e1), (d2, e2)))
    w01, w02, w12 = (c1 * d + c2 * e for d, e in ((d01, e01), (d02, e02), (d12, e12)))
    for c in range(3):
        fx, fy, fz = deform[c]
        px = fx * w0 - (fy * w01 + fz * w02)
        py = fy * w1 - (fx * w01 + fz * w12)
        pz = fz * w2 - (fx * w02 + fy * w12)
        s, t = py + px, py - px
        for k, part in enumerate((s + pz, s - pz, t + pz, t - pz)):
            corners[4 * c + k, span(row + VOFF, stride), :] = part


def update(state, u, prev, inertial, rate, corners, omega, lane, row, stride=1):
    seen = state.setdefault(stride, {})

    def spread(c, k):
        def get(r):
            if (c, k, r) not in seen:
                below = corners[4 * c + k, span(r + VOFF - SLAB, stride), :]
                seen[c, k, r] = below - corners[4 * c + 3 - k, span(r + VOFF, stride), :]
            return seen[c, k, r]

        return get

    a = rate[span(row, stride), :]
    result = []
    for c in range(3):
        force = (
            earlier(spread(c, 0), row, lane, EZ + 1) + earlier(spread(c, 1), row, lane, EZ)
        ) + (earlier(spread(c, 2), row, lane, 1) + spread(c, 3)(row))
        here = u[c, span(row, stride), :]
        new = here - a * ((here - inertial[c, span(row, stride), :]) + force)
        if omega is not None:
            old = prev[c, span(row, stride), :]
            new = omega * (new - old) + old
        result.append(new)
    return result


def kernel(
    start_hbm,
    inertial_hbm,
    material_hbm,
    pinned_hbm,
    stiffness,
    out,
    start_v,
    inertial_v,
    material_v,
    pinned_v,
    in_sems,
    ulat,
    wflat,
    iflat,
    pflat,
    rate,
    sums,
    grads,
    corners,
    *group_refs,
):
    pos = [lax.axis_index(a) for a in AXES]
    sizes = [lax.axis_size(a) for a in AXES]
    has = [{-1: p > 0, 0: True, 1: p < n - 1} for p, n in zip(pos, sizes)]
    loads = [
        pltpu.make_async_copy(src, dst, in_sems.at[i])
        for i, (src, dst) in enumerate(
            (
                (start_hbm, start_v),
                (inertial_hbm, inertial_v),
                (material_hbm, material_v),
                (pinned_hbm, pinned_v),
            )
        )
    ]
    for load in loads:
        load.start()
    ends = [5 + len(First.extra_shapes), 10 + len(First.extra_shapes)]
    first = First(group_refs[: ends[0]])
    targets = Targets(group_refs[ends[0] : ends[1]], first)
    second = Second(group_refs[ends[1] :])
    barrier = pltpu.get_barrier_semaphore()
    for d in sorted(DIRS, key=lambda e: -sum(map(abs, e))):

        def greet(d=d):
            pl.semaphore_signal(
                barrier,
                inc=1,
                device_id={a: p + e for a, p, e in zip(AXES, pos, d)},
                device_id_type=pl.DeviceIdType.MESH,
            )

        guarded(every([has[a][d[a]] for a in range(3)]), greet)
    first.clear(has)
    targets.clear(has)

    for load in loads:
        load.wait()
    lane = lax.broadcasted_iota(jnp.int32, (BX, 128), 1)
    grid_y = lax.broadcasted_iota(jnp.int32, (BX, 128), 0) + pos[1] * BX
    grid_z = lane + pos[2] * 128
    inner = (grid_y < BX * sizes[1] - 1) & (grid_z < 128 * sizes[2] - 1)

    lane4 = lane >> 2
    nothing = jnp.zeros((BX, 128), jnp.float32)
    packs = [[nothing, nothing], [nothing, nothing]]
    for i in range(BX):
        pins = pinned_v[i] > 0
        goal = [inertial_v[c, i] * 0.25 for c in range(3)]
        disp = [jnp.where(pins, goal[c], start_v[c, i] * 0.25) for c in range(3)]
        kinds = material_v[i]
        weight = nothing
        for m in range(MATS):
            weight = jnp.where(kinds == m, stiffness[m] * 0.0625, weight)
        valid = inner & (pos[0] * BX + i < BX * sizes[0] - 1)
        fields = (disp + [jnp.where(valid, weight, 0.0)], goal + [jnp.where(pins, 1.0, 0.0)])
        for group, pack, tiles in zip((first, targets), packs, fields):
            group.put(i, tiles)
            pack_block(pack, i, tiles, lane4)
    first.seal([packs[g][k] for k in range(2) for g in range(2)])

    sides = [1 + (p > 0).astype(jnp.int32) + (p < n - 1).astype(jnp.int32) for p, n in zip(pos, sizes)]
    pl.semaphore_wait(barrier, sides[0] * sides[1] * sides[2] - 1)
    first.send(pos, has)
    targets.send(pos, has)
    second.clear(has)

    u0, u1, u2 = (ulat.at[k] for k in range(3))
    firsts = [u0.at[c] for c in range(3)] + [wflat]
    goals = [iflat.at[c] for c in range(3)] + [pflat]

    def wide(group, fields, u, between):
        def inside(t):
            stresses(grads, wflat, corners, 26 + 8 * t)

        def outside(t):
            stresses(grads, wflat, corners, jnp.where(t < 4, 0, 82) + 8 * t)

        def columns(numbers, shift):
            for r in numbers:
                differences(u, grads, lane, HALO * SLAB + r, SLAB)
            loop(6, lambda t: stresses(grads, wflat, corners, HALO * SLAB + shift(t), SLAB))

        if group is second:
            columns(range(3, 9), lambda t: 3 + t)
            group.wait_recv(pos, has, False)
            group.to_flat(fields, False, True)
            columns((0, 1, 2, 9, 10, 11), lambda t: t + jnp.where(t < 3, 0, 6))
        else:
            group.wait_recv(pos, has, False)
            group.to_flat(fields, False)
            for r in range(26, 130, 8):
                differences(u, grads, lane, r)
            loop(12, inside)
        between()
        group.wait_recv(pos, has, True)
        group.to_flat(fields, True)
        for r in (*range(0, 32, 8), *range(130, 162, 8)):
            differences(u, grads, lane, r)
        loop(8, outside)

    def narrow(u):
        for r in range(1, 11):
            differences(u, grads, lane, SLAB + r, SLAB)
        for r in (9 * SLAB + 1, 9 * SLAB + 3, 10 * SLAB + 1, 10 * SLAB + 3):
            differences(u, grads, lane, r)

        def column(t):
            stresses(grads, wflat, corners, SLAB + 1 + t, SLAB)

        loop(10, column)
        for r in (9 * SLAB + 1, 9 * SLAB + 3):
            stresses(grads, wflat, corners, r)

    inner = range(3 * SLAB, 9 * SLAB, 8)
    outer = (*range(SLAB, 3 * SLAB, 8), *range(9 * SLAB, 11 * SLAB, 8))

    def update_rows(blocks, u, prev, fresh, omega):
        for r in blocks:
            new = update({}, u, prev, iflat, rate, corners, omega, lane, r)
            for c in range(3):
                fresh[c, pl.ds(r, 8), :] = new[c]

    def rates(blocks):
        for r in blocks:
            sums[pl.ds(r, 8), :] = wflat[pl.ds(r, 8), :] + wflat[pl.ds(r - SLAB, 8), :]

        def get(row):
            return sums[pl.ds(row, 8), :]

        for r in blocks:
            total = (earlier(get, r, lane, EZ + 1) + earlier(get, r, lane, EZ)) + (
                earlier(get, r, lane, 1) + get(r)
            )
            rate[pl.ds(r, 8), :] = jnp.where(
                pflat[pl.ds(r, 8), :] > 0.0, 0.0, relax / (1.0 + 3.0 * total)
            )

    def update_own(u, prev, omega):
        state = {}
        return [
            update(state, u, prev, iflat, rate, corners, omega, lane, HALO * SLAB + r, SLAB)
            for r in range(HALO, HALO + BX + 1)
        ]

    def own_tile(rows, i, c):
        shift = 8 * (HALO + i) + HZ
        return pltpu.roll(jnp.where(lane >= shift, rows[i][c], rows[i + 1][c]), 128 - shift, 1)

    omega1 = 2.0 / (2.0 - radius * radius)
    omega2 = 4.0 / (4.0 - radius * radius * omega1)
    omega3 = 4.0 / (4.0 - radius * radius * omega2)

    def inner_first():
        targets.wait_recv(pos, has, False)
        targets.to_flat(goals, False)
        rates(inner)
        update_rows(inner, u0, None, u1, None)

    wide(first, firsts, u0, inner_first)
    targets.wait_recv(pos, has, True)
    targets.to_flat(goals, True)
    rates(outer)
    update_rows(outer, u0, None, u1, None)
    narrow(u1)
    rows = update_own(u1, u0, omega1)
    pack = [nothing, nothing]
    for i in range(BX):
        second.put(i, [own_tile(rows, i, c) for c in range(3)])
    for i in range(BX + 1):
        place = HALO + i
        for c in range(3):
            if i > 0:
                merge(pack, i % BX, c, 0, rows[i][c], lane4, 8 * place - HZ)
            if i < BX:
                merge(pack, i, c, 1, rows[i][c], lane4, 8 * place)
    second.seal(pack)
    second.send(pos, has)
    for i in range(BX + 1):
        for c in range(3):
            u2[c, pl.ds(HALO * SLAB + HALO + i, BX, stride=SLAB), :] = rows[i][c]

    first.wait_send(pos, has)
    targets.wait_send(pos, has)
    wide(
        second,
        [u2.at[c] for c in range(3)],
        u2,
        lambda: update_rows(inner, u2, u1, u0, omega2),
    )
    second.wait_send(pos, has)
    update_rows(outer, u2, u1, u0, omega2)
    narrow(u0)
    rows = update_own(u0, u2, omega3)
    for i in range(BX):
        for c in range(3):
            out[c, i] = 4.0 * own_tile(rows, i, c)


def per_device(start_disp, inertial, material, pinned, stiffness):
    f = jnp.float32
    flat = (ROWS, 128)
    hbm = pl.BlockSpec(memory_space=pl.ANY)
    return pl.pallas_call(
        kernel,
        out_shape=pltpu.VMEM(start_disp.shape, f),
        in_specs=[hbm, hbm, hbm, hbm, pl.BlockSpec(memory_space=pltpu.SMEM)],
        out_specs=pl.BlockSpec(memory_space=pltpu.VMEM),
        scratch_shapes=[
            pltpu.VMEM(start_disp.shape, f),
            pltpu.VMEM(inertial.shape, f),
            pltpu.VMEM(material.shape, jnp.int32),
            pltpu.VMEM(pinned.shape, jnp.int32),
            pltpu.SemaphoreType.DMA((4,)),
            pltpu.VMEM((3, 3, *flat), f),
            pltpu.VMEM(flat, f),
            pltpu.VMEM((3, *flat), f),
            pltpu.VMEM(flat, f),
            pltpu.VMEM(flat, f),
            pltpu.VMEM(flat, f),
            pltpu.VMEM((9, *flat), f),
            pltpu.VMEM((12, *flat), f),
            *Group.scratch(HALO, len(DIRS), First.extra_shapes),
            *Group.scratch(1, 8),
            *Group.scratch(HALO, 10, Second.extra_shapes),
        ],
        compiler_params=pltpu.CompilerParams(collective_id=0, has_side_effects=True),
    )(start_disp, inertial, material, pinned, stiffness)


def solution(mesh):
    placed = (
        P(None, "gx", "gy", "gz"),
        P(None, "gx", "gy", "gz"),
        P("gx", "gy", "gz"),
        P("gx", "gy", "gz"),
        P(),
    )
    return jax.shard_map(
        per_device, mesh=mesh, in_specs=placed, out_specs=P(None, "gx", "gy", "gz"), check_vma=False
    )
```
